256 devices in a mesh: dp: 8 (over z), expert: 8 (over x, y_lo), shard: 4 (over y_hi, core).
Axes of the slice: x: 4, y: 4 (y_hi: 2, y_lo: 2; y = y_hi * 2 + y_lo), z: 8, core: 2. Of those that a mesh axis runs over, the one named last changes fastest.
Arguments:
- activations: bfloat16 [2, 8, 4096, 256], P(None, 'expert', ('dp', 'shard')), may hold values from -6 to 6
- out_grads: bfloat16 [2, 8, 4096, 14336], P(None, 'expert', ('dp', 'shard')), may hold values from -0.25 to 0.25
- weights: float32 [2, 8, 256, 14336], P(None, 'expert', ('dp', 'shard')), may hold values from -4 to 4
- shadow: float32 [2, 8, 256, 14336], P(None, 'expert', ('dp', 'shard')), may hold values from -4 to 4
- counts: int32 [2, 256, 8], P(None, ('dp', 'expert', 'shard')), may hold values from 1 to 1024, as said below
Outputs:
- new_weights: float32 [2, 8, 256, 14336], P(None, 'expert', ('dp', 'shard'))
- new_shadow: float32 [2, 8, 256, 14336], P(None, 'expert', ('dp', 'shard'))
The draws below stay inside these ranges and needn't reach their ends.
Inputs may be any that keep to these rules, and one draw needn't show every extreme that they name: `counts`: loads differ between the experts of a layer.
All inputs are finite; a program needn't handle non-finite values.
Results may differ from the reference program's by a relative error of at most 0.0003.
Values sent between devices are 32-bit elements; how exact they have to be, the bound alone decides.
A program may use at most 128 MiB of HBM per device.

```python
import jax
import jax.numpy as jnp
from jax import lax

FF = 14336
ROWS = 256
TOK_DEV = 128
LAYERS = 2
EXPERTS = 8
TOKENS = 4096
DEVICES = 256


def draw_activations(key, part):
    base = jax.random.normal(key, (LAYERS, EXPERTS, TOKENS, ROWS), jnp.float32)
    return jnp.clip(base, -6.0, 6.0).astype(jnp.bfloat16)


def draw_out_grads(key, part):
    base = 0.03 * jax.random.normal(key, (LAYERS, EXPERTS, TOKENS, FF), jnp.float32)
    return jnp.clip(base, -0.25, 0.25).astype(jnp.bfloat16)


def draw_counts(key, part):
    ranges = jax.random.randint(jax.random.fold_in(key, 3), (LAYERS, 1, EXPERTS), 1, 9)
    raw = jax.random.randint(key, (LAYERS, DEVICES, EXPERTS), 0, 1 << 20)
    values = 1 + raw % (TOK_DEV * ranges)
    chosen_device = jax.random.randint(jax.random.fold_in(key, 5), (LAYERS, 1, 1), 0, DEVICES)
    chosen_expert = jax.random.randint(jax.random.fold_in(key, 6), (LAYERS, 1, 1), 0, EXPERTS)
    device_ids = jnp.arange(DEVICES, dtype=jnp.int32)[None, :, None]
    expert_ids = jnp.arange(EXPERTS, dtype=jnp.int32)[None, None, :]
    marked = (device_ids == chosen_device) & (expert_ids == chosen_expert)
    values = jnp.where(marked, 8 * TOK_DEV, values)
    return values.astype(jnp.int32)


def levels(key, dims, pieces, low, largest):
    level, own = 1.0, jax.random.fold_in(key, 6)
    for axis_at, parts in pieces:
        steps = jnp.exp(jax.random.uniform(jax.random.fold_in(own, axis_at), (parts,), jnp.float32, low / len(pieces), largest / len(pieces)))
        level = level * jnp.repeat(steps, dims[axis_at] // parts).reshape([-1 if axis == axis_at else 1 for axis in range(len(dims))])
    return level


def normal_values(stream_key, dims, spread, reach, pieces=(), held_as=jnp.bfloat16):
    drawn = spread * jax.random.normal(stream_key, dims, jnp.float32)
    if pieces:
        drawn = drawn * levels(stream_key, dims, pieces, -0.22, 0.18)
    return jnp.clip(drawn, -reach, reach).astype(held_as)


def setup_inputs(seed: int = 0) -> dict:
    streams_of = jax.random.split(jax.random.key(seed), 6)
    return {
        "activations": draw_activations(jax.random.fold_in(streams_of[5], 71), 0),
        "out_grads": draw_out_grads(jax.random.fold_in(streams_of[5], 71), 0),
        "weights": normal_values(streams_of[2], (LAYERS, EXPERTS, ROWS, FF), 0.5, 4.0, ((1, 8), (2, 32)), jnp.float32),
        "shadow": normal_values(streams_of[3], (LAYERS, EXPERTS, ROWS, FF), 0.5, 4.0, ((1, 8), (2, 32)), jnp.float32),
        "counts": draw_counts(jax.random.fold_in(streams_of[5], 71), 0),
    }


step_size = 0.5
clip_level = 1.0

def reference(activations, out_grads, weights, shadow, counts):
    totals = lax.optimization_barrier(jnp.sum(counts, axis=1, dtype=jnp.int32))
    all_weights = []
    all_shadow = []
    for layer_index in range(LAYERS):
        loads = totals[layer_index].astype(jnp.float32)
        mean_load = jnp.mean(loads)

        def update_one(item):
            inputs, cotangent, current, smooth, own_load = item
            summed = jnp.dot(inputs.T, cotangent, preferred_element_type=jnp.float32)
            numel = summed.shape[0] * summed.shape[1]
            root_mean = jnp.sqrt(jnp.sum(summed * summed) / numel)
            factor = step_size * (own_load / mean_load) * clip_level / jnp.maximum(root_mean, clip_level)
            updated = current - factor * summed
            beta = own_load / (own_load + mean_load)
            return (updated, smooth + beta * (updated - smooth))
        updated, smoothed = lax.map(update_one, (activations[layer_index], out_grads[layer_index], weights[layer_index], shadow[layer_index], loads))
        all_weights.append(updated)
        all_shadow.append(smoothed)
    return (jnp.stack(all_weights), jnp.stack(all_shadow))
```

```python
import functools

import jax
import jax.numpy as jnp
from jax import lax
from jax.experimental import pallas as pl
from jax.experimental.pallas import tpu as pltpu
from jax.sharding import Mesh
from jax.sharding import PartitionSpec as P

MESH = pl.DeviceIdType.MESH
LAYERS = 2
EXPERT = ("expert_0", "expert_1")
DP_EXPERT_SHARD = ("dp", "expert_0", "expert_1", "shard_0", "shard_1")
DP_SHARD = ("dp", "shard_0", "shard_1")

step_size = 0.5
clip_level = 1.0

NZ = 8
BLOCKS = 8
ZF = 4


def kernel(
    acts, og, counts, grad, factor_out, beta_out,
    part, ring, y_got, y_relay, z_got, z_relay, x_got, x_out, own_half, other_half,
    a_out, a_got, a_rows, a_t, gbuf, c_own, c_got, d_own, d_got, q_own, q_got, q_acc,
    og_sem, x_send, x_recv, a_sem, ring_send, ring_recv, y_sem, z_sem, g_sem, c_sem, d_sem, q_sem, out_sem,
):
    z = lax.axis_index("dp")
    x = lax.axis_index("expert_0")
    y_lo = lax.axis_index("expert_1")
    y_hi = lax.axis_index("shard_0")
    core = lax.axis_index("shard_1")
    y = y_hi * 2 + y_lo
    tokens = acts.shape[1]
    rows = acts.shape[2]
    half_rows = rows // 2
    unit = half_rows // NZ
    width = part.shape[-1]
    own_rows = unit // 2
    half_cols = BLOCKS * width

    def at(z=z, x=x, y_lo=y_lo, y_hi=y_hi, core=core):
        return (z, x, y_lo, y_hi, core)

    def z_next(sign):
        return at(z=lax.rem(z + sign + NZ, NZ))

    def y_next(sign):
        to = lax.rem(y + sign + 4, 4)
        return at(y_lo=lax.rem(to, 2), y_hi=to // 2)

    mate = at(core=1 - core)
    me_group = z * 4 + y_hi * 2 + core
    me_expert = x * 2 + y_lo

    def group_device(offset):
        to = lax.rem(me_group + offset, 32)
        return at(z=to // 4, y_hi=lax.rem(to // 2, 2), core=lax.rem(to, 2))

    def expert_device(offset):
        to = lax.rem(me_expert + offset, 8)
        return at(x=to // 2, y_lo=lax.rem(to, 2))

    def remote(src, dst, send, recv, device):
        return pltpu.make_async_remote_copy(
            src_ref=src, dst_ref=dst, send_sem=send, recv_sem=recv, device_id=device, device_id_type=MESH
        )

    def og_copy(layer, which, b):
        first = core if which == 0 else 1 - core
        to = own_half if which == 0 else other_half
        cols = pl.ds(pl.multiple_of(first * half_cols + b * width, 128), width)
        return pltpu.make_async_copy(og.at[layer, :, cols], to.at[layer, b], og_sem.at[layer, which, b])

    for layer in range(LAYERS):
        def start(b, _):
            og_copy(layer, 1, b).start()
            og_copy(layer, 0, b).start()
            return 0
        lax.fori_loop(0, BLOCKS, start, 0)

    barrier = pltpu.get_barrier_semaphore()

    def greet_group(offset, _):
        pl.semaphore_signal(barrier, inc=1, device_id=group_device(offset), device_id_type=MESH)
        return 0

    def greet_expert(offset, _):
        pl.semaphore_signal(barrier, inc=1, device_id=expert_device(offset), device_id_type=MESH)
        return 0

    lax.fori_loop(1, 32, greet_group, 0)
    lax.fori_loop(1, 8, greet_expert, 0)
    pl.semaphore_signal(barrier, inc=1, device_id=at(y_lo=1 - y_lo, y_hi=1 - y_hi), device_id_type=MESH)

    a_out[...] = acts[...].astype(jnp.float32)
    c_own[...] = jnp.zeros_like(c_own)
    c_own[:, 0:8] = counts[:, 0, :].astype(jnp.float32)
    q_acc[...] = jnp.zeros_like(q_acc)

    def convert(layer, b):
        og_copy(layer, 1, b).wait()
        x_out[b] = other_half[layer, b].astype(jnp.float32)

    def x_copy(layer, b):
        return remote(x_out.at[b], x_got.at[layer, b], x_send.at[b], x_recv.at[layer, b], mate)

    convert(0, 0)
    pl.semaphore_wait(barrier, 39)

    a_copy = remote(a_out, a_got, a_sem.at[0], a_sem.at[1], mate)
    a_copy.start()

    def swap(b, _):
        convert(0, b)
        x_copy(0, b).start()
        return 0

    x_copy(0, 0).start()
    lax.fori_loop(1, BLOCKS, swap, 0)

    def c_copy(offset):
        return remote(c_own, c_got.at[offset - 1], c_sem.at[0, offset - 1], c_sem.at[1, offset - 1], expert_device(offset))

    def each(copy, low, high, what):
        def body(i, _):
            getattr(copy(i), what)()
            return 0
        lax.fori_loop(low, high, body, 0)

    a_copy.wait_recv()
    for layer in range(LAYERS):
        a_rows[:, 0:tokens] = a_out[layer].T
        a_rows[:, tokens : 2 * tokens] = a_got[layer].T
        for half in range(2):
            side = y_hi if half == 0 else 1 - y_hi
            for zz in range(NZ):
                piece = a_rows[pl.ds(pl.multiple_of(zz * 2 * unit + side * unit, unit), unit), :]
                a_t[layer, half * half_rows + zz * unit : half * half_rows + (zz + 1) * unit, :] = piece.astype(jnp.bfloat16)

    def multiply(layer, b):
        x_copy(layer, b).wait_recv()
        og_copy(layer, 0, b).wait()
        both = jnp.concatenate([own_half[layer, b], x_got[layer, b].astype(jnp.bfloat16)], axis=0)
        part[layer, b] = jnp.dot(a_t[layer], both, preferred_element_type=jnp.float32)

    def stream(phase, slot):
        if phase < 2:
            return phase, slot // 2, lax.rem(slot, 2)
        return slot // 4, ZF + lax.rem(slot, 4), 0

    def sign_of(b):
        return 1 - 2 * lax.rem(b, 2)

    def chunk(layer, b, half, index):
        return part.at[layer, b, pl.ds(pl.multiple_of(half * half_rows + index * unit, unit), unit), :]

    def ring_copy(phase, slot, step):
        layer, b, half = stream(phase, slot)
        sign = sign_of(b)
        k = phase * 8 + slot
        if step == 0:
            src = chunk(layer, b, half, lax.rem(z - sign + NZ, NZ))
        else:
            src = ring.at[k, step - 1]
        return remote(src, ring.at[k, step], ring_send.at[k], ring_recv.at[k, step], z_next(sign))

    def ring_step(phase, slot, step):
        layer, b, half = stream(phase, slot)
        k = phase * 8 + slot
        before = ring_copy(phase, slot, step - 1)
        before.wait_recv()
        index = lax.rem(z - sign_of(b) * (1 + step) + 2 * NZ, NZ)
        ring[k, step - 1] = ring[k, step - 1] + chunk(layer, b, half, index)[...]
        before.wait_send()
        ring_copy(phase, slot, step).start()

    def ring_last(phase, slot):
        layer, b, half = stream(phase, slot)
        k = phase * 8 + slot
        before = ring_copy(phase, slot, NZ - 2)
        before.wait_recv()
        before.wait_send()
        return ring[k, NZ - 2] + chunk(layer, b, half, z)[...]

    def round_of(phase, step, low=0, high=8):
        def body(slot, _):
            ring_step(phase, slot, step)
            return 0
        lax.fori_loop(low, high, body, 0)

    def y_copy(layer, j):
        return remote(
            part.at[layer, ZF + j, pl.ds(half_rows, half_rows), :], y_relay.at[layer, j],
            y_sem.at[0, layer, j], y_sem.at[1, layer, j], y_next(sign_of(j)),
        )

    def y_pass(layer, j):
        return remote(
            y_relay.at[layer, j], y_got.at[layer, j], y_sem.at[2, layer, j], y_sem.at[3, layer, j], y_next(sign_of(j))
        )

    def y_forward(layer, low, high):
        def body(j, _):
            y_copy(layer, j).wait_recv()
            y_pass(layer, j).start()
            return 0
        lax.fori_loop(low, high, body, 0)

    def z_copy(layer, j):
        return remote(
            ring.at[layer * 8 + j * 2 + 1, NZ - 2], z_relay.at[layer, j],
            z_sem.at[0, layer, j], z_sem.at[1, layer, j], y_next(sign_of(j)),
        )

    def z_pass(layer, j):
        return remote(
            z_relay.at[layer, j], z_got.at[layer, j], z_sem.at[2, layer, j], z_sem.at[3, layer, j], y_next(sign_of(j))
        )

    def z_forward(layer):
        def body(j, _):
            z_copy(layer, j).wait_recv()
            z_pass(layer, j).start()
            return 0
        lax.fori_loop(0, ZF, body, 0)

    def gcols(side, b):
        return pl.ds(pl.multiple_of(side * half_cols + b * width, 128), width)

    def g_copy(layer, b, k):
        src = ring.at[k, NZ - 2, pl.ds(pl.multiple_of((1 - core) * own_rows, own_rows), own_rows), :]
        return remote(src, gbuf.at[layer, :, gcols(core, b)], g_sem.at[0, layer, b], g_sem.at[1, layer, b], mate)

    def finish(layer, b, k, value):
        ring[k, NZ - 2] = value
        g_copy(layer, b, k).start()
        gbuf[layer, :, gcols(core, b)] = ring[k, NZ - 2, pl.ds(pl.multiple_of(core * own_rows, own_rows), own_rows), :]
        squares = value * value
        folded = squares[0:own_rows] + squares[own_rows : 2 * own_rows]
        total = folded[:, 0:128]
        for i in range(1, width // 128):
            total = total + folded[:, i * 128 : (i + 1) * 128]
        q_acc[layer] = q_acc[layer] + total

    def zf_end(layer):
        def body(j, _):
            slot = j * 2 + 1
            ring[layer * 8 + slot, NZ - 2] = ring_last(layer, slot)
            z_copy(layer, j).start()
            slot = j * 2
            ring[layer * 8 + slot, NZ - 2] = ring_last(layer, slot)
            return 0
        lax.fori_loop(0, ZF, body, 0)

    def zf_finish(layer):
        def body(j, _):
            z_pass(layer, j).wait_recv()
            k = layer * 8 + j * 2
            finish(layer, j, k, ring[k, NZ - 2] + z_got[layer, j])
            return 0
        lax.fori_loop(0, ZF, body, 0)

    def zf_begin(layer):
        def body(b, _):
            multiply(layer, b)
            return 0
        lax.fori_loop(0, ZF, body, 0)

    def zf_start(phase):
        def body(slot, _):
            ring_copy(phase, slot, 0).start()
            return 0
        lax.fori_loop(0, 8, body, 0)

    def first(b, _):
        multiply(0, b)
        ring_copy(0, b * 2, 0).start()
        ring_copy(0, b * 2 + 1, 0).start()
        return 0

    lax.fori_loop(0, ZF, first, 0)

    def second(j, _):
        multiply(0, ZF + j)
        y_copy(0, j).start()
        return 0

    lax.fori_loop(0, BLOCKS - ZF, second, 0)
    each(c_copy, 1, 8, "start")

    def swap_again(b, _):
        x_copy(0, b).wait_send()
        convert(1, b)
        x_copy(1, b).start()
        return 0

    lax.fori_loop(0, BLOCKS, swap_again, 0)
    round_of(0, 1)

    def more(b, _):
        multiply(1, b)
        return 0

    lax.fori_loop(0, ZF, more, 0)
    round_of(0, 2)
    lax.fori_loop(ZF, BLOCKS, more, 0)
    round_of(0, 3)
    y_forward(0, 0, 2)

    each(c_copy, 1, 8, "wait_recv")
    d_own[...] = c_own[...] + jnp.sum(c_got[...], axis=0)

    def d_copy(offset):
        return remote(d_own, d_got.at[offset - 1], d_sem.at[0, offset - 1], d_sem.at[1, offset - 1], group_device(offset))

    each(d_copy, 1, 32, "start")
    round_of(0, 4)
    round_of(0, 5)
    y_forward(0, 2, 4)
    each(lambda j: y_copy(1, j), 0, 4, "start")
    round_of(0, 6)

    zf_start(1)
    zf_end(0)
    round_of(1, 1)
    round_of(1, 2)
    round_of(1, 3)
    round_of(1, 4)
    y_forward(1, 0, 2)
    round_of(1, 5)
    z_forward(0)
    round_of(1, 6)
    y_forward(1, 2, 4)

    def yf_start(slot, _):
        layer, b, half = stream(2, slot)
        y_pass(layer, b - ZF).wait_recv()
        part[layer, b, 0:half_rows, :] = part[layer, b, 0:half_rows, :] + y_got[layer, b - ZF]
        ring_copy(2, slot, 0).start()
        return 0

    lax.fori_loop(0, 4, yf_start, 0)
    zf_end(1)
    lax.fori_loop(4, 6, yf_start, 0)
    zf_finish(0)
    round_of(2, 1, 0, 6)
    z_forward(1)
    lax.fori_loop(6, 8, yf_start, 0)
    for step in range(2, 7):
        round_of(2, step, 0, 6)
        round_of(2, step - 1, 6, 8)
    zf_finish(1)

    def yf_end(slot, _):
        layer, b, half = stream(2, slot)
        finish(layer, b, 16 + slot, ring_last(2, slot))
        return 0

    lax.fori_loop(0, 6, yf_end, 0)
    round_of(2, 6, 6, 8)
    lax.fori_loop(6, 8, yf_end, 0)

    q_own[...] = jnp.sum(q_acc[...], axis=1)

    def q_copy(offset):
        return remote(q_own, q_got.at[offset - 1], q_sem.at[0, offset - 1], q_sem.at[1, offset - 1], group_device(offset))

    each(q_copy, 1, 32, "start")

    each(d_copy, 1, 32, "wait_recv")
    totals = d_own[...] + jnp.sum(d_got[...], axis=0)
    lanes = lax.broadcasted_iota(jnp.int32, totals.shape, 1)
    mean_load = jnp.sum(totals, axis=1, keepdims=True) / 8.0
    own_load = jnp.sum(jnp.where(lanes == me_expert, totals, 0.0), axis=1, keepdims=True)
    beta = own_load / (own_load + mean_load)
    beta_out[...] = jnp.broadcast_to(beta, beta_out.shape)

    for layer in range(LAYERS):
        def land(b, _):
            g_copy(layer, b, 0).wait_recv()
            return 0
        lax.fori_loop(0, BLOCKS, land, 0)
    out_copy = pltpu.make_async_copy(gbuf, grad, out_sem)
    out_copy.start()

    def sent(layer):
        def body(j, _):
            y_copy(layer, j).wait_send()
            y_pass(layer, j).wait_send()
            z_copy(layer, j).wait_send()
            z_pass(layer, j).wait_send()
            return 0
        lax.fori_loop(0, 4, body, 0)

        def body_g(b, _):
            g_copy(layer, b, 0).wait_send()
            return 0
        lax.fori_loop(0, BLOCKS, body_g, 0)

    sent(0)
    sent(1)
    each(lambda b: x_copy(1, b), 0, BLOCKS, "wait_send")
    a_copy.wait_send()
    each(c_copy, 1, 8, "wait_send")
    each(d_copy, 1, 32, "wait_send")

    each(q_copy, 1, 32, "wait_recv")
    total = jnp.sum(q_own[...] + jnp.sum(q_got[...], axis=0), axis=1, keepdims=True)
    root_mean = jnp.sqrt(total / float(rows * 2 * half_cols))
    factor = step_size * (own_load / mean_load) * clip_level / jnp.maximum(root_mean, clip_level)
    factor_out[...] = jnp.broadcast_to(factor, factor_out.shape)
    each(q_copy, 1, 32, "wait_send")
    out_copy.wait()


def on_device(activations, out_grads, weights, shadow, counts):
    acts, og, counts = activations[:, 0], out_grads[:, 0], counts
    tokens, rows = acts.shape[1:]
    ff = og.shape[2]
    width = ff // 2 // BLOCKS
    unit = rows // 2 // NZ
    f32 = jnp.float32
    dma = pltpu.SemaphoreType.DMA
    vmem = pl.BlockSpec(memory_space=pltpu.VMEM)
    hbm = pl.BlockSpec(memory_space=pl.ANY)
    half = rows // 2
    grad, factor, beta = pl.pallas_call(
        kernel,
        out_shape=(
            jax.ShapeDtypeStruct((LAYERS, unit // 2, ff), f32),
            jax.ShapeDtypeStruct((LAYERS, 128), f32),
            jax.ShapeDtypeStruct((LAYERS, 128), f32),
        ),
        in_specs=[vmem, hbm, vmem],
        out_specs=(hbm, vmem, vmem),
        scratch_shapes=[
            pltpu.VMEM((LAYERS, BLOCKS, rows, width), f32),
            pltpu.VMEM((24, NZ - 1, unit, width), f32),
            pltpu.VMEM((LAYERS, BLOCKS - ZF, half, width), f32),
            pltpu.VMEM((LAYERS, BLOCKS - ZF, half, width), f32),
            pltpu.VMEM((LAYERS, ZF, unit, width), f32),
            pltpu.VMEM((LAYERS, ZF, unit, width), f32),
            pltpu.VMEM((LAYERS, BLOCKS, tokens, width), f32),
            pltpu.VMEM((BLOCKS, tokens, width), f32),
            pltpu.VMEM((LAYERS, BLOCKS, tokens, width), jnp.bfloat16),
            pltpu.VMEM((LAYERS, BLOCKS, tokens, width), jnp.bfloat16),
            pltpu.VMEM((LAYERS, tokens, rows), f32),
            pltpu.VMEM((LAYERS, tokens, rows), f32),
            pltpu.VMEM((rows, 2 * tokens), f32),
            pltpu.VMEM((LAYERS, rows, 2 * tokens), jnp.bfloat16),
            pltpu.VMEM((LAYERS, unit // 2, ff), f32),
            pltpu.VMEM((LAYERS, 128), f32),
            pltpu.VMEM((7, LAYERS, 128), f32),
            pltpu.VMEM((LAYERS, 128), f32),
            pltpu.VMEM((31, LAYERS, 128), f32),
            pltpu.VMEM((LAYERS, 128), f32),
            pltpu.VMEM((31, LAYERS, 128), f32),
            pltpu.VMEM((LAYERS, unit // 2, 128), f32),
            dma((LAYERS, 2, BLOCKS)),
            dma((BLOCKS,)),
            dma((LAYERS, BLOCKS)),
            dma((2,)),
            dma((24,)),
            dma((24, NZ - 1)),
            dma((4, LAYERS, BLOCKS - ZF)),
            dma((4, LAYERS, ZF)),
            dma((2, LAYERS, BLOCKS)),
            dma((2, 7)),
            dma((2, 31)),
            dma((2, 31)),
            dma,
        ],
        compiler_params=pltpu.CompilerParams(
            collective_id=0, has_side_effects=True, vmem_limit_bytes=62 * 1024 * 1024
        ),
    )(acts, og, counts)
    summed = grad[:, None]
    factor = factor[:, None, None, :1]
    beta = beta[:, None, None, :1]
    updated = weights - factor * summed
    return updated, shadow + beta * (updated - shadow)


def solution(mesh):
    split = Mesh(
        mesh.devices.reshape(mesh.shape["dp"], 4, 2, 2, 2),
        ("dp", "expert_0", "expert_1", "shard_0", "shard_1"),
    )
    return jax.shard_map(
        on_device,
        mesh=split,
        in_specs=(
            P(None, EXPERT, DP_SHARD, None),
            P(None, EXPERT, DP_SHARD, None),
            P(None, EXPERT, DP_SHARD, None),
            P(None, EXPERT, DP_SHARD, None),
            P(None, DP_EXPERT_SHARD, None),
        ),
        out_specs=(P(None, EXPERT, DP_SHARD, None), P(None, EXPERT, DP_SHARD, None)),
        check_vma=False,
    )
```

```python
import functools

import jax
import jax.numpy as jnp
from jax import lax
from jax.experimental import pallas as pl
from jax.experimental.pallas import tpu as pltpu
from jax.sharding import Mesh
from jax.sharding import PartitionSpec as P

MESH = pl.DeviceIdType.MESH
LAYERS = 2
EXPERT = ("expert_0", "expert_1")
DP_EXPERT_SHARD = ("dp", "expert_0", "expert_1", "shard_0", "shard_1")
DP_SHARD = ("dp", "shard_0", "shard_1")

step_size = 0.5
clip_level = 1.0

NZ = 8
BLOCKS = 8
ZF = 4


def kernel(
    acts, og, counts, grad, factor_out, beta_out,
    part, ring, y_got, y_relay, z_got, z_relay, x_got, x_out, own_half, other_half,
    a_out, a_got, a_rows, a_t, gbuf, c_own, c_got, d_own, d_got, q_own, q_got, q_acc,
    og_sem, x_send, x_recv, a_sem, ring_send, ring_recv, y_sem, z_sem, g_sem, c_sem, d_sem, q_sem, out_sem,
):
    z = lax.axis_index("dp")
    x = lax.axis_index("expert_0")
    y_lo = lax.axis_index("expert_1")
    y_hi = lax.axis_index("shard_0")
    core = lax.axis_index("shard_1")
    y = y_hi * 2 + y_lo
    tokens = acts.shape[1]
    rows = acts.shape[2]
    half_rows = rows // 2
    unit = half_rows // NZ
    width = part.shape[-1]
    own_rows = unit // 2
    half_cols = BLOCKS * width

    def at(z=z, x=x, y_lo=y_lo, y_hi=y_hi, core=core):
        return (z, x, y_lo, y_hi, core)

    def z_next(sign):
        return at(z=lax.rem(z + sign + NZ, NZ))

    def y_next(sign):
        to = lax.rem(y + sign + 4, 4)
        return at(y_lo=lax.rem(to, 2), y_hi=to // 2)

    mate = at(core=1 - core)
    me_group = z * 4 + y_hi * 2 + core
    me_expert = x * 2 + y_lo

    def group_device(offset):
        to = lax.rem(me_group + offset, 32)
        return at(z=to // 4, y_hi=lax.rem(to // 2, 2), core=lax.rem(to, 2))

    def expert_device(offset):
        to = lax.rem(me_expert + offset, 8)
        return at(x=to // 2, y_lo=lax.rem(to, 2))

    def remote(src, dst, send, recv, device):
        return pltpu.make_async_remote_copy(
            src_ref=src, dst_ref=dst, send_sem=send, recv_sem=recv, device_id=device, device_id_type=MESH
        )

    def og_copy(layer, which, b):
        first = core if which == 0 else 1 - core
        to = own_half if which == 0 else other_half
        cols = pl.ds(pl.multiple_of(first * half_cols + b * width, 128), width)
        return pltpu.make_async_copy(og.at[layer, :, cols], to.at[layer, b], og_sem.at[layer, which, b])

    for layer in range(LAYERS):
        def start(b, _):
            og_copy(layer, 1, b).start()
            og_copy(layer, 0, b).start()
            return 0
        lax.fori_loop(0, BLOCKS, start, 0)

    barrier = pltpu.get_barrier_semaphore()

    def greet_group(offset, _):
        pl.semaphore_signal(barrier, inc=1, device_id=group_device(offset), device_id_type=MESH)
        return 0

    def greet_expert(offset, _):
        pl.semaphore_signal(barrier, inc=1, device_id=expert_device(offset), device_id_type=MESH)
        return 0

    lax.fori_loop(1, 32, greet_group, 0)
    lax.fori_loop(1, 8, greet_expert, 0)
    pl.semaphore_signal(barrier, inc=1, device_id=at(y_lo=1 - y_lo, y_hi=1 - y_hi), device_id_type=MESH)

    a_out[...] = acts[...].astype(jnp.float32)
    c_own[...] = jnp.zeros_like(c_own)
    c_own[:, 0:8] = counts[:, 0, :].astype(jnp.float32)
    q_acc[...] = jnp.zeros_like(q_acc)

    def convert(layer, b):
        og_copy(layer, 1, b).wait()
        x_out[b] = other_half[layer, b].astype(jnp.float32)

    def x_copy(layer, b):
        return remote(x_out.at[b], x_got.at[layer, b], x_send.at[b], x_recv.at[layer, b], mate)

    convert(0, 0)
    pl.semaphore_wait(barrier, 39)

    a_copy = remote(a_out, a_got, a_sem.at[0], a_sem.at[1], mate)
    a_copy.start()

    def swap(b, _):
        convert(0, b)
        x_copy(0, b).start()
        return 0

    def c_copy(offset):
        return remote(c_own, c_got.at[offset - 1], c_sem.at[0, offset - 1], c_sem.at[1, offset - 1], expert_device(offset))

    def each(copy, low, high, what):
        def body(i, _):
            getattr(copy(i), what)()
            return 0
        lax.fori_loop(low, high, body, 0)

    x_copy(0, 0).start()
    lax.fori_loop(1, BLOCKS, swap, 0)
    each(c_copy, 1, 8, "start")

    a_copy.wait_recv()
    for layer in range(LAYERS):
        a_rows[:, 0:tokens] = a_out[layer].T
        a_rows[:, tokens : 2 * tokens] = a_got[layer].T
        for half in range(2):
            side = y_hi if half == 0 else 1 - y_hi
            for zz in range(NZ):
                piece = a_rows[pl.ds(pl.multiple_of(zz * 2 * unit + side * unit, unit), unit), :]
                a_t[layer, half * half_rows + zz * unit : half * half_rows + (zz + 1) * unit, :] = piece.astype(jnp.bfloat16)

    def multiply(layer, b):
        x_copy(layer, b).wait_recv()
        og_copy(layer, 0, b).wait()
        both = jnp.concatenate([own_half[layer, b], x_got[layer, b].astype(jnp.bfloat16)], axis=0)
        part[layer, b] = jnp.dot(a_t[layer], both, preferred_element_type=jnp.float32)

    def sign_of(slot):
        return 1 - 2 * lax.rem(slot, 2)

    def block_of(k):
        if isinstance(k, tuple):
            layer, slot = k
            return layer, slot // 4 * 4 + lax.rem(slot, 2), lax.rem(slot // 2, 2), layer * 8 + slot
        return k // 4, lax.rem(k, 4) // 2 * 4 + 2 + lax.rem(k, 2), 0, 16 + k

    def parity(k):
        return sign_of(k[1] if isinstance(k, tuple) else k)

    def chunk(layer, b, half, index):
        return part.at[layer, b, pl.ds(pl.multiple_of(half * half_rows + index * unit, unit), unit), :]

    def ring_copy(stream, step):
        layer, b, half, k = block_of(stream)
        sign = parity(stream)
        if step == 0:
            src = chunk(layer, b, half, lax.rem(z - sign + NZ, NZ))
        else:
            src = ring.at[k, step - 1]
        return remote(src, ring.at[k, step], ring_send.at[k], ring_recv.at[k, step], z_next(sign))

    def ring_step(stream, step):
        layer, b, half, k = block_of(stream)
        before = ring_copy(stream, step - 1)
        before.wait_recv()
        index = lax.rem(z - parity(stream) * (1 + step) + 2 * NZ, NZ)
        ring[k, step - 1] = ring[k, step - 1] + chunk(layer, b, half, index)[...]
        before.wait_send()
        ring_copy(stream, step).start()

    def ring_last(stream):
        layer, b, half, k = block_of(stream)
        before = ring_copy(stream, NZ - 2)
        before.wait_recv()
        before.wait_send()
        return ring[k, NZ - 2] + chunk(layer, b, half, z)[...]

    def loop(low, high, act):
        def body(i, _):
            act(i)
            return 0
        lax.fori_loop(low, high, body, 0)

    def z_steps(layer, low, high, step):
        loop(low, high, lambda slot: ring_step((layer, slot), step))

    def y_steps(low, high, step):
        loop(low, high, lambda slot: ring_step(slot, step))

    def z_start(layer, low, high):
        loop(low, high, lambda slot: ring_copy((layer, slot), 0).start())

    def z_end(layer, low, high):
        def act(slot):
            ring[layer * 8 + slot, NZ - 2] = ring_last((layer, slot))
        loop(low, high, act)

    def y_copy(layer, j):
        b = j // 2 * 4 + 2 + lax.rem(j, 2)
        return remote(
            part.at[layer, b, pl.ds(half_rows, half_rows), :], y_relay.at[layer, j],
            y_sem.at[0, layer, j], y_sem.at[1, layer, j], y_next(sign_of(j)),
        )

    def y_pass(layer, j):
        return remote(
            y_relay.at[layer, j], y_got.at[layer, j], y_sem.at[2, layer, j], y_sem.at[3, layer, j], y_next(sign_of(j))
        )

    def y_forward(layer, low, high):
        def act(j):
            y_copy(layer, j).wait_recv()
            y_pass(layer, j).start()
        loop(low, high, act)

    def y_start(low, high):
        def act(slot):
            layer, b, _, _ = block_of(slot)
            j = lax.rem(slot, 4)
            y_pass(layer, j).wait_recv()
            part[layer, b, 0:half_rows, :] = part[layer, b, 0:half_rows, :] + y_got[layer, j]
            ring_copy(slot, 0).start()
        loop(low, high, act)

    def z_copy(layer, j):
        return remote(
            ring.at[layer * 8 + j // 2 * 4 + 2 + lax.rem(j, 2), NZ - 2], z_relay.at[layer, j],
            z_sem.at[0, layer, j], z_sem.at[1, layer, j], y_next(sign_of(j)),
        )

    def z_pass(layer, j):
        return remote(
            z_relay.at[layer, j], z_got.at[layer, j], z_sem.at[2, layer, j], z_sem.at[3, layer, j], y_next(sign_of(j))
        )

    def z_forward(layer):
        def act(j):
            z_copy(layer, j).wait_recv()
            z_pass(layer, j).start()
        loop(0, ZF, act)

    def gcols(side, b):
        return pl.ds(pl.multiple_of(side * half_cols + b * width, 128), width)

    def g_copy(layer, b, k):
        src = ring.at[k, NZ - 2, pl.ds(pl.multiple_of((1 - core) * own_rows, own_rows), own_rows), :]
        return remote(src, gbuf.at[layer, :, gcols(core, b)], g_sem.at[0, layer, b], g_sem.at[1, layer, b], mate)

    def finish(layer, b, k, value):
        ring[k, NZ - 2] = value
        g_copy(layer, b, k).start()
        gbuf[layer, :, gcols(core, b)] = ring[k, NZ - 2, pl.ds(pl.multiple_of(core * own_rows, own_rows), own_rows), :]
        squares = value * value
        folded = squares[0:own_rows] + squares[own_rows : 2 * own_rows]
        total = folded[:, 0:128]
        for i in range(1, width // 128):
            total = total + folded[:, i * 128 : (i + 1) * 128]
        q_acc[layer] = q_acc[layer] + total

    def z_finish(layer):
        def act(j):
            z_pass(layer, j).wait_recv()
            k = layer * 8 + j // 2 * 4 + lax.rem(j, 2)
            finish(layer, j // 2 * 4 + lax.rem(j, 2), k, ring[k, NZ - 2] + z_got[layer, j])
        loop(0, ZF, act)

    def y_finish(low, high):
        def act(slot):
            layer, b, _, k = block_of(slot)
            finish(layer, b, k, ring_last(slot))
        loop(low, high, act)

    def d_copy(offset):
        return remote(d_own, d_got.at[offset - 1], d_sem.at[0, offset - 1], d_sem.at[1, offset - 1], group_device(offset))

    def q_copy(offset):
        return remote(q_own, q_got.at[offset - 1], q_sem.at[0, offset - 1], q_sem.at[1, offset - 1], group_device(offset))

    for pair in range(2):
        def first(odd):
            multiply(0, pair * 4 + odd)
            ring_copy((0, pair * 4 + odd), 0).start()
            ring_copy((0, pair * 4 + 2 + odd), 0).start()

        loop(0, 2, first)

        def second(odd):
            multiply(0, pair * 4 + 2 + odd)
            y_copy(0, pair * 2 + odd).start()

        loop(0, 2, second)

    def swap_again(b):
        x_copy(0, b).wait_send()
        convert(1, b)
        x_copy(1, b).start()

    loop(0, BLOCKS, swap_again)
    z_steps(0, 0, 8, 1)
    loop(0, 2, lambda b: multiply(1, b))
    z_start(1, 0, 2)
    z_steps(0, 0, 8, 2)
    z_steps(1, 0, 2, 1)
    y_forward(0, 0, 2)
    loop(2, BLOCKS, lambda b: multiply(1, b))
    z_steps(0, 0, 8, 3)
    z_steps(1, 0, 2, 2)
    z_steps(0, 0, 8, 4)
    z_steps(1, 0, 2, 3)
    y_forward(0, 2, 4)
    each(lambda j: y_copy(1, j), 0, 4, "start")
    each(c_copy, 1, 8, "wait_recv")
    d_own[...] = c_own[...] + jnp.sum(c_got[...], axis=0)
    each(d_copy, 1, 32, "start")
    z_steps(0, 0, 8, 5)
    z_steps(1, 0, 2, 4)
    z_steps(0, 0, 8, 6)
    z_steps(1, 0, 2, 5)

    z_start(1, 2, 8)
    y_start(0, 2)
    z_end(0, 0, 8)
    z_steps(1, 0, 2, 6)
    z_steps(1, 2, 8, 1)
    y_steps(0, 2, 1)
    z_end(1, 0, 2)
    z_steps(1, 2, 8, 2)
    y_steps(0, 2, 2)
    y_forward(1, 0, 2)
    z_steps(1, 2, 8, 3)
    y_steps(0, 2, 3)
    z_steps(1, 2, 8, 4)
    y_steps(0, 2, 4)
    y_forward(1, 2, 4)
    each(lambda j: z_copy(0, j), 0, 4, "start")
    z_steps(1, 2, 8, 5)
    y_steps(0, 2, 5)
    z_steps(1, 2, 8, 6)
    y_steps(0, 2, 6)

    y_start(2, 6)
    z_end(1, 2, 8)
    each(lambda j: z_copy(1, j), 0, 4, "start")
    y_finish(0, 2)
    y_start(6, 8)
    y_steps(2, 8, 1)
    y_steps(2, 8, 2)
    z_forward(0)
    z_forward(1)
    y_steps(2, 8, 3)
    y_steps(2, 8, 4)
    z_finish(0)
    y_steps(2, 8, 5)
    z_finish(1)
    y_steps(2, 8, 6)
    y_finish(2, 8)

    q_own[...] = jnp.sum(q_acc[...], axis=1)

    def far_first(i):
        m = i // 4
        q_copy((4 + m // 2 - lax.rem(m, 2) * (2 * (m // 2) + 1)) * 4 + lax.rem(i, 4)).start()

    loop(0, 28, far_first)
    each(q_copy, 1, 4, "start")

    each(d_copy, 1, 32, "wait_recv")
    totals = d_own[...] + jnp.sum(d_got[...], axis=0)
    lanes = lax.broadcasted_iota(jnp.int32, totals.shape, 1)
    mean_load = jnp.sum(totals, axis=1, keepdims=True) / 8.0
    own_load = jnp.sum(jnp.where(lanes == me_expert, totals, 0.0), axis=1, keepdims=True)
    beta = own_load / (own_load + mean_load)

    for layer in range(LAYERS):
        loop(0, BLOCKS, lambda b: g_copy(layer, b, 0).wait_recv())
    out_copy = pltpu.make_async_copy(gbuf, grad, out_sem)
    out_copy.start()

    for layer in range(LAYERS):
        def sent(j):
            y_copy(layer, j).wait_send()
            y_pass(layer, j).wait_send()
            z_copy(layer, j).wait_send()
            z_pass(layer, j).wait_send()

        loop(0, 4, sent)
        loop(0, BLOCKS, lambda b: g_copy(layer, b, 0).wait_send())

    each(lambda b: x_copy(1, b), 0, BLOCKS, "wait_send")
    a_copy.wait_send()
    each(c_copy, 1, 8, "wait_send")
    each(d_copy, 1, 32, "wait_send")
    each(q_copy, 1, 32, "wait_send")

    each(q_copy, 1, 32, "wait_recv")
    total = jnp.sum(q_own[...] + jnp.sum(q_got[...], axis=0), axis=1, keepdims=True)
    root_mean = jnp.sqrt(total / float(rows * 2 * half_cols))
    factor = step_size * (own_load / mean_load) * clip_level / jnp.maximum(root_mean, clip_level)
    for layer in range(LAYERS):
        factor_out[layer] = factor[layer, 0]
        beta_out[layer] = beta[layer, 0]
    out_copy.wait()


def on_device(activations, out_grads, weights, shadow, counts):
    acts, og, counts = activations[:, 0], out_grads[:, 0], counts
    tokens, rows = acts.shape[1:]
    ff = og.shape[2]
    width = ff // 2 // BLOCKS
    unit = rows // 2 // NZ
    f32 = jnp.float32
    dma = pltpu.SemaphoreType.DMA
    vmem = pl.BlockSpec(memory_space=pltpu.VMEM)
    smem = pl.BlockSpec(memory_space=pltpu.SMEM)
    hbm = pl.BlockSpec(memory_space=pl.ANY)
    half = rows // 2
    grad, factor, beta = pl.pallas_call(
        kernel,
        out_shape=(
            jax.ShapeDtypeStruct((LAYERS, unit // 2, ff), f32),
            jax.ShapeDtypeStruct((LAYERS,), f32),
            jax.ShapeDtypeStruct((LAYERS,), f32),
        ),
        in_specs=[vmem, hbm, vmem],
        out_specs=(hbm, smem, smem),
        scratch_shapes=[
            pltpu.VMEM((LAYERS, BLOCKS, rows, width), f32),
            pltpu.VMEM((24, NZ - 1, unit, width), f32),
            pltpu.VMEM((LAYERS, BLOCKS - ZF, half, width), f32),
            pltpu.VMEM((LAYERS, BLOCKS - ZF, half, width), f32),
            pltpu.VMEM((LAYERS, ZF, unit, width), f32),
            pltpu.VMEM((LAYERS, ZF, unit, width), f32),
            pltpu.VMEM((LAYERS, BLOCKS, tokens, width), f32),
            pltpu.VMEM((BLOCKS, tokens, width), f32),
            pltpu.VMEM((LAYERS, BLOCKS, tokens, width), jnp.bfloat16),
            pltpu.VMEM((LAYERS, BLOCKS, tokens, width), jnp.bfloat16),
            pltpu.VMEM((LAYERS, tokens, rows), f32),
            pltpu.VMEM((LAYERS, tokens, rows), f32),
            pltpu.VMEM((rows, 2 * tokens), f32),
            pltpu.VMEM((LAYERS, rows, 2 * tokens), jnp.bfloat16),
            pltpu.VMEM((LAYERS, unit // 2, ff), f32),
            pltpu.VMEM((LAYERS, 128), f32),
            pltpu.VMEM((7, LAYERS, 128), f32),
            pltpu.VMEM((LAYERS, 128), f32),
            pltpu.VMEM((31, LAYERS, 128), f32),
            pltpu.VMEM((LAYERS, 128), f32),
            pltpu.VMEM((31, LAYERS, 128), f32),
            pltpu.VMEM((LAYERS, unit // 2, 128), f32),
            dma((LAYERS, 2, BLOCKS)),
            dma((BLOCKS,)),
            dma((LAYERS, BLOCKS)),
            dma((2,)),
            dma((24,)),
            dma((24, NZ - 1)),
            dma((4, LAYERS, BLOCKS - ZF)),
            dma((4, LAYERS, ZF)),
            dma((2, LAYERS, BLOCKS)),
            dma((2, 7)),
            dma((2, 31)),
            dma((2, 31)),
            dma,
        ],
        compiler_params=pltpu.CompilerParams(
            collective_id=0, has_side_effects=True, vmem_limit_bytes=62 * 1024 * 1024
        ),
    )(acts, og, counts)
    summed = grad[:, None]
    factor = factor[:, None, None, None]
    beta = beta[:, None, None, None]
    updated = weights - factor * summed
    return updated, shadow + beta * (updated - shadow)


def solution(mesh):
    split = Mesh(
        mesh.devices.reshape(mesh.shape["dp"], 4, 2, 2, 2),
        ("dp", "expert_0", "expert_1", "shard_0", "shard_1"),
    )
    return jax.shard_map(
        on_device,
        mesh=split,
        in_specs=(
            P(None, EXPERT, DP_SHARD, None),
            P(None, EXPERT, DP_SHARD, None),
            P(None, EXPERT, DP_SHARD, None),
            P(None, EXPERT, DP_SHARD, None),
            P(None, DP_EXPERT_SHARD, None),
        ),
        out_specs=(P(None, EXPERT, DP_SHARD, None), P(None, EXPERT, DP_SHARD, None)),
        check_vma=False,
    )
```

```python
import jax
import jax.numpy as jnp
from jax import lax
from jax.experimental import pallas as pl
from jax.experimental.pallas import tpu as pltpu
from jax.sharding import Mesh
from jax.sharding import PartitionSpec as P

MESH = pl.DeviceIdType.MESH
LAYERS = 2
EXPERT = ("expert_0", "expert_1")
DP_EXPERT_SHARD = ("dp", "expert_0", "expert_1", "shard_0", "shard_1")
DP_SHARD = ("dp", "shard_0", "shard_1")

step_size = 0.5
clip_level = 1.0

NZ = 8
BLOCKS = 4
Z, Y = 0, 1


def kernel(
    acts, og, counts, grad, factor_out, beta_out,
    part_z, part_y, ring_z, ring_y, y_got, y_relay, z_got, z_relay, x_got_z, x_got_y, x_out_z, x_out_y,
    own_half, other_half, a_out, a_got, a_rows, a_t, gbuf, c_own, c_got, d_own, d_got, q_own, q_got, q_acc,
    og_sem, x_send, x_recv, x_recv_late, a_sem, ring_send, ring_recv,
    y_send, y_mid, y_end, y_units, z_send, z_mid, z_end_sem, g_sem, c_sem, d_sem, q_sem, out_sem,
):
    z = lax.axis_index("dp")
    x = lax.axis_index("expert_0")
    y_lo = lax.axis_index("expert_1")
    y_hi = lax.axis_index("shard_0")
    core = lax.axis_index("shard_1")
    y = y_hi * 2 + y_lo
    tokens = acts.shape[1]
    rows = acts.shape[2]
    half_rows = rows // 2
    unit = half_rows // NZ
    own_rows = unit // 2
    part = (part_z, part_y)
    ring = (ring_z, ring_y)
    x_got = (x_got_z, x_got_y)
    x_out = (x_out_z, x_out_y)
    width = (part_z.shape[-1], part_y.shape[-1])
    first_col = (0, BLOCKS * width[Z])
    half_cols = BLOCKS * (width[Z] + width[Y])

    def at(z=z, x=x, y_lo=y_lo, y_hi=y_hi, core=core):
        return (z, x, y_lo, y_hi, core)

    def z_next(sign):
        return at(z=lax.rem(z + sign + NZ, NZ))

    def y_next(sign):
        to = lax.rem(y + sign + 4, 4)
        return at(y_lo=lax.rem(to, 2), y_hi=to // 2)

    mate = at(core=1 - core)
    me_group = z * 4 + y_hi * 2 + core
    me_expert = x * 2 + y_lo

    def group_device(offset):
        to = lax.rem(me_group + offset, 32)
        return at(z=to // 4, y_hi=lax.rem(to // 2, 2), core=lax.rem(to, 2))

    def expert_device(offset):
        to = lax.rem(me_expert + offset, 8)
        return at(x=to // 2, y_lo=lax.rem(to, 2))

    def remote(src, dst, send, recv, device):
        return pltpu.make_async_remote_copy(
            src_ref=src, dst_ref=dst, send_sem=send, recv_sem=recv, device_id=device, device_id_type=MESH
        )

    def loop(low, high, act):
        def body(i, _):
            act(i)
            return 0
        lax.fori_loop(low, high, body, 0)

    def og_copy(layer, which, kind):
        first = core if which == 0 else 1 - core
        to = own_half if which == 0 else other_half
        size = BLOCKS * width[kind]
        cols = pl.ds(pl.multiple_of(first * half_cols + first_col[kind], 128), size)
        return pltpu.make_async_copy(
            og.at[layer, :, cols], to.at[layer, :, first_col[kind] : first_col[kind] + size], og_sem.at[layer, which, kind]
        )

    for layer in range(LAYERS):
        for which, kind in ((1, Y), (0, Y), (1, Z), (0, Z)):
            og_copy(layer, which, kind).start()

    barrier = pltpu.get_barrier_semaphore()

    def greet(device):
        pl.semaphore_signal(barrier, inc=1, device_id=device, device_id_type=MESH)

    loop(1, 32, lambda offset: greet(group_device(offset)))
    loop(1, 8, lambda offset: greet(expert_device(offset)))
    greet(at(y_lo=1 - y_lo, y_hi=1 - y_hi))

    def cols_of(kind, j):
        return pl.ds(pl.multiple_of(first_col[kind] + j * width[kind], 128), width[kind])

    def convert(layer, kind, j):
        x_out[kind][j] = other_half[layer, :, cols_of(kind, j)].astype(jnp.float32)

    def x_copy(layer, kind, j):
        sem = x_recv.at[kind, j] if layer == 0 else x_recv_late.at[kind]
        return remote(x_out[kind].at[j], x_got[kind].at[layer, j], x_send.at[kind], sem, mate)

    def x_all(layer, kind):
        return remote(x_out[kind], x_got[kind].at[layer], x_send.at[kind], x_recv_late.at[kind], mate)

    a_out[...] = acts[...].astype(jnp.float32)
    c_own[...] = jnp.zeros_like(c_own)
    c_own[:, 0:8] = counts[:, 0, :].astype(jnp.float32)
    q_acc[...] = jnp.zeros_like(q_acc)
    og_copy(0, 1, Y).wait()
    loop(0, 2, lambda j: convert(0, Y, j))
    pl.semaphore_wait(barrier, 39)

    a_copy = remote(a_out, a_got, a_sem.at[0], a_sem.at[1], mate)
    a_copy.start()

    def swap(layer, kind, low, high):
        def act(j):
            convert(layer, kind, j)
            x_copy(layer, kind, j).start()
        loop(low, high, act)

    loop(0, 2, lambda j: x_copy(0, Y, j).start())
    og_copy(0, 1, Z).wait()
    swap(0, Z, 0, 4)
    swap(0, Y, 2, 4)

    def c_copy(offset):
        return remote(c_own, c_got.at[offset - 1], c_sem.at[0], c_sem.at[1], expert_device(offset))

    loop(1, 8, lambda offset: c_copy(offset).start())

    a_copy.wait_recv()
    for layer in range(LAYERS):
        a_rows[:, 0:tokens] = a_out[layer].T
        a_rows[:, tokens : 2 * tokens] = a_got[layer].T
        for half in range(2):
            side = y_hi if half == 0 else 1 - y_hi
            for zz in range(NZ):
                piece = a_rows[pl.ds(pl.multiple_of(zz * 2 * unit + side * unit, unit), unit), :]
                a_t[layer, half * half_rows + zz * unit : half * half_rows + (zz + 1) * unit, :] = piece.astype(jnp.bfloat16)

    def multiply(layer, kind, j):
        if layer == 0:
            x_copy(layer, kind, j).wait_recv()
        theirs = x_got[kind][layer, j].astype(jnp.bfloat16)
        both = jnp.concatenate([own_half[layer, :, cols_of(kind, j)], theirs], axis=0)
        part[kind][layer, j] = jnp.dot(a_t[layer], both, preferred_element_type=jnp.float32)

    def stream(kind, layer, slot):
        if kind == Z:
            return slot // 2, lax.rem(slot, 2), layer * 8 + slot, layer * 8 + slot
        return slot, 0, layer * 4 + slot, layer * 4 + slot

    def sign_of(slot):
        return 1 - 2 * lax.rem(slot, 2)

    def chunk(kind, layer, j, half, away):
        index = lax.rem(z + away + NZ, NZ)
        return part[kind].at[layer, j, pl.ds(pl.multiple_of(half * half_rows + index * unit, unit), unit), :]

    def long_copy(kind, layer, slot, step):
        j, half, k, sem = stream(kind, layer, slot)
        sign = sign_of(slot)
        src = chunk(kind, layer, j, half, sign * 4) if step == 0 else ring[kind].at[k, step - 1]
        return remote(src, ring[kind].at[k, step], ring_send.at[sem], ring_recv.at[sem, step % 2], z_next(sign))

    def short_copy(kind, layer, slot, step):
        j, half, k, sem = stream(kind, layer, slot)
        sign = sign_of(slot)
        src = chunk(kind, layer, j, half, sign * -3) if step == 0 else ring[kind].at[k, 4 + step - 1]
        return remote(src, ring[kind].at[k, 4 + step], ring_send.at[sem], ring_recv.at[sem, step % 2], z_next(-sign))

    def both_of(kind, layer, slot, step):
        _, _, k, sem = stream(kind, layer, slot)
        two = ring[kind].at[k, 0:2]
        return remote(two, two, ring_send.at[sem], ring_recv.at[sem, step % 2], z_next(1))

    def chain_start(kind, layer, slot):
        long_copy(kind, layer, slot, 0).start()
        short_copy(kind, layer, slot, 0).start()

    def chain_step(kind, layer, slot, step):
        j, half, k, _ = stream(kind, layer, slot)
        sign = sign_of(slot)
        before = both_of(kind, layer, slot, step - 1)
        before.wait_recv()
        ring[kind][k, step - 1] = ring[kind][k, step - 1] + chunk(kind, layer, j, half, sign * (4 - step))[...]
        if step < 3:
            ring[kind][k, 3 + step] = ring[kind][k, 3 + step] + chunk(kind, layer, j, half, sign * (step - 3))[...]
        before.wait_send()
        long_copy(kind, layer, slot, step).start()
        if step < 3:
            short_copy(kind, layer, slot, step).start()

    def chain_last(kind, layer, slot):
        j, half, k, _ = stream(kind, layer, slot)
        before = long_copy(kind, layer, slot, 3)
        before.wait_recv()
        before.wait_send()
        return k, ring[kind][k, 3] + chunk(kind, layer, j, half, 0)[...]

    def steps(kind, layer, low, high, step):
        loop(low, high, lambda slot: chain_step(kind, layer, slot, step))

    def starts(kind, layer, low, high):
        loop(low, high, lambda slot: chain_start(kind, layer, slot))

    def z_last(layer):
        def act(slot):
            k, value = chain_last(Z, layer, slot)
            ring_z[k, 3] = value + ring_z[k, 6]
        loop(0, 8, act)

    def y_copy(layer, j):
        return remote(
            part_y.at[layer, j, pl.ds(half_rows, half_rows), :], y_relay.at[layer, j],
            y_send.at[0], y_mid.at[layer, j // 2], y_next(sign_of(j)),
        )

    def y_pass(layer, j):
        return remote(y_relay.at[layer, j], y_got.at[layer, j], y_send.at[1], y_end.at[layer, j // 2], y_next(sign_of(j)))

    def pair(layer, p, sems):
        two = y_relay.at[layer, 2 * p : 2 * p + 2]
        return remote(two, two, y_send.at[1], sems.at[layer, p], mate)

    def y_forward(layer, p):
        pair(layer, p, y_mid).wait_recv()
        loop(2 * p, 2 * p + 2, lambda j: y_pass(layer, j).start())

    groups = ((4, -3), (3, -2), (2, -1), (1,), (0,))

    def unit_rows(away):
        return pl.ds(pl.multiple_of(lax.rem(z + away + NZ, NZ) * unit, unit), unit)

    def y_forward_units(layer, p):
        pair(layer, p, y_mid).wait_recv()
        for g, aways in enumerate(groups):
            for away in aways:
                def act(j):
                    sign = sign_of(j)
                    at_rows = unit_rows(sign * away)
                    remote(
                        y_relay.at[layer, j, at_rows, :], y_got.at[layer, j, at_rows, :],
                        y_send.at[1], y_units.at[g], y_next(sign),
                    ).start()
                loop(2 * p, 2 * p + 2, act)

    def y_units_add(layer, p, g):
        four = y_got.at[layer, 2 * p : 2 * p + 2, 0 : unit * len(groups[g]), :]
        remote(four, four, y_send.at[1], y_units.at[g], mate).wait_recv()
        for away in groups[g]:
            def act(j):
                at_rows = unit_rows(sign_of(j) * away)
                part_y[layer, j, at_rows, :] = part_y[layer, j, at_rows, :] + y_got[layer, j, at_rows, :]
            loop(2 * p, 2 * p + 2, act)

    def y_begin(layer, p):
        pair(layer, p, y_end).wait_recv()

        def act(j):
            part_y[layer, j, 0:half_rows, :] = part_y[layer, j, 0:half_rows, :] + y_got[layer, j]
            chain_start(Y, layer, j)
        loop(2 * p, 2 * p + 2, act)

    def z_copy(layer, j):
        return remote(
            ring_z.at[layer * 8 + j * 2 + 1, 3], z_relay.at[layer, j], z_send.at[0], z_mid.at[layer], y_next(sign_of(j))
        )

    def z_pass(layer, j):
        return remote(z_relay.at[layer, j], z_got.at[layer, j], z_send.at[1], z_end_sem.at[layer], y_next(sign_of(j)))

    def z_all(layer, sems):
        return remote(z_relay.at[layer], z_got.at[layer], z_send.at[1], sems.at[layer], mate)

    def z_forward(layer):
        z_all(layer, z_mid).wait_recv()
        loop(0, BLOCKS, lambda j: z_pass(layer, j).start())

    def gcols(side, kind, j):
        return pl.ds(pl.multiple_of(side * half_cols + first_col[kind] + j * width[kind], 128), width[kind])

    def finish(kind, layer, j, k, value):
        ring[kind][k, 3] = value
        src = ring[kind].at[k, 3, pl.ds(pl.multiple_of((1 - core) * own_rows, own_rows), own_rows), :]
        remote(src, gbuf.at[layer, :, gcols(core, kind, j)], g_sem.at[0], g_sem.at[1], mate).start()
        mine = ring[kind][k, 3, pl.ds(pl.multiple_of(core * own_rows, own_rows), own_rows), :]
        gbuf[layer, :, gcols(core, kind, j)] = mine
        squares = value * value
        folded = squares[0:own_rows] + squares[own_rows : 2 * own_rows]
        total = folded[:, 0:128]
        for i in range(1, width[kind] // 128):
            total = total + folded[:, i * 128 : (i + 1) * 128]
        q_acc[layer] = q_acc[layer] + total

    def z_finish(layer):
        z_all(layer, z_end_sem).wait_recv()

        def act(j):
            k = layer * 8 + j * 2
            finish(Z, layer, j, k, ring_z[k, 3] + z_got[layer, j])
        loop(0, BLOCKS, act)

    def y_finish(layer, low, high):
        def act(j):
            k, value = chain_last(Y, layer, j)
            finish(Y, layer, j, k, value + ring_y[k, 6])
        loop(low, high, act)

    def d_copy(offset):
        return remote(d_own, d_got.at[offset - 1], d_sem.at[0], d_sem.at[1], group_device(offset))

    def q_copy(offset):
        return remote(q_own, q_got.at[offset - 1], q_sem.at[0], q_sem.at[1], group_device(offset))

    def all_of(got, sems):
        return remote(got, got, sems.at[0], sems.at[1], mate)

    def to_y(j):
        multiply(0, Y, j)
        y_copy(0, j).start()

    def to_z(j):
        multiply(0, Z, j)
        chain_start(Z, 0, 2 * j)
        chain_start(Z, 0, 2 * j + 1)

    og_copy(0, 0, Y).wait()
    loop(0, 2, to_y)
    og_copy(0, 0, Z).wait()
    loop(0, 4, to_z)
    loop(2, 4, to_y)

    for kind in (Z, Y):
        x_all(0, kind).wait_send()
        og_copy(1, 1, kind).wait()
        swap(1, kind, 0, 4)
    og_copy(1, 0, Z).wait()
    og_copy(1, 0, Y).wait()

    steps(Z, 0, 0, 8, 1)
    x_all(1, Z).wait_recv()
    loop(0, 4, lambda j: multiply(1, Z, j))
    steps(Z, 0, 0, 8, 2)
    y_forward(0, 0)
    x_all(1, Y).wait_recv()
    loop(0, 4, lambda j: multiply(1, Y, j))
    steps(Z, 0, 0, 8, 3)
    starts(Z, 1, 0, 8)
    y_forward(0, 1)
    loop(0, 4, lambda j: y_copy(1, j).start())
    z_last(0)
    all_of(c_got, c_sem).wait_recv()
    d_own[...] = c_own[...] + jnp.sum(c_got[...], axis=0)
    loop(1, 32, lambda offset: d_copy(offset).start())

    steps(Z, 1, 0, 8, 1)
    steps(Z, 1, 0, 8, 2)
    steps(Z, 1, 0, 8, 3)
    y_begin(0, 0)
    y_begin(0, 1)
    z_last(1)
    y_forward(1, 0)
    steps(Y, 0, 0, 4, 1)
    steps(Y, 0, 0, 4, 2)
    y_forward_units(1, 1)
    for layer in range(LAYERS):
        loop(0, BLOCKS, lambda j: z_copy(layer, j).start())
    steps(Y, 0, 0, 4, 3)
    y_finish(0, 0, 4)

    y_begin(1, 0)
    y_units_add(1, 1, 0)
    starts(Y, 1, 2, 4)
    steps(Y, 1, 0, 2, 1)
    y_units_add(1, 1, 1)
    steps(Y, 1, 2, 4, 1)
    steps(Y, 1, 0, 2, 2)
    y_units_add(1, 1, 2)
    steps(Y, 1, 2, 4, 2)
    z_forward(0)
    z_forward(1)
    steps(Y, 1, 0, 2, 3)
    y_units_add(1, 1, 3)
    steps(Y, 1, 2, 4, 3)
    y_units_add(1, 1, 4)
    y_finish(1, 0, 2)
    z_finish(0)
    z_finish(1)
    y_finish(1, 2, 4)

    q_own[...] = jnp.sum(q_acc[...], axis=1)
    for away in (4, 3, 5, 2, 6, 1, 7):
        loop(away * 4, away * 4 + 4, lambda offset: q_copy(offset).start())
    loop(1, 4, lambda offset: q_copy(offset).start())

    all_of(d_got, d_sem).wait_recv()
    totals = d_own[...] + jnp.sum(d_got[...], axis=0)
    lanes = lax.broadcasted_iota(jnp.int32, totals.shape, 1)
    mean_load = jnp.sum(totals, axis=1, keepdims=True) / 8.0
    own_load = jnp.sum(jnp.where(lanes == me_expert, totals, 0.0), axis=1, keepdims=True)
    beta = own_load / (own_load + mean_load)

    landed = gbuf.at[:, :, 0:half_cols]
    all_g = remote(landed, landed, g_sem.at[0], g_sem.at[1], mate)
    all_g.wait_recv()
    out_copy = pltpu.make_async_copy(gbuf, grad, out_sem)
    out_copy.start()

    all_g.wait_send()
    for i in range(2):
        remote(y_relay, y_got, y_send.at[i], y_units.at[0], mate).wait_send()
        remote(z_relay, z_got, z_send.at[i], z_mid.at[0], mate).wait_send()
    for kind in (Z, Y):
        x_all(1, kind).wait_send()
    a_copy.wait_send()
    all_of(c_got, c_sem).wait_send()
    all_of(d_got, d_sem).wait_send()
    all_of(q_got, q_sem).wait_send()

    all_of(q_got, q_sem).wait_recv()
    total = jnp.sum(q_own[...] + jnp.sum(q_got[...], axis=0), axis=1, keepdims=True)
    root_mean = jnp.sqrt(total / float(rows * 2 * half_cols))
    factor = step_size * (own_load / mean_load) * clip_level / jnp.maximum(root_mean, clip_level)
    for layer in range(LAYERS):
        factor_out[layer] = factor[layer, 0]
        beta_out[layer] = beta[layer, 0]
    out_copy.wait()


def on_device(activations, out_grads, weights, shadow, counts):
    acts, og = activations[:, 0], out_grads[:, 0]
    tokens, rows = acts.shape[1:]
    ff = og.shape[2]
    unit = rows // 2 // NZ
    half = rows // 2
    tiles = ff // 2 // 128 // BLOCKS
    wide_z, wide_y = (tiles * 3 // 7) * 128, (tiles - tiles * 3 // 7) * 128
    f32, bf16 = jnp.float32, jnp.bfloat16
    dma = pltpu.SemaphoreType.DMA
    vmem = pl.BlockSpec(memory_space=pltpu.VMEM)
    smem = pl.BlockSpec(memory_space=pltpu.SMEM)
    hbm = pl.BlockSpec(memory_space=pl.ANY)
    grad, factor, beta = pl.pallas_call(
        kernel,
        out_shape=(
            jax.ShapeDtypeStruct((LAYERS, unit // 2, ff), f32),
            jax.ShapeDtypeStruct((LAYERS,), f32),
            jax.ShapeDtypeStruct((LAYERS,), f32),
        ),
        in_specs=[vmem, hbm, vmem],
        out_specs=(hbm, smem, smem),
        scratch_shapes=[
            pltpu.VMEM((LAYERS, BLOCKS, rows, wide_z), f32),
            pltpu.VMEM((LAYERS, BLOCKS, rows, wide_y), f32),
            pltpu.VMEM((LAYERS * 8, NZ - 1, unit, wide_z), f32),
            pltpu.VMEM((LAYERS * 4, NZ - 1, unit, wide_y), f32),
            pltpu.VMEM((LAYERS, BLOCKS, half, wide_y), f32),
            pltpu.VMEM((LAYERS, BLOCKS, half, wide_y), f32),
            pltpu.VMEM((LAYERS, BLOCKS, unit, wide_z), f32),
            pltpu.VMEM((LAYERS, BLOCKS, unit, wide_z), f32),
            pltpu.VMEM((LAYERS, BLOCKS, tokens, wide_z), f32),
            pltpu.VMEM((LAYERS, BLOCKS, tokens, wide_y), f32),
            pltpu.VMEM((BLOCKS, tokens, wide_z), f32),
            pltpu.VMEM((BLOCKS, tokens, wide_y), f32),
            pltpu.VMEM((LAYERS, tokens, ff // 2), bf16),
            pltpu.VMEM((LAYERS, tokens, ff // 2), bf16),
            pltpu.VMEM((LAYERS, tokens, rows), f32),
            pltpu.VMEM((LAYERS, tokens, rows), f32),
            pltpu.VMEM((rows, 2 * tokens), f32),
            pltpu.VMEM((LAYERS, rows, 2 * tokens), bf16),
            pltpu.VMEM((LAYERS, unit // 2, ff), f32),
            pltpu.VMEM((LAYERS, 128), f32),
            pltpu.VMEM((7, LAYERS, 128), f32),
            pltpu.VMEM((LAYERS, 128), f32),
            pltpu.VMEM((31, LAYERS, 128), f32),
            pltpu.VMEM((LAYERS, 128), f32),
            pltpu.VMEM((31, LAYERS, 128), f32),
            pltpu.VMEM((LAYERS, unit // 2, 128), f32),
            dma((LAYERS, 2, 2)),
            dma((2,)),
            dma((2, BLOCKS)),
            dma((2,)),
            dma((2,)),
            dma((16,)),
            dma((16, 2)),
            dma((2,)),
            dma((LAYERS, 2)),
            dma((LAYERS, 2)),
            dma((5,)),
            dma((2,)),
            dma((LAYERS,)),
            dma((LAYERS,)),
            dma((2,)),
            dma((2,)),
            dma((2,)),
            dma((2,)),
            dma,
        ],
        compiler_params=pltpu.CompilerParams(
            collective_id=0, has_side_effects=True, vmem_limit_bytes=62 * 1024 * 1024
        ),
    )(acts, og, counts)
    summed = grad[:, None]
    factor = factor[:, None, None, None]
    beta = beta[:, None, None, None]
    updated = weights - factor * summed
    return updated, shadow + beta * (updated - shadow)


def solution(mesh):
    split = Mesh(
        mesh.devices.reshape(mesh.shape["dp"], 4, 2, 2, 2),
        ("dp", "expert_0", "expert_1", "shard_0", "shard_1"),
    )
    return jax.shard_map(
        on_device,
        mesh=split,
        in_specs=(
            P(None, EXPERT, DP_SHARD, None),
            P(None, EXPERT, DP_SHARD, None),
            P(None, EXPERT, DP_SHARD, None),
            P(None, EXPERT, DP_SHARD, None),
            P(None, DP_EXPERT_SHARD, None),
        ),
        out_specs=(P(None, EXPERT, DP_SHARD, None), P(None, EXPERT, DP_SHARD, None)),
        check_vma=False,
    )
```

```python
import jax
import jax.numpy as jnp
from jax import lax
from jax.experimental import pallas as pl
from jax.experimental.pallas import tpu as pltpu
from jax.sharding import Mesh
from jax.sharding import PartitionSpec as P

MESH = pl.DeviceIdType.MESH
LAYERS = 2
EXPERT = ("expert_0", "expert_1")
DP_EXPERT_SHARD = ("dp", "expert_0", "expert_1", "shard_0", "shard_1")
DP_SHARD = ("dp", "shard_0", "shard_1")

step_size = 0.5
clip_level = 1.0

NZ = 8
BLOCKS = 4
Z, Y = 0, 1


def kernel(
    acts_in, og, counts_in, weights, shadow, new_weights, new_shadow,
    part_z, part_y, ring_z, ring_y, y_got, y_relay, z_got, z_relay, x_got_z, x_got_y, x_out_z, x_out_y,
    own_half, other_half, acts, counts, w_in, s_in, a_out, a_got, a_rows, a_t, gbuf, c_own, c_got, q_own, q_got, q_acc,
    og_sem, in_sem, x_send, x_recv, x_recv_late, a_sem, ring_send, ring_recv,
    y_send, y_mid, y_end, y_units, z_send, z_mid, z_end_sem, g_sem, c_sem, q_sem,
):
    z = lax.axis_index("dp")
    x = lax.axis_index("expert_0")
    y_lo = lax.axis_index("expert_1")
    y_hi = lax.axis_index("shard_0")
    core = lax.axis_index("shard_1")
    y = y_hi * 2 + y_lo
    tokens = acts.shape[1]
    rows = acts.shape[2]
    half_rows = rows // 2
    unit = half_rows // NZ
    own_rows = unit // 2
    part = (part_z, part_y)
    ring = (ring_z, ring_y)
    x_got = (x_got_z, x_got_y)
    x_out = (x_out_z, x_out_y)
    width = (part_z.shape[-1], part_y.shape[-1])
    first_col = (0, BLOCKS * width[Z])
    half_cols = BLOCKS * (width[Z] + width[Y])

    def at(z=z, x=x, y_lo=y_lo, y_hi=y_hi, core=core):
        return (z, x, y_lo, y_hi, core)

    def z_next(sign):
        return at(z=lax.rem(z + sign + NZ, NZ))

    def y_next(sign):
        to = lax.rem(y + sign + 4, 4)
        return at(y_lo=lax.rem(to, 2), y_hi=to // 2)

    mate = at(core=1 - core)
    me_group = z * 4 + y_hi * 2 + core
    me_expert = x * 2 + y_lo

    def group_device(offset):
        to = lax.rem(me_group + offset, 32)
        return at(z=to // 4, y_hi=lax.rem(to // 2, 2), core=lax.rem(to, 2))

    def remote(src, dst, send, recv, device):
        return pltpu.make_async_remote_copy(
            src_ref=src, dst_ref=dst, send_sem=send, recv_sem=recv, device_id=device, device_id_type=MESH
        )

    def loop(low, high, act):
        def body(i, _):
            act(i)
            return 0
        lax.fori_loop(low, high, body, 0)

    def og_copy(layer, which, kind):
        first = core if which == 0 else 1 - core
        to = own_half if which == 0 else other_half
        size = BLOCKS * width[kind]
        cols = pl.ds(pl.multiple_of(first * half_cols + first_col[kind], 128), size)
        return pltpu.make_async_copy(
            og.at[layer, :, cols], to.at[layer, :, first_col[kind] : first_col[kind] + size], og_sem.at[layer, which, kind]
        )

    in_copies = [
        pltpu.make_async_copy(src, dst, in_sem.at[i])
        for i, (src, dst) in enumerate(((acts_in, acts), (counts_in, counts), (weights, w_in), (shadow, s_in)))
    ]

    barrier = pltpu.get_barrier_semaphore()
    near = (
        mate, z_next(1), z_next(-1), y_next(1), y_next(-1), at(x=x + 1 - 2 * lax.rem(x, 2)), at(x=3 - x)
    )
    for device in near:
        pl.semaphore_signal(barrier, inc=1, device_id=device, device_id_type=MESH)

    in_copies[0].start()
    in_copies[1].start()
    for layer in range(LAYERS):
        for which, kind in ((1, Y), (0, Y), (1, Z), (0, Z)):
            og_copy(layer, which, kind).start()
    in_copies[2].start()
    in_copies[3].start()

    def cols_of(kind, j):
        return pl.ds(pl.multiple_of(first_col[kind] + j * width[kind], 128), width[kind])

    def convert(layer, kind, j):
        x_out[kind][j] = other_half[layer, :, cols_of(kind, j)].astype(jnp.float32)

    def x_copy(layer, kind, j):
        sem = x_recv.at[kind, j] if layer == 0 else x_recv_late.at[kind]
        return remote(x_out[kind].at[j], x_got[kind].at[layer, j], x_send.at[kind], sem, mate)

    def x_all(layer, kind):
        return remote(x_out[kind], x_got[kind].at[layer], x_send.at[kind], x_recv_late.at[kind], mate)

    in_copies[0].wait()
    a_out[...] = acts[...].astype(jnp.float32)
    in_copies[1].wait()
    c_own[0] = jnp.zeros_like(c_own[0])
    c_own[0, :, 0:8] = counts[:, 0, :].astype(jnp.float32)
    q_acc[...] = jnp.zeros_like(q_acc)
    og_copy(0, 1, Y).wait()
    loop(0, 2, lambda j: convert(0, Y, j))
    pl.semaphore_wait(barrier, len(near))

    a_copy = remote(a_out, a_got, a_sem.at[0], a_sem.at[1], mate)
    a_copy.start()

    def swap(layer, kind, low, high):
        def act(j):
            convert(layer, kind, j)
            x_copy(layer, kind, j).start()
        loop(low, high, act)

    loop(0, 2, lambda j: x_copy(0, Y, j).start())
    og_copy(0, 1, Z).wait()
    swap(0, Z, 0, 4)
    swap(0, Y, 2, 4)

    c_copies = [
        remote(c_own.at[i], c_got.at[i], c_sem.at[0, i], c_sem.at[1, i], device)
        for i, device in enumerate((near[5], near[6], at(y_lo=1 - y_lo)))
    ]
    c_copies[0].start()

    def c_next(i):
        c_copies[i].wait_recv()
        c_own[i + 1] = c_own[i] + c_got[i]
        if i < 2:
            c_copies[i + 1].start()

    a_copy.wait_recv()
    for layer in range(LAYERS):
        a_rows[:, 0:tokens] = a_out[layer].T
        a_rows[:, tokens : 2 * tokens] = a_got[layer].T
        for half in range(2):
            side = y_hi if half == 0 else 1 - y_hi
            for zz in range(NZ):
                piece = a_rows[pl.ds(pl.multiple_of(zz * 2 * unit + side * unit, unit), unit), :]
                a_t[layer, half * half_rows + zz * unit : half * half_rows + (zz + 1) * unit, :] = piece.astype(jnp.bfloat16)

    def multiply(layer, kind, j):
        if layer == 0:
            x_copy(layer, kind, j).wait_recv()
        theirs = x_got[kind][layer, j].astype(jnp.bfloat16)
        both = jnp.concatenate([own_half[layer, :, cols_of(kind, j)], theirs], axis=0)
        part[kind][layer, j] = jnp.dot(a_t[layer], both, preferred_element_type=jnp.float32)

    def stream(kind, layer, slot):
        if kind == Z:
            return slot // 2, lax.rem(slot, 2), layer * 8 + slot, layer * 8 + slot
        return slot, 0, layer * 4 + slot, layer * 4 + slot

    def sign_of(slot):
        return 1 - 2 * lax.rem(slot, 2)

    def chunk(kind, layer, j, half, away):
        index = lax.rem(z + away + NZ, NZ)
        return part[kind].at[layer, j, pl.ds(pl.multiple_of(half * half_rows + index * unit, unit), unit), :]

    def long_copy(kind, layer, slot, step):
        j, half, k, sem = stream(kind, layer, slot)
        sign = sign_of(slot)
        src = chunk(kind, layer, j, half, sign * 4) if step == 0 else ring[kind].at[k, step - 1]
        return remote(src, ring[kind].at[k, step], ring_send.at[sem], ring_recv.at[sem, step % 2], z_next(sign))

    def short_copy(kind, layer, slot, step):
        j, half, k, sem = stream(kind, layer, slot)
        sign = sign_of(slot)
        src = chunk(kind, layer, j, half, sign * -3) if step == 0 else ring[kind].at[k, 4 + step - 1]
        return remote(src, ring[kind].at[k, 4 + step], ring_send.at[sem], ring_recv.at[sem, step % 2], z_next(-sign))

    def both_of(kind, layer, slot, step):
        _, _, k, sem = stream(kind, layer, slot)
        two = ring[kind].at[k, 0:2]
        return remote(two, two, ring_send.at[sem], ring_recv.at[sem, step % 2], z_next(1))

    def chain_start(kind, layer, slot):
        long_copy(kind, layer, slot, 0).start()
        short_copy(kind, layer, slot, 0).start()

    def chain_step(kind, layer, slot, step):
        j, half, k, _ = stream(kind, layer, slot)
        sign = sign_of(slot)
        before = both_of(kind, layer, slot, step - 1)
        before.wait_recv()
        ring[kind][k, step - 1] = ring[kind][k, step - 1] + chunk(kind, layer, j, half, sign * (4 - step))[...]
        if step < 3:
            ring[kind][k, 3 + step] = ring[kind][k, 3 + step] + chunk(kind, layer, j, half, sign * (step - 3))[...]
        before.wait_send()
        long_copy(kind, layer, slot, step).start()
        if step < 3:
            short_copy(kind, layer, slot, step).start()

    def chain_last(kind, layer, slot):
        j, half, k, _ = stream(kind, layer, slot)
        before = long_copy(kind, layer, slot, 3)
        before.wait_recv()
        before.wait_send()
        return k, ring[kind][k, 3] + chunk(kind, layer, j, half, 0)[...]

    def steps(kind, layer, low, high, step):
        loop(low, high, lambda slot: chain_step(kind, layer, slot, step))

    def starts(kind, layer, low, high):
        loop(low, high, lambda slot: chain_start(kind, layer, slot))

    def z_last(layer):
        def act(slot):
            k, value = chain_last(Z, layer, slot)
            ring_z[k, 3] = value + ring_z[k, 6]
        loop(0, 8, act)

    def y_copy(layer, j):
        return remote(
            part_y.at[layer, j, pl.ds(half_rows, half_rows), :], y_relay.at[layer, j],
            y_send.at[0], y_mid.at[layer, j // 2], y_next(sign_of(j)),
        )

    def y_pass(layer, j):
        return remote(y_relay.at[layer, j], y_got.at[layer, j], y_send.at[1], y_end.at[layer, j // 2], y_next(sign_of(j)))

    def pair(layer, p, sems):
        two = y_relay.at[layer, 2 * p : 2 * p + 2]
        return remote(two, two, y_send.at[1], sems.at[layer, p], mate)

    def y_forward(layer, p):
        pair(layer, p, y_mid).wait_recv()
        loop(2 * p, 2 * p + 2, lambda j: y_pass(layer, j).start())

    groups = ((4, -3), (3, -2), (2, -1), (1,), (0,))

    def unit_rows(away):
        return pl.ds(pl.multiple_of(lax.rem(z + away + NZ, NZ) * unit, unit), unit)

    def y_forward_units(layer, p):
        pair(layer, p, y_mid).wait_recv()
        for g, aways in enumerate(groups):
            for away in aways:
                def act(j):
                    sign = sign_of(j)
                    at_rows = unit_rows(sign * away)
                    remote(
                        y_relay.at[layer, j, at_rows, :], y_got.at[layer, j, at_rows, :],
                        y_send.at[1], y_units.at[g], y_next(sign),
                    ).start()
                loop(2 * p, 2 * p + 2, act)

    def y_units_add(layer, p, g):
        four = y_got.at[layer, 2 * p : 2 * p + 2, 0 : unit * len(groups[g]), :]
        remote(four, four, y_send.at[1], y_units.at[g], mate).wait_recv()
        for away in groups[g]:
            def act(j):
                at_rows = unit_rows(sign_of(j) * away)
                part_y[layer, j, at_rows, :] = part_y[layer, j, at_rows, :] + y_got[layer, j, at_rows, :]
            loop(2 * p, 2 * p + 2, act)

    def y_begin(layer, p):
        pair(layer, p, y_end).wait_recv()

        def act(j):
            part_y[layer, j, 0:half_rows, :] = part_y[layer, j, 0:half_rows, :] + y_got[layer, j]
            chain_start(Y, layer, j)
        loop(2 * p, 2 * p + 2, act)

    def z_copy(layer, j):
        return remote(
            ring_z.at[layer * 8 + j * 2 + 1, 3], z_relay.at[layer, j], z_send.at[0], z_mid.at[layer], y_next(sign_of(j))
        )

    def z_pass(layer, j):
        return remote(z_relay.at[layer, j], z_got.at[layer, j], z_send.at[1], z_end_sem.at[layer], y_next(sign_of(j)))

    def z_all(layer, sems):
        return remote(z_relay.at[layer], z_got.at[layer], z_send.at[1], sems.at[layer], mate)

    def z_forward(layer):
        z_all(layer, z_mid).wait_recv()
        loop(0, BLOCKS, lambda j: z_pass(layer, j).start())

    def gcols(side, kind, j):
        return pl.ds(pl.multiple_of(side * half_cols + first_col[kind] + j * width[kind], 128), width[kind])

    def finish(kind, layer, j, k, value):
        ring[kind][k, 3] = value
        src = ring[kind].at[k, 3, pl.ds(pl.multiple_of((1 - core) * own_rows, own_rows), own_rows), :]
        remote(src, gbuf.at[layer, :, gcols(core, kind, j)], g_sem.at[0], g_sem.at[1], mate).start()
        mine = ring[kind][k, 3, pl.ds(pl.multiple_of(core * own_rows, own_rows), own_rows), :]
        gbuf[layer, :, gcols(core, kind, j)] = mine
        squares = value * value
        folded = squares[0:own_rows] + squares[own_rows : 2 * own_rows]
        total = folded[:, 0:128]
        for i in range(1, width[kind] // 128):
            total = total + folded[:, i * 128 : (i + 1) * 128]
        q_acc[layer] = q_acc[layer] + total

    def z_finish(layer):
        z_all(layer, z_end_sem).wait_recv()

        def act(j):
            k = layer * 8 + j * 2
            finish(Z, layer, j, k, ring_z[k, 3] + z_got[layer, j])
        loop(0, BLOCKS, act)

    def y_finish(layer, low, high):
        def act(j):
            k, value = chain_last(Y, layer, j)
            finish(Y, layer, j, k, value + ring_y[k, 6])
        loop(low, high, act)

    def q_copy(offset):
        return remote(q_own, q_got.at[offset - 1], q_sem.at[0], q_sem.at[1], group_device(offset))

    def all_of(got, sems):
        return remote(got, got, sems.at[0], sems.at[1], mate)

    def to_y(j):
        multiply(0, Y, j)
        y_copy(0, j).start()

    def to_z(j):
        multiply(0, Z, j)
        chain_start(Z, 0, 2 * j)
        chain_start(Z, 0, 2 * j + 1)

    og_copy(0, 0, Y).wait()
    loop(0, 2, to_y)
    og_copy(0, 0, Z).wait()
    loop(0, 4, to_z)
    loop(2, 4, to_y)

    for kind in (Z, Y):
        x_all(0, kind).wait_send()
        og_copy(1, 1, kind).wait()
        swap(1, kind, 0, 4)
    og_copy(1, 0, Z).wait()
    og_copy(1, 0, Y).wait()

    steps(Z, 0, 0, 8, 1)
    x_all(1, Z).wait_recv()
    loop(0, 4, lambda j: multiply(1, Z, j))
    steps(Z, 0, 0, 8, 2)
    y_forward(0, 0)
    x_all(1, Y).wait_recv()
    loop(0, 4, lambda j: multiply(1, Y, j))
    steps(Z, 0, 0, 8, 3)
    starts(Z, 1, 0, 8)
    y_forward(0, 1)
    loop(0, 4, lambda j: y_copy(1, j).start())
    z_last(0)
    c_next(0)
    steps(Z, 1, 0, 8, 1)
    steps(Z, 1, 0, 8, 2)
    c_next(1)
    steps(Z, 1, 0, 8, 3)
    y_begin(0, 0)
    y_begin(0, 1)
    z_last(1)
    y_forward(1, 0)
    steps(Y, 0, 0, 4, 1)
    steps(Y, 0, 0, 4, 2)
    y_forward_units(1, 1)
    for layer in range(LAYERS):
        loop(0, BLOCKS, lambda j: z_copy(layer, j).start())
    steps(Y, 0, 0, 4, 3)
    y_begin(1, 0)
    y_finish(0, 0, 4)

    y_units_add(1, 1, 0)
    starts(Y, 1, 2, 4)
    steps(Y, 1, 0, 2, 1)
    y_units_add(1, 1, 1)
    steps(Y, 1, 2, 4, 1)
    steps(Y, 1, 0, 2, 2)
    y_units_add(1, 1, 2)
    steps(Y, 1, 2, 4, 2)
    z_forward(0)
    z_forward(1)
    c_next(2)
    steps(Y, 1, 0, 2, 3)
    y_units_add(1, 1, 3)
    steps(Y, 1, 2, 4, 3)
    y_units_add(1, 1, 4)
    y_finish(1, 0, 2)
    z_finish(0)
    z_finish(1)
    y_finish(1, 2, 4)

    q_own[0:2] = jnp.sum(q_acc[...], axis=1)
    q_own[2:4] = c_own[3]
    for away in (4, 3, 5, 2, 6, 1, 7):
        loop(away * 4, away * 4 + 4, lambda offset: q_copy(offset).start())
    loop(1, 4, lambda offset: q_copy(offset).start())

    landed = gbuf.at[:, :, 0:half_cols]
    all_g = remote(landed, landed, g_sem.at[0], g_sem.at[1], mate)
    all_g.wait_recv()
    in_copies[2].wait()
    in_copies[3].wait()

    all_g.wait_send()
    for i in range(2):
        remote(y_relay, y_got, y_send.at[i], y_units.at[0], mate).wait_send()
        remote(z_relay, z_got, z_send.at[i], z_mid.at[0], mate).wait_send()
    for kind in (Z, Y):
        x_all(1, kind).wait_send()
    a_copy.wait_send()
    for copy in c_copies:
        copy.wait_send()
    all_of(q_got, q_sem).wait_send()

    all_of(q_got, q_sem).wait_recv()
    sums = q_own[...] + jnp.sum(q_got[...], axis=0)
    root_mean = jnp.sqrt(jnp.sum(sums[0:2], axis=1, keepdims=True) / float(rows * 2 * half_cols))
    totals = sums[2:4]
    lanes = lax.broadcasted_iota(jnp.int32, totals.shape, 1)
    mean_load = jnp.sum(totals, axis=1, keepdims=True) / 8.0
    own_load = jnp.sum(jnp.where(lanes == me_expert, totals, 0.0), axis=1, keepdims=True)
    factor = step_size * (own_load / mean_load) * clip_level / jnp.maximum(root_mean, clip_level)
    beta = own_load / (own_load + mean_load)
    for layer in range(LAYERS):
        this_factor = jnp.broadcast_to(factor[layer : layer + 1], (own_rows, 128))
        this_beta = jnp.broadcast_to(beta[layer : layer + 1], (own_rows, 128))

        def update(i):
            for n in range(8):
                cols = pl.ds(pl.multiple_of(i * 1024 + n * 128, 128), 128)
                updated = w_in[layer, 0, :, cols] - this_factor * gbuf[layer, :, cols]
                new_weights[layer, 0, :, cols] = updated
                previous = s_in[layer, 0, :, cols]
                new_shadow[layer, 0, :, cols] = previous + this_beta * (updated - previous)
        loop(0, 2 * half_cols // 1024, update)


def on_device(activations, out_grads, weights, shadow, counts):
    acts, og = activations[:, 0], out_grads[:, 0]
    tokens, rows = acts.shape[1:]
    ff = og.shape[2]
    unit = rows // 2 // NZ
    half = rows // 2
    tiles = ff // 2 // 128 // BLOCKS
    wide_z, wide_y = (tiles * 3 // 7) * 128, (tiles - tiles * 3 // 7) * 128
    f32, bf16 = jnp.float32, jnp.bfloat16
    dma = pltpu.SemaphoreType.DMA
    vmem = pl.BlockSpec(memory_space=pltpu.VMEM)
    hbm = pl.BlockSpec(memory_space=pl.ANY)
    return pl.pallas_call(
        kernel,
        out_shape=(pltpu.VMEM(weights.shape, f32), pltpu.VMEM(shadow.shape, f32)),
        in_specs=[hbm] * 5,
        out_specs=(vmem, vmem),
        scratch_shapes=[
            pltpu.VMEM((LAYERS, BLOCKS, rows, wide_z), f32),
            pltpu.VMEM((LAYERS, BLOCKS, rows, wide_y), f32),
            pltpu.VMEM((LAYERS * 8, NZ - 1, unit, wide_z), f32),
            pltpu.VMEM((LAYERS * 4, NZ - 1, unit, wide_y), f32),
            pltpu.VMEM((LAYERS, BLOCKS, half, wide_y), f32),
            pltpu.VMEM((LAYERS, BLOCKS, half, wide_y), f32),
            pltpu.VMEM((LAYERS, BLOCKS, unit, wide_z), f32),
            pltpu.VMEM((LAYERS, BLOCKS, unit, wide_z), f32),
            pltpu.VMEM((LAYERS, BLOCKS, tokens, wide_z), f32),
            pltpu.VMEM((LAYERS, BLOCKS, tokens, wide_y), f32),
            pltpu.VMEM((BLOCKS, tokens, wide_z), f32),
            pltpu.VMEM((BLOCKS, tokens, wide_y), f32),
            pltpu.VMEM((LAYERS, tokens, ff // 2), bf16),
            pltpu.VMEM((LAYERS, tokens, ff // 2), bf16),
            pltpu.VMEM(acts.shape, bf16),
            pltpu.VMEM(counts.shape, counts.dtype),
            pltpu.VMEM(weights.shape, f32),
            pltpu.VMEM(shadow.shape, f32),
            pltpu.VMEM((LAYERS, tokens, rows), f32),
            pltpu.VMEM((LAYERS, tokens, rows), f32),
            pltpu.VMEM((rows, 2 * tokens), f32),
            pltpu.VMEM((LAYERS, rows, 2 * tokens), bf16),
            pltpu.VMEM((LAYERS, unit // 2, ff), f32),
            pltpu.VMEM((4, LAYERS, 128), f32),
            pltpu.VMEM((3, LAYERS, 128), f32),
            pltpu.VMEM((2 * LAYERS, 128), f32),
            pltpu.VMEM((31, 2 * LAYERS, 128), f32),
            pltpu.VMEM((LAYERS, unit // 2, 128), f32),
            dma((LAYERS, 2, 2)),
            dma((4,)),
            dma((2,)),
            dma((2, BLOCKS)),
            dma((2,)),
            dma((2,)),
            dma((16,)),
            dma((16, 2)),
            dma((2,)),
            dma((LAYERS, 2)),
            dma((LAYERS, 2)),
            dma((5,)),
            dma((2,)),
            dma((LAYERS,)),
            dma((LAYERS,)),
            dma((2,)),
            dma((2, 3)),
            dma((2,)),
        ],
        compiler_params=pltpu.CompilerParams(
            collective_id=0, has_side_effects=True, vmem_limit_bytes=58 * 1024 * 1024
        ),
    )(acts, og, counts, weights, shadow)


def solution(mesh):
    split = Mesh(
        mesh.devices.reshape(mesh.shape["dp"], 4, 2, 2, 2),
        ("dp", "expert_0", "expert_1", "shard_0", "shard_1"),
    )
    return jax.shard_map(
        on_device,
        mesh=split,
        in_specs=(
            P(None, EXPERT, DP_SHARD, None),
            P(None, EXPERT, DP_SHARD, None),
            P(None, EXPERT, DP_SHARD, None),
            P(None, EXPERT, DP_SHARD, None),
            P(None, DP_EXPERT_SHARD, None),
        ),
        out_specs=(P(None, EXPERT, DP_SHARD, None), P(None, EXPERT, DP_SHARD, None)),
        check_vma=False,
    )
```

```python
import jax
import jax.numpy as jnp
from jax import lax
from jax.experimental import pallas as pl
from jax.experimental.pallas import tpu as pltpu
from jax.sharding import Mesh
from jax.sharding import PartitionSpec as P

MESH = pl.DeviceIdType.MESH
LAYERS = 2
EXPERT = ("expert_0", "expert_1")
DP_EXPERT_SHARD = ("dp", "expert_0", "expert_1", "shard_0", "shard_1")
DP_SHARD = ("dp", "shard_0", "shard_1")

step_size = 0.5
clip_level = 1.0

NZ = 8
BLOCKS = 4
Z, Y = 0, 1


def kernel(
    acts_in, og, counts_in, weights, shadow, new_weights, new_shadow,
    part_z, part_y, ring_z, ring_y, y_got, y_relay, z_got, z_relay, x_got_z, x_got_y, x_out_z, x_out_y,
    own_half, other_half, acts, counts, w_in, s_in, a_out, a_got, a_rows, a_t, gbuf, c_own, c_got, q_own, q_got, q_acc,
    og_sem, in_sem, x_send, x_recv, x_recv_late, a_sem, ring_send, ring_recv,
    y_send, y_mid, y_end, y_parts, y_unit, z_send, z_mid, z_end_sem, g_sem, c_sem, q_sem,
):
    z = lax.axis_index("dp")
    x = lax.axis_index("expert_0")
    y_lo = lax.axis_index("expert_1")
    y_hi = lax.axis_index("shard_0")
    core = lax.axis_index("shard_1")
    y = y_hi * 2 + y_lo
    tokens = acts.shape[1]
    rows = acts.shape[2]
    half_rows = rows // 2
    unit = half_rows // NZ
    own_rows = unit // 2
    part = (part_z, part_y)
    ring = (ring_z, ring_y)
    x_got = (x_got_z, x_got_y)
    x_out = (x_out_z, x_out_y)
    width = (part_z.shape[-1], part_y.shape[-1])
    first_col = (0, BLOCKS * width[Z])
    half_cols = BLOCKS * (width[Z] + width[Y])

    def at(z=z, x=x, y_lo=y_lo, y_hi=y_hi, core=core):
        return (z, x, y_lo, y_hi, core)

    def z_next(sign):
        return at(z=lax.rem(z + sign + NZ, NZ))

    def y_next(sign):
        to = lax.rem(y + sign + 4, 4)
        return at(y_lo=lax.rem(to, 2), y_hi=to // 2)

    mate = at(core=1 - core)
    me_group = z * 4 + y_hi * 2 + core
    me_expert = x * 2 + y_lo

    def group_device(offset):
        to = lax.rem(me_group + offset, 32)
        return at(z=to // 4, y_hi=lax.rem(to // 2, 2), core=lax.rem(to, 2))

    def remote(src, dst, send, recv, device):
        return pltpu.make_async_remote_copy(
            src_ref=src, dst_ref=dst, send_sem=send, recv_sem=recv, device_id=device, device_id_type=MESH
        )

    def loop(low, high, act):
        def body(i, _):
            act(i)
            return 0
        lax.fori_loop(low, high, body, 0)

    def og_copy(layer, which, kind):
        first = core if which == 0 else 1 - core
        to = own_half if which == 0 else other_half
        size = BLOCKS * width[kind]
        cols = pl.ds(pl.multiple_of(first * half_cols + first_col[kind], 128), size)
        return pltpu.make_async_copy(
            og.at[layer, :, cols], to.at[layer, :, first_col[kind] : first_col[kind] + size], og_sem.at[layer, which, kind]
        )

    in_copies = [
        pltpu.make_async_copy(src, dst, in_sem.at[i])
        for i, (src, dst) in enumerate(((acts_in, acts), (counts_in, counts), (weights, w_in), (shadow, s_in)))
    ]

    barrier = pltpu.get_barrier_semaphore()
    near = (
        mate, z_next(1), z_next(-1), y_next(1), y_next(-1), at(x=x + 1 - 2 * lax.rem(x, 2)), at(x=3 - x)
    )
    for device in near:
        pl.semaphore_signal(barrier, inc=1, device_id=device, device_id_type=MESH)

    og_copy(0, 1, Y).start()
    in_copies[0].start()
    for which, kind in ((0, Y), (1, Z), (0, Z)):
        og_copy(0, which, kind).start()
    in_copies[1].start()

    def cols_of(kind, j):
        return pl.ds(pl.multiple_of(first_col[kind] + j * width[kind], 128), width[kind])

    def convert(layer, kind, j):
        x_out[kind][j] = other_half[layer, :, cols_of(kind, j)].astype(jnp.float32)

    def x_copy(layer, kind, j):
        sem = x_recv.at[kind, j] if layer == 0 else x_recv_late.at[kind]
        return remote(x_out[kind].at[j], x_got[kind].at[layer, j], x_send.at[kind], sem, mate)

    def x_all(layer, kind):
        return remote(x_out[kind], x_got[kind].at[layer], x_send.at[kind], x_recv_late.at[kind], mate)

    def a_copy(layer):
        return remote(a_out.at[layer], a_got.at[layer], a_sem.at[0, layer], a_sem.at[1, layer], mate)

    def a_join(layer):
        a_rows[:, 0:tokens] = a_out[layer].T
        a_copy(layer).wait_recv()
        a_rows[:, tokens : 2 * tokens] = a_got[layer].T
        for half in range(2):
            side = y_hi if half == 0 else 1 - y_hi
            for zz in range(NZ):
                piece = a_rows[pl.ds(pl.multiple_of(zz * 2 * unit + side * unit, unit), unit), :]
                a_t[layer, half * half_rows + zz * unit : half * half_rows + (zz + 1) * unit, :] = piece.astype(jnp.bfloat16)

    def swap(layer, kind, low, high):
        def act(j):
            convert(layer, kind, j)
            x_copy(layer, kind, j).start()
        loop(low, high, act)

    c_copies = [
        remote(c_own.at[i], c_got.at[i], c_sem.at[0, i], c_sem.at[1, i], device)
        for i, device in enumerate((near[5], near[6], at(y_lo=1 - y_lo)))
    ]

    def c_next(i):
        c_copies[i].wait_recv()
        c_own[i + 1] = c_own[i] + c_got[i]
        if i < 2:
            c_copies[i + 1].start()

    og_copy(0, 1, Y).wait()
    loop(0, 2, lambda j: convert(0, Y, j))
    in_copies[0].wait()
    a_out[...] = acts[...].astype(jnp.float32)
    pl.semaphore_wait(barrier, len(near))

    a_copy(0).start()
    loop(0, 2, lambda j: x_copy(0, Y, j).start())
    og_copy(0, 1, Z).wait()
    swap(0, Z, 0, 4)
    swap(0, Y, 2, 4)
    a_copy(1).start()
    a_join(0)

    def multiply(layer, kind, j):
        if layer == 0:
            x_copy(layer, kind, j).wait_recv()
        theirs = x_got[kind][layer, j].astype(jnp.bfloat16)
        both = jnp.concatenate([own_half[layer, :, cols_of(kind, j)], theirs], axis=0)
        part[kind][layer, j] = jnp.dot(a_t[layer], both, preferred_element_type=jnp.float32)

    def stream(kind, layer, slot):
        if kind == Z:
            return slot // 2, lax.rem(slot, 2), layer * 8 + slot, layer * 8 + slot
        return slot, 0, layer * 4 + slot, layer * 4 + slot

    def sign_of(slot):
        return 1 - 2 * lax.rem(slot, 2)

    def chunk(kind, layer, j, half, away):
        index = lax.rem(z + away + NZ, NZ)
        return part[kind].at[layer, j, pl.ds(pl.multiple_of(half * half_rows + index * unit, unit), unit), :]

    def long_copy(kind, layer, slot, step):
        j, half, k, sem = stream(kind, layer, slot)
        sign = sign_of(slot)
        src = chunk(kind, layer, j, half, sign * 4) if step == 0 else ring[kind].at[k, step - 1]
        return remote(src, ring[kind].at[k, step], ring_send.at[sem], ring_recv.at[sem, step % 2], z_next(sign))

    def short_copy(kind, layer, slot, step):
        j, half, k, sem = stream(kind, layer, slot)
        sign = sign_of(slot)
        src = chunk(kind, layer, j, half, sign * -3) if step == 0 else ring[kind].at[k, 4 + step - 1]
        return remote(src, ring[kind].at[k, 4 + step], ring_send.at[sem], ring_recv.at[sem, step % 2], z_next(-sign))

    def both_of(kind, layer, slot, step):
        _, _, k, sem = stream(kind, layer, slot)
        two = ring[kind].at[k, 0:2]
        return remote(two, two, ring_send.at[sem], ring_recv.at[sem, step % 2], z_next(1))

    def chain_start(kind, layer, slot):
        long_copy(kind, layer, slot, 0).start()
        short_copy(kind, layer, slot, 0).start()

    def chain_step(kind, layer, slot, step):
        j, half, k, _ = stream(kind, layer, slot)
        sign = sign_of(slot)
        before = both_of(kind, layer, slot, step - 1)
        before.wait_recv()
        ring[kind][k, step - 1] = ring[kind][k, step - 1] + chunk(kind, layer, j, half, sign * (4 - step))[...]
        if step < 3:
            ring[kind][k, 3 + step] = ring[kind][k, 3 + step] + chunk(kind, layer, j, half, sign * (step - 3))[...]
        before.wait_send()
        long_copy(kind, layer, slot, step).start()
        if step < 3:
            short_copy(kind, layer, slot, step).start()

    def chain_last(kind, layer, slot):
        j, half, k, _ = stream(kind, layer, slot)
        before = long_copy(kind, layer, slot, 3)
        before.wait_recv()
        before.wait_send()
        return k, ring[kind][k, 3] + chunk(kind, layer, j, half, 0)[...]

    def steps(kind, layer, low, high, step):
        loop(low, high, lambda slot: chain_step(kind, layer, slot, step))

    def starts(kind, layer, low, high):
        loop(low, high, lambda slot: chain_start(kind, layer, slot))

    def z_last(layer):
        def act(slot):
            k, value = chain_last(Z, layer, slot)
            ring_z[k, 3] = value + ring_z[k, 6]
        loop(0, 8, act)

    def y_copy(layer, j):
        return remote(
            part_y.at[layer, j, pl.ds(half_rows, half_rows), :], y_relay.at[layer, j],
            y_send.at[0], y_mid.at[layer, j // 2], y_next(sign_of(j)),
        )

    def y_pass(layer, j):
        return remote(y_relay.at[layer, j], y_got.at[layer, j], y_send.at[1], y_end.at[layer, j // 2], y_next(sign_of(j)))

    def pair(layer, p, sems):
        two = y_relay.at[layer, 2 * p : 2 * p + 2]
        return remote(two, two, y_send.at[1], sems.at[layer, p], mate)

    def y_forward(layer, p):
        pair(layer, p, y_mid).wait_recv()
        loop(2 * p, 2 * p + 2, lambda j: y_pass(layer, j).start())

    groups = ((4, -3), (3, -2), (2, -1), (1,), (0,))

    def unit_rows(away):
        return pl.ds(pl.multiple_of(lax.rem(z + away + NZ, NZ) * unit, unit), unit)

    def y_first(layer, j, at_rows, sign, part_of, g):
        others = pl.ds(pl.multiple_of(half_rows + at_rows.start, unit), unit)
        return remote(
            part_y.at[layer, j, others, :], y_relay.at[layer, j, at_rows, :], y_send.at[0], y_parts.at[part_of], y_next(sign)
        )

    def y_second(layer, j, at_rows, sign, part_of, g):
        return remote(
            y_relay.at[layer, j, at_rows, :], y_got.at[layer, j, at_rows, :], y_send.at[1], y_unit.at[g], y_next(sign)
        )

    def y_units(layer, p, hop, part_of, which):
        for g in which:
            for away in groups[g]:
                def act(j):
                    sign = sign_of(j)
                    hop(layer, j, unit_rows(sign * away), sign, part_of, g).start()
                loop(2 * p, 2 * p + 2, act)

    def y_units_wait(layer, p, part_of, units):
        these = y_relay.at[layer, 2 * p : 2 * p + 2, 0 : unit * units, :]
        remote(these, these, y_send.at[0], y_parts.at[part_of], mate).wait_recv()

    def y_units_add(layer, p, g):
        four = y_got.at[layer, 2 * p : 2 * p + 2, 0 : unit * len(groups[g]), :]
        remote(four, four, y_send.at[1], y_unit.at[g], mate).wait_recv()
        for away in groups[g]:
            def act(j):
                at_rows = unit_rows(sign_of(j) * away)
                part_y[layer, j, at_rows, :] = part_y[layer, j, at_rows, :] + y_got[layer, j, at_rows, :]
            loop(2 * p, 2 * p + 2, act)

    def y_begin(layer, p):
        pair(layer, p, y_end).wait_recv()

        def act(j):
            part_y[layer, j, 0:half_rows, :] = part_y[layer, j, 0:half_rows, :] + y_got[layer, j]
            chain_start(Y, layer, j)
        loop(2 * p, 2 * p + 2, act)

    def z_copy(layer, j):
        return remote(
            ring_z.at[layer * 8 + j * 2 + 1, 3], z_relay.at[layer, j], z_send.at[0], z_mid.at[layer], y_next(sign_of(j))
        )

    def z_pass(layer, j):
        return remote(z_relay.at[layer, j], z_got.at[layer, j], z_send.at[1], z_end_sem.at[layer], y_next(sign_of(j)))

    def z_all(layer, sems):
        return remote(z_relay.at[layer], z_got.at[layer], z_send.at[1], sems.at[layer], mate)

    def z_forward(layer):
        z_all(layer, z_mid).wait_recv()
        loop(0, BLOCKS, lambda j: z_pass(layer, j).start())

    def gcols(side, kind, j):
        return pl.ds(pl.multiple_of(side * half_cols + first_col[kind] + j * width[kind], 128), width[kind])

    def finish(kind, layer, j, k, value):
        ring[kind][k, 3] = value
        src = ring[kind].at[k, 3, pl.ds(pl.multiple_of((1 - core) * own_rows, own_rows), own_rows), :]
        remote(src, gbuf.at[layer, :, gcols(core, kind, j)], g_sem.at[0], g_sem.at[1], mate).start()
        mine = ring[kind][k, 3, pl.ds(pl.multiple_of(core * own_rows, own_rows), own_rows), :]
        gbuf[layer, :, gcols(core, kind, j)] = mine
        squares = value * value
        folded = squares[0:own_rows] + squares[own_rows : 2 * own_rows]
        total = folded[:, 0:128]
        for i in range(1, width[kind] // 128):
            total = total + folded[:, i * 128 : (i + 1) * 128]
        q_acc[layer] = q_acc[layer] + total

    def z_finish(layer):
        z_all(layer, z_end_sem).wait_recv()

        def act(j):
            k = layer * 8 + j * 2
            finish(Z, layer, j, k, ring_z[k, 3] + z_got[layer, j])
        loop(0, BLOCKS, act)

    def y_finish(layer, low, high):
        def act(j):
            k, value = chain_last(Y, layer, j)
            finish(Y, layer, j, k, value + ring_y[k, 6])
        loop(low, high, act)

    def q_copy(offset):
        return remote(q_own, q_got.at[offset - 1], q_sem.at[0], q_sem.at[1], group_device(offset))

    def all_of(got, sems):
        return remote(got, got, sems.at[0], sems.at[1], mate)

    def to_y(layer, j):
        multiply(layer, Y, j)
        y_copy(layer, j).start()

    def to_z(j):
        multiply(0, Z, j)
        chain_start(Z, 0, 2 * j)
        chain_start(Z, 0, 2 * j + 1)

    og_copy(0, 0, Y).wait()
    loop(0, 2, lambda j: to_y(0, j))
    og_copy(0, 0, Z).wait()
    loop(0, 4, to_z)
    loop(2, 4, lambda j: to_y(0, j))

    for which, kind in ((1, Y), (1, Z), (0, Y), (0, Z)):
        og_copy(1, which, kind).start()
    in_copies[1].wait()
    c_own[0] = jnp.zeros_like(c_own[0])
    c_own[0, :, 0:8] = counts[:, 0, :].astype(jnp.float32)
    c_copies[0].start()
    q_acc[...] = jnp.zeros_like(q_acc)
    for kind in (Y, Z):
        x_all(0, kind).wait_send()
        og_copy(1, 1, kind).wait()
        swap(1, kind, 0, 4)
    in_copies[2].start()
    in_copies[3].start()
    og_copy(1, 0, Y).wait()
    og_copy(1, 0, Z).wait()

    steps(Z, 0, 0, 8, 1)
    a_join(1)
    x_all(1, Y).wait_recv()
    loop(0, 2, lambda j: to_y(1, j))
    x_all(1, Z).wait_recv()
    loop(0, 4, lambda j: multiply(1, Z, j))
    steps(Z, 0, 0, 8, 2)
    y_forward(0, 0)
    loop(2, 4, lambda j: multiply(1, Y, j))
    steps(Z, 0, 0, 8, 3)
    starts(Z, 1, 0, 8)
    y_forward(0, 1)
    z_last(0)
    c_next(0)
    steps(Z, 1, 0, 8, 1)
    y_forward(1, 0)
    y_units(1, 1, y_first, 0, (0, 1))
    y_units(1, 1, y_first, 1, (2, 3, 4))
    steps(Z, 1, 0, 8, 2)
    c_next(1)
    steps(Z, 1, 0, 8, 3)

    y_begin(0, 0)
    y_begin(0, 1)
    z_last(1)
    steps(Y, 0, 0, 4, 1)
    steps(Y, 0, 0, 2, 2)
    y_begin(1, 0)
    steps(Y, 0, 2, 4, 2)
    y_units_wait(1, 1, 0, 4)
    y_units(1, 1, y_second, 0, (0, 1))
    steps(Y, 1, 0, 2, 1)
    steps(Y, 0, 0, 4, 3)
    y_units_wait(1, 1, 1, 4)
    y_units(1, 1, y_second, 0, (2,))
    for layer in range(LAYERS):
        loop(0, BLOCKS, lambda j: z_copy(layer, j).start())
    y_units(1, 1, y_second, 0, (3, 4))

    y_units_add(1, 1, 0)
    starts(Y, 1, 2, 4)
    y_finish(0, 0, 4)
    steps(Y, 1, 0, 2, 2)
    y_units_add(1, 1, 1)
    steps(Y, 1, 2, 4, 1)
    steps(Y, 1, 0, 2, 3)
    y_units_add(1, 1, 2)
    steps(Y, 1, 2, 4, 2)
    c_next(2)
    z_forward(0)
    z_forward(1)
    y_finish(1, 0, 2)
    y_units_add(1, 1, 3)
    steps(Y, 1, 2, 4, 3)
    y_units_add(1, 1, 4)
    z_finish(0)
    z_finish(1)
    y_finish(1, 2, 4)

    q_own[0:2] = jnp.sum(q_acc[...], axis=1)
    q_own[2:4] = c_own[3]
    for away in (4, 3, 5, 2, 6, 1, 7):
        loop(away * 4, away * 4 + 4, lambda offset: q_copy(offset).start())
    loop(1, 4, lambda offset: q_copy(offset).start())

    landed = gbuf.at[:, :, 0:half_cols]
    all_g = remote(landed, landed, g_sem.at[0], g_sem.at[1], mate)
    all_g.wait_recv()
    in_copies[2].wait()
    in_copies[3].wait()

    all_g.wait_send()
    for i in range(2):
        remote(y_relay, y_got, y_send.at[i], y_unit.at[0], mate).wait_send()
        remote(z_relay, z_got, z_send.at[i], z_mid.at[0], mate).wait_send()
    for kind in (Z, Y):
        x_all(1, kind).wait_send()
    for layer in range(LAYERS):
        a_copy(layer).wait_send()
    for copy in c_copies:
        copy.wait_send()
    all_of(q_got, q_sem).wait_send()

    all_of(q_got, q_sem).wait_recv()
    sums = q_own[...] + jnp.sum(q_got[...], axis=0)
    root_mean = jnp.sqrt(jnp.sum(sums[0:2], axis=1, keepdims=True) / float(rows * 2 * half_cols))
    totals = sums[2:4]
    lanes = lax.broadcasted_iota(jnp.int32, totals.shape, 1)
    mean_load = jnp.sum(totals, axis=1, keepdims=True) / 8.0
    own_load = jnp.sum(jnp.where(lanes == me_expert, totals, 0.0), axis=1, keepdims=True)
    factor = step_size * (own_load / mean_load) * clip_level / jnp.maximum(root_mean, clip_level)
    beta = own_load / (own_load + mean_load)
    for layer in range(LAYERS):
        this_factor = jnp.broadcast_to(factor[layer : layer + 1], (own_rows, 128))
        this_beta = jnp.broadcast_to(beta[layer : layer + 1], (own_rows, 128))

        def update(i):
            for n in range(8):
                cols = pl.ds(pl.multiple_of(i * 1024 + n * 128, 128), 128)
                updated = w_in[layer, 0, :, cols] - this_factor * gbuf[layer, :, cols]
                new_weights[layer, 0, :, cols] = updated
                previous = s_in[layer, 0, :, cols]
                new_shadow[layer, 0, :, cols] = previous + this_beta * (updated - previous)
        loop(0, 2 * half_cols // 1024, update)


def writer(updated, smoothed, new_weights, new_shadow, sems):
    copies = [
        pltpu.make_async_copy(src.at[layer], dst.at[layer], sems.at[i, layer])
        for i, (src, dst) in enumerate(((updated, new_weights), (smoothed, new_shadow)))
        for layer in range(LAYERS)
    ]
    for copy in copies:
        copy.start()
    for copy in copies:
        copy.wait()


def on_device(activations, out_grads, weights, shadow, counts):
    acts, og = activations[:, 0], out_grads[:, 0]
    tokens, rows = acts.shape[1:]
    ff = og.shape[2]
    unit = rows // 2 // NZ
    half = rows // 2
    tiles = ff // 2 // 128 // BLOCKS
    wide_z, wide_y = (tiles * 3 // 7) * 128, (tiles - tiles * 3 // 7) * 128
    f32, bf16 = jnp.float32, jnp.bfloat16
    dma = pltpu.SemaphoreType.DMA
    vmem = pl.BlockSpec(memory_space=pltpu.VMEM)
    hbm = pl.BlockSpec(memory_space=pl.ANY)
    updated, smoothed = pl.pallas_call(
        kernel,
        out_shape=(pltpu.VMEM(weights.shape, f32), pltpu.VMEM(shadow.shape, f32)),
        in_specs=[hbm] * 5,
        out_specs=(vmem, vmem),
        scratch_shapes=[
            pltpu.VMEM((LAYERS, BLOCKS, rows, wide_z), f32),
            pltpu.VMEM((LAYERS, BLOCKS, rows, wide_y), f32),
            pltpu.VMEM((LAYERS * 8, NZ - 1, unit, wide_z), f32),
            pltpu.VMEM((LAYERS * 4, NZ - 1, unit, wide_y), f32),
            pltpu.VMEM((LAYERS, BLOCKS, half, wide_y), f32),
            pltpu.VMEM((LAYERS, BLOCKS, half, wide_y), f32),
            pltpu.VMEM((LAYERS, BLOCKS, unit, wide_z), f32),
            pltpu.VMEM((LAYERS, BLOCKS, unit, wide_z), f32),
            pltpu.VMEM((LAYERS, BLOCKS, tokens, wide_z), f32),
            pltpu.VMEM((LAYERS, BLOCKS, tokens, wide_y), f32),
            pltpu.VMEM((BLOCKS, tokens, wide_z), f32),
            pltpu.VMEM((BLOCKS, tokens, wide_y), f32),
            pltpu.VMEM((LAYERS, tokens, ff // 2), bf16),
            pltpu.VMEM((LAYERS, tokens, ff // 2), bf16),
            pltpu.VMEM(acts.shape, bf16),
            pltpu.VMEM(counts.shape, counts.dtype),
            pltpu.VMEM(weights.shape, f32),
            pltpu.VMEM(shadow.shape, f32),
            pltpu.VMEM((LAYERS, tokens, rows), f32),
            pltpu.VMEM((LAYERS, tokens, rows), f32),
            pltpu.VMEM((rows, 2 * tokens), f32),
            pltpu.VMEM((LAYERS, rows, 2 * tokens), bf16),
            pltpu.VMEM((LAYERS, unit // 2, ff), f32),
            pltpu.VMEM((4, LAYERS, 128), f32),
            pltpu.VMEM((3, LAYERS, 128), f32),
            pltpu.VMEM((2 * LAYERS, 128), f32),
            pltpu.VMEM((31, 2 * LAYERS, 128), f32),
            pltpu.VMEM((LAYERS, unit // 2, 128), f32),
            dma((LAYERS, 2, 2)),
            dma((4,)),
            dma((2,)),
            dma((2, BLOCKS)),
            dma((2,)),
            dma((2, LAYERS)),
            dma((16,)),
            dma((16, 2)),
            dma((2,)),
            dma((LAYERS, 2)),
            dma((LAYERS, 2)),
            dma((2,)),
            dma((5,)),
            dma((2,)),
            dma((LAYERS,)),
            dma((LAYERS,)),
            dma((2,)),
            dma((2, 3)),
            dma((2,)),
        ],
        compiler_params=pltpu.CompilerParams(
            collective_id=0, has_side_effects=True, vmem_limit_bytes=58 * 1024 * 1024
        ),
    )(acts, og, counts, weights, shadow)
    return pl.pallas_call(
        writer,
        out_shape=(jax.ShapeDtypeStruct(weights.shape, f32), jax.ShapeDtypeStruct(shadow.shape, f32)),
        in_specs=[vmem, vmem],
        out_specs=(hbm, hbm),
        scratch_shapes=[dma((2, LAYERS))],
    )(*(pltpu.with_memory_space_constraint(a, pltpu.VMEM) for a in (updated, smoothed)))


def solution(mesh):
    split = Mesh(
        mesh.devices.reshape(mesh.shape["dp"], 4, 2, 2, 2),
        ("dp", "expert_0", "expert_1", "shard_0", "shard_1"),
    )
    return jax.shard_map(
        on_device,
        mesh=split,
        in_specs=(
            P(None, EXPERT, DP_SHARD, None),
            P(None, EXPERT, DP_SHARD, None),
            P(None, EXPERT, DP_SHARD, None),
            P(None, EXPERT, DP_SHARD, None),
            P(None, DP_EXPERT_SHARD, None),
        ),
        out_specs=(P(None, EXPERT, DP_SHARD, None), P(None, EXPERT, DP_SHARD, None)),
        check_vma=False,
    )
```

```python
import jax
import jax.numpy as jnp
from jax import lax
from jax.experimental import pallas as pl
from jax.experimental.pallas import tpu as pltpu
from jax.sharding import Mesh
from jax.sharding import PartitionSpec as P

MESH = pl.DeviceIdType.MESH
LAYERS = 2
EXPERT = ("expert_0", "expert_1")
DP_EXPERT_SHARD = ("dp", "expert_0", "expert_1", "shard_0", "shard_1")
DP_SHARD = ("dp", "shard_0", "shard_1")

step_size = 0.5
clip_level = 1.0

NZ = 8
BLOCKS = 4
Z, Y, YH = 0, 1, 2


def kernel(
    acts_in, og, counts_in, weights, shadow, new_weights, new_shadow,
    part_z, part_y, ring_z, ring_y, y_got, y_relay, z_got, z_relay, x_got_z, x_got_y, x_out_z, x_out_y,
    own_half, other_half, acts, counts, w_in, s_in, a_out, a_got, a_rows, a_t, gbuf, c_own, c_got, q_own, q_got, q_acc,
    og_sem, in_sem, x_send, x_recv, x_recv_late, a_sem, ring_send, ring_recv,
    y_send, y_mid, y_end, y_parts, y_unit, z_send, z_mid, z_end_sem, g_sem, c_sem, q_sem,
):
    z = lax.axis_index("dp")
    x = lax.axis_index("expert_0")
    y_lo = lax.axis_index("expert_1")
    y_hi = lax.axis_index("shard_0")
    core = lax.axis_index("shard_1")
    y = y_hi * 2 + y_lo
    tokens = acts.shape[1]
    rows = acts.shape[2]
    half_rows = rows // 2
    unit = half_rows // NZ
    own_rows = unit // 2
    part = (part_z, part_y, part_y)
    ring = (ring_z, ring_y, ring_y)
    x_got = (x_got_z, x_got_y)
    x_out = (x_out_z, x_out_y)
    width = (part_z.shape[-1], part_y.shape[-1], part_y.shape[-1] // 2)
    first_col = (0, BLOCKS * width[Z])
    half_cols = BLOCKS * (width[Z] + width[Y])

    def at(z=z, x=x, y_lo=y_lo, y_hi=y_hi, core=core):
        return (z, x, y_lo, y_hi, core)

    def z_next(sign):
        return at(z=lax.rem(z + sign + NZ, NZ))

    def y_next(sign):
        to = lax.rem(y + sign + 4, 4)
        return at(y_lo=lax.rem(to, 2), y_hi=to // 2)

    mate = at(core=1 - core)
    me_group = z * 4 + y_hi * 2 + core
    me_expert = x * 2 + y_lo

    def group_device(offset):
        to = lax.rem(me_group + offset, 32)
        return at(z=to // 4, y_hi=lax.rem(to // 2, 2), core=lax.rem(to, 2))

    def remote(src, dst, send, recv, device):
        return pltpu.make_async_remote_copy(
            src_ref=src, dst_ref=dst, send_sem=send, recv_sem=recv, device_id=device, device_id_type=MESH
        )

    def loop(low, high, act):
        def body(i, _):
            act(i)
            return 0
        lax.fori_loop(low, high, body, 0)

    pieces = ((0, 4 * width[Z]), (first_col[Y], 2 * width[Y]), (first_col[Y] + 2 * width[Y], 2 * width[Y]))

    def og_copy(layer, which, piece):
        first = core if which == 0 else 1 - core
        to = own_half if which == 0 else other_half
        begin, size = pieces[piece]
        cols = pl.ds(pl.multiple_of(first * half_cols + begin, 128), size)
        return pltpu.make_async_copy(
            og.at[layer, :, cols], to.at[layer, :, begin : begin + size], og_sem.at[layer, which, piece]
        )

    in_copies = [
        pltpu.make_async_copy(src, dst, in_sem.at[i])
        for i, (src, dst) in enumerate(((acts_in, acts), (counts_in, counts), (weights, w_in), (shadow, s_in)))
    ]

    barrier = pltpu.get_barrier_semaphore()
    near = (
        mate, z_next(1), z_next(-1), y_next(1), y_next(-1), at(x=x + 1 - 2 * lax.rem(x, 2)), at(x=3 - x)
    )
    for device in near:
        pl.semaphore_signal(barrier, inc=1, device_id=device, device_id_type=MESH)

    og_copy(0, 1, 1).start()
    in_copies[0].start()
    for which, piece in ((0, 1), (1, 0), (0, 0), (1, 2), (0, 2)):
        og_copy(0, which, piece).start()
    in_copies[1].start()

    def cols_of(kind, j):
        return pl.ds(pl.multiple_of(first_col[kind] + j * width[kind], 128), width[kind])

    def convert(layer, kind, j):
        x_out[kind][j] = other_half[layer, :, cols_of(kind, j)].astype(jnp.float32)

    def x_copy(layer, kind, j):
        sem = x_recv.at[4 * kind + j] if layer == 0 else x_recv_late.at[kind]
        return remote(x_out[kind].at[j], x_got[kind].at[layer, j], x_send.at[kind], sem, mate)

    def half_cols_of(h):
        return pl.ds(h * width[YH], width[YH])

    def x_half(j, h):
        cols = half_cols_of(h)
        return remote(x_out_y.at[j, :, cols], x_got_y.at[0, j, :, cols], x_send.at[Y], x_recv.at[4 + j + 4 * h], mate)

    def x_all(layer, kind):
        return remote(x_out[kind], x_got[kind].at[layer], x_send.at[kind], x_recv_late.at[kind], mate)

    def a_copy(layer):
        return remote(a_out.at[layer], a_got.at[layer], a_sem.at[0, layer], a_sem.at[1, layer], mate)

    def a_join(layer):
        a_rows[:, 0:tokens] = a_out[layer].T
        a_copy(layer).wait_recv()
        a_rows[:, tokens : 2 * tokens] = a_got[layer].T
        for half in range(2):
            side = y_hi if half == 0 else 1 - y_hi
            for zz in range(NZ):
                piece = a_rows[pl.ds(pl.multiple_of(zz * 2 * unit + side * unit, unit), unit), :]
                a_t[layer, half * half_rows + zz * unit : half * half_rows + (zz + 1) * unit, :] = piece.astype(jnp.bfloat16)

    def swap(layer, kind, low, high):
        def act(j):
            convert(layer, kind, j)
            x_copy(layer, kind, j).start()
        loop(low, high, act)

    c_copies = [
        remote(c_own.at[i], c_got.at[i], c_sem.at[0, i], c_sem.at[1, i], device)
        for i, device in enumerate((near[5], near[6], at(y_lo=1 - y_lo)))
    ]

    def c_next(i):
        c_copies[i].wait_recv()
        c_own[i + 1] = c_own[i] + c_got[i]
        if i < 2:
            c_copies[i + 1].start()

    og_copy(0, 1, 1).wait()
    loop(0, 2, lambda j: convert(0, Y, j))
    in_copies[0].wait()
    a_out[...] = acts[...].astype(jnp.float32)
    pl.semaphore_wait(barrier, len(near))

    a_copy(0).start()
    loop(0, 2, lambda j: x_half(j, 0).start())
    og_copy(0, 1, 0).wait()
    swap(0, Z, 0, 2)
    loop(0, 2, lambda j: x_half(j, 1).start())
    swap(0, Z, 2, 4)
    og_copy(0, 1, 2).wait()
    swap(0, Y, 2, 4)
    a_copy(1).start()
    a_join(0)

    def multiply(layer, kind, j):
        if layer == 0:
            x_copy(layer, kind, j).wait_recv()
        theirs = x_got[kind][layer, j].astype(jnp.bfloat16)
        both = jnp.concatenate([own_half[layer, :, cols_of(kind, j)], theirs], axis=0)
        part[kind][layer, j] = jnp.dot(a_t[layer], both, preferred_element_type=jnp.float32)

    def stream(kind, layer, slot):
        full = pl.ds(0, width[kind])
        if kind == Z:
            return slot // 2, lax.rem(slot, 2), layer * 8 + slot, layer * 8 + slot, full
        if kind == Y:
            return slot, 0, layer * 4 + slot, layer * 4 + slot, full
        j = 2 + lax.rem(slot, 2)
        cols = pl.ds(pl.multiple_of(slot // 2 * width[YH], 128), width[YH])
        return j, 0, layer * 4 + j, layer * 4 + 2 + slot, cols

    def sign_of(slot):
        return 1 - 2 * lax.rem(slot, 2)

    def chunk(kind, layer, slot, away):
        j, half, _, _, cols = stream(kind, layer, slot)
        index = lax.rem(z + away + NZ, NZ)
        return part[kind].at[layer, j, pl.ds(pl.multiple_of(half * half_rows + index * unit, unit), unit), cols]

    def long_copy(kind, layer, slot, step):
        _, _, k, sem, cols = stream(kind, layer, slot)
        sign = sign_of(slot)
        src = chunk(kind, layer, slot, sign * 4) if step == 0 else ring[kind].at[k, step - 1, :, cols]
        dst = ring[kind].at[k, step, :, cols]
        return remote(src, dst, ring_send.at[min(kind, Y)], ring_recv.at[sem, step % 2], z_next(sign))

    def short_copy(kind, layer, slot, step):
        _, _, k, sem, cols = stream(kind, layer, slot)
        sign = sign_of(slot)
        src = chunk(kind, layer, slot, sign * -3) if step == 0 else ring[kind].at[k, 3 + step, :, cols]
        dst = ring[kind].at[k, 4 + step, :, cols]
        return remote(src, dst, ring_send.at[min(kind, Y)], ring_recv.at[sem, step % 2], z_next(-sign))

    def both_of(kind, layer, slot, step):
        _, _, k, sem, cols = stream(kind, layer, slot)
        two = ring[kind].at[k, 0:2, :, cols]
        return remote(two, two, ring_send.at[min(kind, Y)], ring_recv.at[sem, step % 2], z_next(1))

    def chain_start(kind, layer, slot):
        long_copy(kind, layer, slot, 0).start()
        short_copy(kind, layer, slot, 0).start()

    def chain_step(kind, layer, slot, step):
        _, _, k, _, cols = stream(kind, layer, slot)
        held = ring[kind]
        sign = sign_of(slot)
        both_of(kind, layer, slot, step - 1).wait_recv()
        held[k, step - 1, :, cols] = held[k, step - 1, :, cols] + chunk(kind, layer, slot, sign * (4 - step))[...]
        if step < 3:
            held[k, 3 + step, :, cols] = held[k, 3 + step, :, cols] + chunk(kind, layer, slot, sign * (step - 3))[...]
        long_copy(kind, layer, slot, step).start()
        if step < 3:
            short_copy(kind, layer, slot, step).start()

    def chain_last(kind, layer, slot):
        _, _, k, _, cols = stream(kind, layer, slot)
        long_copy(kind, layer, slot, 3).wait_recv()
        return ring[kind][k, 3, :, cols] + chunk(kind, layer, slot, 0)[...] + ring[kind][k, 6, :, cols]

    def steps(kind, layer, low, high, step):
        loop(low, high, lambda slot: chain_step(kind, layer, slot, step))

    def starts(kind, layer, low, high):
        loop(low, high, lambda slot: chain_start(kind, layer, slot))

    def z_last(layer):
        def act(slot):
            ring_z[layer * 8 + slot, 3] = chain_last(Z, layer, slot)
        loop(0, 8, act)

    def y_copy(layer, j):
        return remote(
            part_y.at[layer, j, pl.ds(half_rows, half_rows), :], y_relay.at[layer, j],
            y_send.at[0], y_mid.at[layer, j // 2], y_next(sign_of(j)),
        )

    def y_pass(layer, j):
        return remote(y_relay.at[layer, j], y_got.at[layer, j], y_send.at[1], y_end.at[layer, j // 2], y_next(sign_of(j)))

    def pair(layer, p, sems):
        two = y_relay.at[layer, 2 * p : 2 * p + 2]
        return remote(two, two, y_send.at[1], sems.at[layer, p], mate)

    def y_forward(layer, p):
        pair(layer, p, y_mid).wait_recv()
        loop(2 * p, 2 * p + 2, lambda j: y_pass(layer, j).start())

    groups = ((4, -3), (3, -2), (2, -1), (1,), (0,))

    def unit_rows(away):
        return pl.ds(pl.multiple_of(lax.rem(z + away + NZ, NZ) * unit, unit), unit)

    def y_first(layer, j, at_rows, sign, part_of, g):
        others = pl.ds(pl.multiple_of(half_rows + at_rows.start, unit), unit)
        return remote(
            part_y.at[layer, j, others, :], y_relay.at[layer, j, at_rows, :], y_send.at[0], y_parts.at[part_of], y_next(sign)
        )

    def y_second(layer, j, at_rows, sign, part_of, g):
        return remote(
            y_relay.at[layer, j, at_rows, :], y_got.at[layer, j, at_rows, :], y_send.at[1], y_unit.at[g], y_next(sign)
        )

    def y_units(layer, p, hop, part_of, which):
        for g in which:
            for away in groups[g]:
                def act(j):
                    sign = sign_of(j)
                    hop(layer, j, unit_rows(sign * away), sign, part_of, g).start()
                loop(2 * p, 2 * p + 2, act)

    def y_units_wait(layer, p, part_of, units):
        these = y_relay.at[layer, 2 * p : 2 * p + 2, 0 : unit * units, :]
        remote(these, these, y_send.at[0], y_parts.at[part_of], mate).wait_recv()

    def y_units_add(layer, p, g):
        four = y_got.at[layer, 2 * p : 2 * p + 2, 0 : unit * len(groups[g]), :]
        remote(four, four, y_send.at[1], y_unit.at[g], mate).wait_recv()
        for away in groups[g]:
            def act(j):
                at_rows = unit_rows(sign_of(j) * away)
                part_y[layer, j, at_rows, :] = part_y[layer, j, at_rows, :] + y_got[layer, j, at_rows, :]
            loop(2 * p, 2 * p + 2, act)

    def y_begin(layer, p):
        pair(layer, p, y_end).wait_recv()

        def act(j):
            part_y[layer, j, 0:half_rows, :] = part_y[layer, j, 0:half_rows, :] + y_got[layer, j]
            chain_start(Y, layer, j)
        loop(2 * p, 2 * p + 2, act)

    def z_copy(layer, j):
        return remote(
            ring_z.at[layer * 8 + j * 2 + 1, 3], z_relay.at[layer, j], z_send.at[0], z_mid.at[layer], y_next(sign_of(j))
        )

    def z_pass(layer, j):
        return remote(z_relay.at[layer, j], z_got.at[layer, j], z_send.at[1], z_end_sem.at[layer], y_next(sign_of(j)))

    def z_all(layer, sems):
        return remote(z_relay.at[layer], z_got.at[layer], z_send.at[1], sems.at[layer], mate)

    def z_forward(layer):
        z_all(layer, z_mid).wait_recv()
        loop(0, BLOCKS, lambda j: z_pass(layer, j).start())

    def finish(kind, layer, slot, value):
        j, _, k, _, cols = stream(kind, layer, slot)
        held = ring[kind]
        held[k, 3, :, cols] = value
        col = core * half_cols + first_col[min(kind, Y)] + j * width[min(kind, Y)] + cols.start
        where = pl.ds(pl.multiple_of(col, 128), width[kind])

        def of(c):
            return pl.ds(pl.multiple_of(c * own_rows, own_rows), own_rows)

        remote(
            held.at[k, 3, of(1 - core), cols], gbuf.at[layer, :, where], g_sem.at[0], g_sem.at[1], mate
        ).start()
        gbuf[layer, :, where] = held[k, 3, of(core), cols]
        squares = value * value
        folded = squares[0:own_rows] + squares[own_rows : 2 * own_rows]
        total = folded[:, 0:128]
        for i in range(1, width[kind] // 128):
            total = total + folded[:, i * 128 : (i + 1) * 128]
        q_acc[layer] = q_acc[layer] + total

    def z_finish(layer):
        z_all(layer, z_end_sem).wait_recv()
        loop(0, BLOCKS, lambda j: finish(Z, layer, 2 * j, ring_z[layer * 8 + 2 * j, 3] + z_got[layer, j]))

    def y_finish(layer, low, high, kind=Y):
        loop(low, high, lambda slot: finish(kind, layer, slot, chain_last(kind, layer, slot)))

    def q_copy(offset):
        return remote(q_own, q_got.at[offset - 1], q_sem.at[0], q_sem.at[1], group_device(offset))

    def all_of(got, sems):
        return remote(got, got, sems.at[0], sems.at[1], mate)

    def to_y(layer, j):
        multiply(layer, Y, j)
        y_copy(layer, j).start()

    def to_z(j):
        multiply(0, Z, j)
        chain_start(Z, 0, 2 * j)
        chain_start(Z, 0, 2 * j + 1)

    def to_y_half(j, h):
        cols = half_cols_of(h)
        x_half(j, h).wait_recv()
        mine = own_half[0, :, pl.ds(pl.multiple_of(first_col[Y] + j * width[Y] + h * width[YH], 128), width[YH])]
        both = jnp.concatenate([mine, x_got_y[0, j, :, cols].astype(jnp.bfloat16)], axis=0)
        part_y[0, j, :, cols] = jnp.dot(a_t[0], both, preferred_element_type=jnp.float32)
        remote(
            part_y.at[0, j, pl.ds(half_rows, half_rows), cols], y_relay.at[0, j, :, cols],
            y_send.at[0], y_mid.at[0, 0], y_next(sign_of(j)),
        ).start()

    og_copy(0, 0, 1).wait()
    loop(0, 2, lambda j: to_y_half(j, 0))
    og_copy(0, 0, 0).wait()
    loop(0, 2, to_z)
    loop(0, 2, lambda j: to_y_half(j, 1))
    loop(2, 4, to_z)
    og_copy(0, 0, 2).wait()
    loop(2, 4, lambda j: to_y(0, j))

    for which in (1, 0):
        for piece in (1, 2, 0):
            og_copy(1, which, piece).start()
    in_copies[1].wait()
    c_own[0] = jnp.zeros_like(c_own[0])
    c_own[0, :, 0:8] = counts[:, 0, :].astype(jnp.float32)
    c_copies[0].start()
    q_acc[...] = jnp.zeros_like(q_acc)
    for kind in (Y, Z):
        x_all(0, kind).wait_send()
        for piece in ((0,), (1, 2))[kind]:
            og_copy(1, 1, piece).wait()
        swap(1, kind, 0, 4)
    in_copies[2].start()
    in_copies[3].start()
    for piece in range(3):
        og_copy(1, 0, piece).wait()

    steps(Z, 0, 0, 8, 1)
    a_join(1)
    x_all(1, Y).wait_recv()
    loop(0, 2, lambda j: to_y(1, j))
    x_all(1, Z).wait_recv()
    loop(0, 4, lambda j: multiply(1, Z, j))
    steps(Z, 0, 0, 8, 2)
    y_forward(0, 0)
    loop(2, 4, lambda j: multiply(1, Y, j))
    steps(Z, 0, 0, 8, 3)
    starts(Z, 1, 0, 8)
    y_forward(0, 1)
    z_last(0)
    c_next(0)
    steps(Z, 1, 0, 8, 1)
    y_forward(1, 0)
    y_units(1, 1, y_first, 0, (0, 1))
    y_units(1, 1, y_first, 1, (2, 3, 4))
    steps(Z, 1, 0, 8, 2)
    c_next(1)
    steps(Z, 1, 0, 8, 3)

    y_begin(0, 0)
    y_begin(0, 1)
    z_last(1)
    steps(Y, 0, 0, 4, 1)
    y_begin(1, 0)
    steps(Y, 0, 0, 2, 2)
    y_units_wait(1, 1, 0, 4)
    y_units(1, 1, y_second, 0, (0, 1))
    steps(Y, 1, 0, 2, 1)
    steps(Y, 0, 2, 4, 2)
    y_units_wait(1, 1, 1, 4)
    y_units(1, 1, y_second, 0, (2,))
    for layer in range(LAYERS):
        loop(0, BLOCKS, lambda j: z_copy(layer, j).start())
    y_units(1, 1, y_second, 0, (3, 4))
    steps(Y, 1, 0, 2, 2)

    y_units_add(1, 1, 0)
    starts(YH, 1, 0, 4)
    steps(Y, 0, 0, 2, 3)
    y_units_add(1, 1, 1)
    steps(YH, 1, 0, 4, 1)
    steps(Y, 0, 2, 4, 3)
    steps(Y, 1, 0, 2, 3)
    y_finish(0, 0, 2)
    y_units_add(1, 1, 2)
    steps(YH, 1, 0, 4, 2)
    z_forward(0)
    z_forward(1)
    c_next(2)
    y_units_add(1, 1, 3)
    steps(YH, 1, 0, 4, 3)
    y_finish(0, 2, 4)
    y_finish(1, 0, 2)
    z_finish(0)
    y_units_add(1, 1, 4)
    y_finish(1, 0, 4, YH)
    z_finish(1)

    q_own[0:2] = jnp.sum(q_acc[...], axis=1)
    q_own[2:4] = c_own[3]
    for away in (4, 3, 5, 2, 6, 1, 7):
        loop(away * 4, away * 4 + 4, lambda offset: q_copy(offset).start())
    loop(1, 4, lambda offset: q_copy(offset).start())

    landed = gbuf.at[:, :, 0:half_cols]
    all_g = remote(landed, landed, g_sem.at[0], g_sem.at[1], mate)
    all_g.wait_recv()
    in_copies[2].wait()
    in_copies[3].wait()

    all_g.wait_send()
    for i in range(2):
        remote(y_relay, y_got, y_send.at[i], y_unit.at[0], mate).wait_send()
        remote(z_relay, z_got, z_send.at[i], z_mid.at[0], mate).wait_send()
    for kind in (Z, Y):
        x_all(1, kind).wait_send()
        remote(ring[kind], ring[kind], ring_send.at[kind], ring_recv.at[0, 0], mate).wait_send()
    for layer in range(LAYERS):
        a_copy(layer).wait_send()
    for copy in c_copies:
        copy.wait_send()
    all_of(q_got, q_sem).wait_send()

    all_of(q_got, q_sem).wait_recv()
    sums = q_own[...] + jnp.sum(q_got[...], axis=0)
    root_mean = jnp.sqrt(jnp.sum(sums[0:2], axis=1, keepdims=True) / float(rows * 2 * half_cols))
    totals = sums[2:4]
    lanes = lax.broadcasted_iota(jnp.int32, totals.shape, 1)
    mean_load = jnp.sum(totals, axis=1, keepdims=True) / 8.0
    own_load = jnp.sum(jnp.where(lanes == me_expert, totals, 0.0), axis=1, keepdims=True)
    factor = step_size * (own_load / mean_load) * clip_level / jnp.maximum(root_mean, clip_level)
    beta = own_load / (own_load + mean_load)
    for layer in range(LAYERS):
        this_factor = jnp.broadcast_to(factor[layer : layer + 1], (own_rows, 128))
        this_beta = jnp.broadcast_to(beta[layer : layer + 1], (own_rows, 128))

        def update(i):
            for n in range(8):
                cols = pl.ds(pl.multiple_of(i * 1024 + n * 128, 128), 128)
                updated = w_in[layer, 0, :, cols] - this_factor * gbuf[layer, :, cols]
                new_weights[layer, 0, :, cols] = updated
                previous = s_in[layer, 0, :, cols]
                new_shadow[layer, 0, :, cols] = previous + this_beta * (updated - previous)
        loop(0, 2 * half_cols // 1024, update)


def writer(updated, smoothed, new_weights, new_shadow, sems):
    copies = [
        pltpu.make_async_copy(src.at[layer], dst.at[layer], sems.at[i, layer])
        for i, (src, dst) in enumerate(((updated, new_weights), (smoothed, new_shadow)))
        for layer in range(LAYERS)
    ]
    for copy in copies:
        copy.start()
    for copy in copies:
        copy.wait()


def on_device(activations, out_grads, weights, shadow, counts):
    acts, og = activations[:, 0], out_grads[:, 0]
    tokens, rows = acts.shape[1:]
    ff = og.shape[2]
    unit = rows // 2 // NZ
    half = rows // 2
    tiles = ff // 2 // 128 // BLOCKS
    wide_z, wide_y = (tiles * 3 // 7) * 128, (tiles - tiles * 3 // 7) * 128
    f32, bf16 = jnp.float32, jnp.bfloat16
    dma = pltpu.SemaphoreType.DMA
    vmem = pl.BlockSpec(memory_space=pltpu.VMEM)
    hbm = pl.BlockSpec(memory_space=pl.ANY)
    updated, smoothed = pl.pallas_call(
        kernel,
        out_shape=(pltpu.VMEM(weights.shape, f32), pltpu.VMEM(shadow.shape, f32)),
        in_specs=[hbm] * 5,
        out_specs=(vmem, vmem),
        scratch_shapes=[
            pltpu.VMEM((LAYERS, BLOCKS, rows, wide_z), f32),
            pltpu.VMEM((LAYERS, BLOCKS, rows, wide_y), f32),
            pltpu.VMEM((LAYERS * 8, NZ - 1, unit, wide_z), f32),
            pltpu.VMEM((LAYERS * 4, NZ - 1, unit, wide_y), f32),
            pltpu.VMEM((LAYERS, BLOCKS, half, wide_y), f32),
            pltpu.VMEM((LAYERS, BLOCKS, half, wide_y), f32),
            pltpu.VMEM((LAYERS, BLOCKS, unit, wide_z), f32),
            pltpu.VMEM((LAYERS, BLOCKS, unit, wide_z), f32),
            pltpu.VMEM((LAYERS, BLOCKS, tokens, wide_z), f32),
            pltpu.VMEM((LAYERS, BLOCKS, tokens, wide_y), f32),
            pltpu.VMEM((BLOCKS, tokens, wide_z), f32),
            pltpu.VMEM((BLOCKS, tokens, wide_y), f32),
            pltpu.VMEM((LAYERS, tokens, ff // 2), bf16),
            pltpu.VMEM((LAYERS, tokens, ff // 2), bf16),
            pltpu.VMEM(acts.shape, bf16),
            pltpu.VMEM(counts.shape, counts.dtype),
            pltpu.VMEM(weights.shape, f32),
            pltpu.VMEM(shadow.shape, f32),
            pltpu.VMEM((LAYERS, tokens, rows), f32),
            pltpu.VMEM((LAYERS, tokens, rows), f32),
            pltpu.VMEM((rows, 2 * tokens), f32),
            pltpu.VMEM((LAYERS, rows, 2 * tokens), bf16),
            pltpu.VMEM((LAYERS, unit // 2, ff), f32),
            pltpu.VMEM((4, LAYERS, 128), f32),
            pltpu.VMEM((3, LAYERS, 128), f32),
            pltpu.VMEM((2 * LAYERS, 128), f32),
            pltpu.VMEM((31, 2 * LAYERS, 128), f32),
            pltpu.VMEM((LAYERS, unit // 2, 128), f32),
            dma((LAYERS, 2, 3)),
            dma((4,)),
            dma((2,)),
            dma((10,)),
            dma((2,)),
            dma((2, LAYERS)),
            dma((2,)),
            dma((16, 2)),
            dma((2,)),
            dma((LAYERS, 2)),
            dma((LAYERS, 2)),
            dma((2,)),
            dma((5,)),
            dma((2,)),
            dma((LAYERS,)),
            dma((LAYERS,)),
            dma((2,)),
            dma((2, 3)),
            dma((2,)),
        ],
        compiler_params=pltpu.CompilerParams(
            collective_id=0, has_side_effects=True, vmem_limit_bytes=58 * 1024 * 1024
        ),
    )(acts, og, counts, weights, shadow)
    return pl.pallas_call(
        writer,
        out_shape=(jax.ShapeDtypeStruct(weights.shape, f32), jax.ShapeDtypeStruct(shadow.shape, f32)),
        in_specs=[vmem, vmem],
        out_specs=(hbm, hbm),
        scratch_shapes=[dma((2, LAYERS))],
    )(*(pltpu.with_memory_space_constraint(a, pltpu.VMEM) for a in (updated, smoothed)))


def solution(mesh):
    split = Mesh(
        mesh.devices.reshape(mesh.shape["dp"], 4, 2, 2, 2),
        ("dp", "expert_0", "expert_1", "shard_0", "shard_1"),
    )
    return jax.shard_map(
        on_device,
        mesh=split,
        in_specs=(
            P(None, EXPERT, DP_SHARD, None),
            P(None, EXPERT, DP_SHARD, None),
            P(None, EXPERT, DP_SHARD, None),
            P(None, EXPERT, DP_SHARD, None),
            P(None, DP_EXPERT_SHARD, None),
        ),
        out_specs=(P(None, EXPERT, DP_SHARD, None), P(None, EXPERT, DP_SHARD, None)),
        check_vma=False,
    )
```

```python
import jax
import jax.numpy as jnp
from jax import lax
from jax.experimental import pallas as pl
from jax.experimental.pallas import tpu as pltpu
from jax.sharding import Mesh
from jax.sharding import PartitionSpec as P

MESH = pl.DeviceIdType.MESH
LAYERS = 2
EXPERT = ("expert_0", "expert_1")
DP_EXPERT_SHARD = ("dp", "expert_0", "expert_1", "shard_0", "shard_1")
DP_SHARD = ("dp", "shard_0", "shard_1")

step_size = 0.5
clip_level = 1.0

NZ = 8
BLOCKS = 4
Z, Y, YH = 0, 1, 2


def kernel(
    acts_in, og, counts_in, weights, shadow, new_weights, new_shadow,
    part_z, part_y, ring_z, ring_y, y_got, y_relay, z_got, z_relay, x_got_z, x_got_y, x_out_z, x_out_y,
    own_half, other_half, acts, counts, w_in, s_in, a_out, a_got, a_rows, a_t, gbuf, c_own, c_got, q_own, q_got, q_acc,
    og_sem, in_sem, x_send, x_recv, x_recv_late, a_sem, ring_send, ring_recv,
    y_send, y_mid, y_end, y_parts, y_unit, z_send, z_mid, z_end_sem, g_sem, c_sem, q_sem,
):
    z = lax.axis_index("dp")
    x = lax.axis_index("expert_0")
    y_lo = lax.axis_index("expert_1")
    y_hi = lax.axis_index("shard_0")
    core = lax.axis_index("shard_1")
    y = y_hi * 2 + y_lo
    tokens = acts.shape[1]
    rows = acts.shape[2]
    half_rows = rows // 2
    unit = half_rows // NZ
    own_rows = unit // 2
    part = (part_z, part_y, part_y)
    ring = (ring_z, ring_y, ring_y)
    x_got = (x_got_z, x_got_y)
    x_out = (x_out_z, x_out_y)
    width = (part_z.shape[-1], part_y.shape[-1], part_y.shape[-1] // 2)
    first_col = (0, BLOCKS * width[Z])
    half_cols = BLOCKS * (width[Z] + width[Y])

    def at(z=z, x=x, y_lo=y_lo, y_hi=y_hi, core=core):
        return (z, x, y_lo, y_hi, core)

    def z_next(sign):
        return at(z=lax.rem(z + sign + NZ, NZ))

    def y_next(sign):
        to = lax.rem(y + sign + 4, 4)
        return at(y_lo=lax.rem(to, 2), y_hi=to // 2)

    mate = at(core=1 - core)
    me_group = z * 4 + y_hi * 2 + core
    me_expert = x * 2 + y_lo

    def group_device(offset):
        to = lax.rem(me_group + offset, 32)
        return at(z=to // 4, y_hi=lax.rem(to // 2, 2), core=lax.rem(to, 2))

    def remote(src, dst, send, recv, device):
        return pltpu.make_async_remote_copy(
            src_ref=src, dst_ref=dst, send_sem=send, recv_sem=recv, device_id=device, device_id_type=MESH
        )

    def loop(low, high, act):
        def body(i, _):
            act(i)
            return 0
        lax.fori_loop(low, high, body, 0)

    pieces = ((0, 4 * width[Z]), (first_col[Y], 2 * width[Y]), (first_col[Y] + 2 * width[Y], 2 * width[Y]))

    def og_copy(layer, which, piece):
        first = core if which == 0 else 1 - core
        to = own_half if which == 0 else other_half
        begin, size = pieces[piece]
        cols = pl.ds(pl.multiple_of(first * half_cols + begin, 128), size)
        return pltpu.make_async_copy(
            og.at[layer, :, cols], to.at[layer, :, begin : begin + size], og_sem.at[layer, which, piece]
        )

    in_copies = [
        pltpu.make_async_copy(src, dst, in_sem.at[i])
        for i, (src, dst) in enumerate(((acts_in, acts), (counts_in, counts), (weights, w_in), (shadow, s_in)))
    ]

    barrier = pltpu.get_barrier_semaphore()
    near = (
        mate, z_next(1), z_next(-1), y_next(1), y_next(-1), at(x=x + 1 - 2 * lax.rem(x, 2)), at(x=3 - x)
    )
    for device in near:
        pl.semaphore_signal(barrier, inc=1, device_id=device, device_id_type=MESH)

    og_copy(0, 1, 1).start()
    in_copies[0].start()
    for which, piece in ((0, 1), (1, 0), (0, 0), (1, 2), (0, 2)):
        og_copy(0, which, piece).start()
    in_copies[1].start()

    def cols_of(kind, j):
        return pl.ds(pl.multiple_of(first_col[kind] + j * width[kind], 128), width[kind])

    def convert(layer, kind, j):
        x_out[kind][j] = other_half[layer, :, cols_of(kind, j)].astype(jnp.float32)

    def x_copy(layer, kind, j):
        sem = x_recv.at[4 * kind + j] if layer == 0 else x_recv_late.at[kind]
        return remote(x_out[kind].at[j], x_got[kind].at[layer, j], x_send.at[kind], sem, mate)

    quarter = width[YH] // 2

    def half_cols_of(h):
        return pl.ds(h * quarter, quarter if h == 0 else width[Y] - quarter)

    def x_half(j, h):
        cols = half_cols_of(h)
        return remote(x_out_y.at[j, :, cols], x_got_y.at[0, j, :, cols], x_send.at[Y], x_recv.at[4 + j + 4 * h], mate)

    def x_all(layer, kind):
        return remote(x_out[kind], x_got[kind].at[layer], x_send.at[kind], x_recv_late.at[kind], mate)

    def a_copy(layer):
        return remote(a_out.at[layer], a_got.at[layer], a_sem.at[0, layer], a_sem.at[1, layer], mate)

    def a_join(layer):
        a_rows[:, 0:tokens] = a_out[layer].T
        a_copy(layer).wait_recv()
        a_rows[:, tokens : 2 * tokens] = a_got[layer].T
        for half in range(2):
            side = y_hi if half == 0 else 1 - y_hi
            for zz in range(NZ):
                piece = a_rows[pl.ds(pl.multiple_of(zz * 2 * unit + side * unit, unit), unit), :]
                a_t[layer, half * half_rows + zz * unit : half * half_rows + (zz + 1) * unit, :] = piece.astype(jnp.bfloat16)

    def swap(layer, kind, low, high):
        def act(j):
            convert(layer, kind, j)
            x_copy(layer, kind, j).start()
        loop(low, high, act)

    c_copies = [
        remote(c_own.at[i], c_got.at[i], c_sem.at[0, i], c_sem.at[1, i], device)
        for i, device in enumerate((near[5], near[6], at(y_lo=1 - y_lo)))
    ]

    def c_next(i):
        c_copies[i].wait_recv()
        c_own[i + 1] = c_own[i] + c_got[i]
        if i < 2:
            c_copies[i + 1].start()

    og_copy(0, 1, 1).wait()
    loop(0, 2, lambda j: convert(0, Y, j))
    in_copies[0].wait()
    a_out[...] = acts[...].astype(jnp.float32)
    pl.semaphore_wait(barrier, len(near))

    a_copy(0).start()
    loop(0, 2, lambda j: x_half(j, 0).start())
    og_copy(0, 1, 0).wait()
    swap(0, Z, 0, 2)
    loop(0, 2, lambda j: x_half(j, 1).start())
    swap(0, Z, 2, 4)
    og_copy(0, 1, 2).wait()
    swap(0, Y, 2, 4)
    a_copy(1).start()
    a_join(0)

    def multiply(layer, kind, j):
        if layer == 0:
            x_copy(layer, kind, j).wait_recv()
        theirs = x_got[kind][layer, j].astype(jnp.bfloat16)
        both = jnp.concatenate([own_half[layer, :, cols_of(kind, j)], theirs], axis=0)
        part[kind][layer, j] = jnp.dot(a_t[layer], both, preferred_element_type=jnp.float32)

    def stream(kind, layer, slot):
        full = pl.ds(0, width[kind])
        if kind == Z:
            return slot // 2, lax.rem(slot, 2), layer * 8 + slot, layer * 8 + slot, full
        if kind == Y:
            return slot, 0, layer * 4 + slot, layer * 4 + slot, full
        j = 2 + lax.rem(slot, 2)
        cols = pl.ds(pl.multiple_of(slot // 2 * width[YH], 128), width[YH])
        return j, 0, layer * 4 + j, layer * 4 + 2 + slot, cols

    def sign_of(slot):
        return 1 - 2 * lax.rem(slot, 2)

    def chunk(kind, layer, slot, away):
        j, half, _, _, cols = stream(kind, layer, slot)
        index = lax.rem(z + away + NZ, NZ)
        return part[kind].at[layer, j, pl.ds(pl.multiple_of(half * half_rows + index * unit, unit), unit), cols]

    def long_copy(kind, layer, slot, step):
        _, _, k, sem, cols = stream(kind, layer, slot)
        sign = sign_of(slot)
        src = chunk(kind, layer, slot, sign * 4) if step == 0 else ring[kind].at[k, step - 1, :, cols]
        dst = ring[kind].at[k, step, :, cols]
        return remote(src, dst, ring_send.at[min(kind, Y)], ring_recv.at[sem, step % 2], z_next(sign))

    def short_copy(kind, layer, slot, step):
        _, _, k, sem, cols = stream(kind, layer, slot)
        sign = sign_of(slot)
        src = chunk(kind, layer, slot, sign * -3) if step == 0 else ring[kind].at[k, 3 + step, :, cols]
        dst = ring[kind].at[k, 4 + step, :, cols]
        return remote(src, dst, ring_send.at[min(kind, Y)], ring_recv.at[sem, step % 2], z_next(-sign))

    def both_of(kind, layer, slot, step):
        _, _, k, sem, cols = stream(kind, layer, slot)
        two = ring[kind].at[k, 0:2, :, cols]
        return remote(two, two, ring_send.at[min(kind, Y)], ring_recv.at[sem, step % 2], z_next(1))

    def chain_start(kind, layer, slot):
        long_copy(kind, layer, slot, 0).start()
        short_copy(kind, layer, slot, 0).start()

    def chain_step(kind, layer, slot, step):
        _, _, k, _, cols = stream(kind, layer, slot)
        held = ring[kind]
        sign = sign_of(slot)
        both_of(kind, layer, slot, step - 1).wait_recv()
        held[k, step - 1, :, cols] = held[k, step - 1, :, cols] + chunk(kind, layer, slot, sign * (4 - step))[...]
        if step < 3:
            held[k, 3 + step, :, cols] = held[k, 3 + step, :, cols] + chunk(kind, layer, slot, sign * (step - 3))[...]
        long_copy(kind, layer, slot, step).start()
        if step < 3:
            short_copy(kind, layer, slot, step).start()

    def chain_last(kind, layer, slot):
        _, _, k, _, cols = stream(kind, layer, slot)
        long_copy(kind, layer, slot, 3).wait_recv()
        return ring[kind][k, 3, :, cols] + chunk(kind, layer, slot, 0)[...] + ring[kind][k, 6, :, cols]

    def steps(kind, layer, low, high, step):
        loop(low, high, lambda slot: chain_step(kind, layer, slot, step))

    def starts(kind, layer, low, high):
        loop(low, high, lambda slot: chain_start(kind, layer, slot))

    def z_last(layer):
        def act(slot):
            ring_z[layer * 8 + slot, 3] = chain_last(Z, layer, slot)
        loop(0, 8, act)

    def y_copy(layer, j):
        return remote(
            part_y.at[layer, j, pl.ds(half_rows, half_rows), :], y_relay.at[layer, j],
            y_send.at[0], y_mid.at[layer, j // 2], y_next(sign_of(j)),
        )

    def y_pass(layer, j):
        return remote(y_relay.at[layer, j], y_got.at[layer, j], y_send.at[1], y_end.at[layer, j // 2], y_next(sign_of(j)))

    def pair(layer, p, sems):
        two = y_relay.at[layer, 2 * p : 2 * p + 2]
        return remote(two, two, y_send.at[1], sems.at[layer, p], mate)

    def y_forward(layer, p):
        pair(layer, p, y_mid).wait_recv()
        loop(2 * p, 2 * p + 2, lambda j: y_pass(layer, j).start())

    groups = ((4, -3), (3, -2), (2, -1), (1,), (0,))

    def unit_rows(away):
        return pl.ds(pl.multiple_of(lax.rem(z + away + NZ, NZ) * unit, unit), unit)

    def y_first(layer, j, at_rows, sign, part_of, g):
        others = pl.ds(pl.multiple_of(half_rows + at_rows.start, unit), unit)
        return remote(
            part_y.at[layer, j, others, :], y_relay.at[layer, j, at_rows, :], y_send.at[0], y_parts.at[part_of], y_next(sign)
        )

    def y_second(layer, j, at_rows, sign, part_of, g):
        return remote(
            y_relay.at[layer, j, at_rows, :], y_got.at[layer, j, at_rows, :], y_send.at[1], y_unit.at[g], y_next(sign)
        )

    def y_units(layer, p, hop, part_of, which):
        for g in which:
            for away in groups[g]:
                def act(j):
                    sign = sign_of(j)
                    hop(layer, j, unit_rows(sign * away), sign, part_of, g).start()
                loop(2 * p, 2 * p + 2, act)

    def y_units_wait(layer, p, part_of, units):
        these = y_relay.at[layer, 2 * p : 2 * p + 2, 0 : unit * units, :]
        remote(these, these, y_send.at[0], y_parts.at[part_of], mate).wait_recv()

    def y_units_add(layer, p, g):
        four = y_got.at[layer, 2 * p : 2 * p + 2, 0 : unit * len(groups[g]), :]
        remote(four, four, y_send.at[1], y_unit.at[g], mate).wait_recv()
        for away in groups[g]:
            def act(j):
                at_rows = unit_rows(sign_of(j) * away)
                part_y[layer, j, at_rows, :] = part_y[layer, j, at_rows, :] + y_got[layer, j, at_rows, :]
            loop(2 * p, 2 * p + 2, act)

    def y_begin(layer, p):
        pair(layer, p, y_end).wait_recv()

        def act(j):
            part_y[layer, j, 0:half_rows, :] = part_y[layer, j, 0:half_rows, :] + y_got[layer, j]
            chain_start(Y, layer, j)
        loop(2 * p, 2 * p + 2, act)

    def z_copy(layer, j):
        return remote(
            ring_z.at[layer * 8 + j * 2 + 1, 3], z_relay.at[layer, j], z_send.at[0], z_mid.at[layer], y_next(sign_of(j))
        )

    def z_pass(layer, j):
        return remote(z_relay.at[layer, j], z_got.at[layer, j], z_send.at[1], z_end_sem.at[layer], y_next(sign_of(j)))

    def z_all(layer, sems):
        return remote(z_relay.at[layer], z_got.at[layer], z_send.at[1], sems.at[layer], mate)

    def z_forward(layer):
        z_all(layer, z_mid).wait_recv()
        loop(0, BLOCKS, lambda j: z_pass(layer, j).start())

    def finish(kind, layer, slot, value):
        j, _, k, _, cols = stream(kind, layer, slot)
        held = ring[kind]
        held[k, 3, :, cols] = value
        col = core * half_cols + first_col[min(kind, Y)] + j * width[min(kind, Y)] + cols.start
        where = pl.ds(pl.multiple_of(col, 128), width[kind])

        def of(c):
            return pl.ds(pl.multiple_of(c * own_rows, own_rows), own_rows)

        remote(
            held.at[k, 3, of(1 - core), cols], gbuf.at[layer, :, where], g_sem.at[0], g_sem.at[1], mate
        ).start()
        gbuf[layer, :, where] = held[k, 3, of(core), cols]
        squares = value * value
        folded = squares[0:own_rows] + squares[own_rows : 2 * own_rows]
        total = folded[:, 0:128]
        for i in range(1, width[kind] // 128):
            total = total + folded[:, i * 128 : (i + 1) * 128]
        q_acc[layer] = q_acc[layer] + total

    def z_finish(layer):
        z_all(layer, z_end_sem).wait_recv()
        loop(0, BLOCKS, lambda j: finish(Z, layer, 2 * j, ring_z[layer * 8 + 2 * j, 3] + z_got[layer, j]))

    def y_finish(layer, low, high, kind=Y):
        loop(low, high, lambda slot: finish(kind, layer, slot, chain_last(kind, layer, slot)))

    def q_copy(offset):
        return remote(q_own, q_got.at[offset - 1], q_sem.at[0], q_sem.at[1], group_device(offset))

    def all_of(got, sems):
        return remote(got, got, sems.at[0], sems.at[1], mate)

    def to_y(layer, j):
        multiply(layer, Y, j)
        y_copy(layer, j).start()

    def to_z(j):
        multiply(0, Z, j)
        chain_start(Z, 0, 2 * j)
        chain_start(Z, 0, 2 * j + 1)

    def to_y_half(j, h):
        cols = half_cols_of(h)
        x_half(j, h).wait_recv()
        mine = own_half[0, :, pl.ds(pl.multiple_of(first_col[Y] + j * width[Y] + cols.start, 128), cols.size)]
        both = jnp.concatenate([mine, x_got_y[0, j, :, cols].astype(jnp.bfloat16)], axis=0)
        part_y[0, j, :, cols] = jnp.dot(a_t[0], both, preferred_element_type=jnp.float32)
        remote(
            part_y.at[0, j, pl.ds(half_rows, half_rows), cols], y_relay.at[0, j, :, cols],
            y_send.at[0], y_mid.at[0, 0], y_next(sign_of(j)),
        ).start()

    og_copy(0, 0, 1).wait()
    loop(0, 2, lambda j: to_y_half(j, 0))
    og_copy(0, 0, 0).wait()
    loop(0, 2, to_z)
    loop(0, 2, lambda j: to_y_half(j, 1))
    loop(2, 4, to_z)
    og_copy(0, 0, 2).wait()
    loop(2, 4, lambda j: to_y(0, j))

    for which in (1, 0):
        for piece in (1, 2, 0):
            og_copy(1, which, piece).start()
    in_copies[1].wait()
    c_own[0] = jnp.zeros_like(c_own[0])
    c_own[0, :, 0:8] = counts[:, 0, :].astype(jnp.float32)
    c_copies[0].start()
    q_acc[...] = jnp.zeros_like(q_acc)
    for kind in (Y, Z):
        x_all(0, kind).wait_send()
        for piece in ((0,), (1, 2))[kind]:
            og_copy(1, 1, piece).wait()
        swap(1, kind, 0, 4)
    in_copies[2].start()
    in_copies[3].start()
    for piece in range(3):
        og_copy(1, 0, piece).wait()

    steps(Z, 0, 0, 8, 1)
    a_join(1)
    x_all(1, Y).wait_recv()
    loop(0, 2, lambda j: to_y(1, j))
    x_all(1, Z).wait_recv()
    loop(0, 4, lambda j: multiply(1, Z, j))
    steps(Z, 0, 0, 8, 2)
    y_forward(0, 0)
    loop(2, 4, lambda j: multiply(1, Y, j))
    steps(Z, 0, 0, 8, 3)
    starts(Z, 1, 0, 8)
    y_forward(0, 1)
    z_last(0)
    c_next(0)
    steps(Z, 1, 0, 8, 1)
    y_units(1, 1, y_first, 0, (0, 1, 2))
    y_forward(1, 0)
    steps(Z, 1, 0, 8, 2)
    c_next(1)
    steps(Z, 1, 0, 8, 3)

    y_begin(0, 0)
    y_begin(0, 1)
    z_last(1)
    steps(Y, 0, 0, 4, 1)
    y_units_wait(1, 1, 0, 6)
    y_units(1, 1, y_second, 0, (0, 1, 2))
    y_units(1, 1, y_first, 1, (3, 4))
    for layer in range(LAYERS):
        loop(0, BLOCKS, lambda j: z_copy(layer, j).start())
    steps(Y, 0, 0, 4, 2)
    steps(Y, 0, 0, 2, 3)
    y_begin(1, 0)
    y_units_add(1, 1, 0)
    starts(YH, 1, 0, 4)
    steps(Y, 1, 0, 2, 1)
    y_units_add(1, 1, 1)
    steps(YH, 1, 0, 4, 1)
    y_units_wait(1, 1, 1, 2)
    y_units(1, 1, y_second, 0, (3, 4))
    steps(Y, 1, 0, 2, 2)
    y_units_add(1, 1, 2)
    steps(YH, 1, 0, 4, 2)
    z_forward(0)
    steps(Y, 1, 0, 2, 3)
    z_forward(1)
    c_next(2)
    y_units_add(1, 1, 3)
    steps(YH, 1, 0, 4, 3)
    steps(Y, 0, 2, 4, 3)
    y_finish(0, 0, 2)
    y_finish(1, 0, 2)
    z_finish(0)
    y_units_add(1, 1, 4)
    y_finish(1, 0, 4, YH)
    y_finish(0, 2, 4)
    z_finish(1)

    q_own[0:2] = jnp.sum(q_acc[...], axis=1)
    q_own[2:4] = c_own[3]
    for away in (4, 3, 5, 2, 6, 1, 7):
        loop(away * 4, away * 4 + 4, lambda offset: q_copy(offset).start())
    loop(1, 4, lambda offset: q_copy(offset).start())

    landed = gbuf.at[:, :, 0:half_cols]
    all_g = remote(landed, landed, g_sem.at[0], g_sem.at[1], mate)
    all_g.wait_recv()
    in_copies[2].wait()
    in_copies[3].wait()

    all_g.wait_send()
    for i in range(2):
        remote(y_relay, y_got, y_send.at[i], y_unit.at[0], mate).wait_send()
        remote(z_relay, z_got, z_send.at[i], z_mid.at[0], mate).wait_send()
    for kind in (Z, Y):
        x_all(1, kind).wait_send()
        remote(ring[kind], ring[kind], ring_send.at[kind], ring_recv.at[0, 0], mate).wait_send()
    for layer in range(LAYERS):
        a_copy(layer).wait_send()
    for copy in c_copies:
        copy.wait_send()
    all_of(q_got, q_sem).wait_send()

    all_of(q_got, q_sem).wait_recv()
    sums = q_own[...] + jnp.sum(q_got[...], axis=0)
    root_mean = jnp.sqrt(jnp.sum(sums[0:2], axis=1, keepdims=True) / float(rows * 2 * half_cols))
    totals = sums[2:4]
    lanes = lax.broadcasted_iota(jnp.int32, totals.shape, 1)
    mean_load = jnp.sum(totals, axis=1, keepdims=True) / 8.0
    own_load = jnp.sum(jnp.where(lanes == me_expert, totals, 0.0), axis=1, keepdims=True)
    factor = step_size * (own_load / mean_load) * clip_level / jnp.maximum(root_mean, clip_level)
    beta = own_load / (own_load + mean_load)
    for layer in range(LAYERS):
        this_factor = jnp.broadcast_to(factor[layer : layer + 1], (own_rows, 128))
        this_beta = jnp.broadcast_to(beta[layer : layer + 1], (own_rows, 128))

        def update(i):
            for n in range(8):
                cols = pl.ds(pl.multiple_of(i * 1024 + n * 128, 128), 128)
                updated = w_in[layer, 0, :, cols] - this_factor * gbuf[layer, :, cols]
                new_weights[layer, 0, :, cols] = updated
                previous = s_in[layer, 0, :, cols]
                new_shadow[layer, 0, :, cols] = previous + this_beta * (updated - previous)
        loop(0, 2 * half_cols // 1024, update)


def writer(updated, smoothed, new_weights, new_shadow, sems):
    copies = [
        pltpu.make_async_copy(src.at[layer], dst.at[layer], sems.at[i, layer])
        for i, (src, dst) in enumerate(((updated, new_weights), (smoothed, new_shadow)))
        for layer in range(LAYERS)
    ]
    for copy in copies:
        copy.start()
    for copy in copies:
        copy.wait()


def on_device(activations, out_grads, weights, shadow, counts):
    acts, og = activations[:, 0], out_grads[:, 0]
    tokens, rows = acts.shape[1:]
    ff = og.shape[2]
    unit = rows // 2 // NZ
    half = rows // 2
    tiles = ff // 2 // 128 // BLOCKS
    wide_z, wide_y = (tiles * 3 // 7) * 128, (tiles - tiles * 3 // 7) * 128
    f32, bf16 = jnp.float32, jnp.bfloat16
    dma = pltpu.SemaphoreType.DMA
    vmem = pl.BlockSpec(memory_space=pltpu.VMEM)
    hbm = pl.BlockSpec(memory_space=pl.ANY)
    updated, smoothed = pl.pallas_call(
        kernel,
        out_shape=(pltpu.VMEM(weights.shape, f32), pltpu.VMEM(shadow.shape, f32)),
        in_specs=[hbm] * 5,
        out_specs=(vmem, vmem),
        scratch_shapes=[
            pltpu.VMEM((LAYERS, BLOCKS, rows, wide_z), f32),
            pltpu.VMEM((LAYERS, BLOCKS, rows, wide_y), f32),
            pltpu.VMEM((LAYERS * 8, NZ - 1, unit, wide_z), f32),
            pltpu.VMEM((LAYERS * 4, NZ - 1, unit, wide_y), f32),
            pltpu.VMEM((LAYERS, BLOCKS, half, wide_y), f32),
            pltpu.VMEM((LAYERS, BLOCKS, half, wide_y), f32),
            pltpu.VMEM((LAYERS, BLOCKS, unit, wide_z), f32),
            pltpu.VMEM((LAYERS, BLOCKS, unit, wide_z), f32),
            pltpu.VMEM((LAYERS, BLOCKS, tokens, wide_z), f32),
            pltpu.VMEM((LAYERS, BLOCKS, tokens, wide_y), f32),
            pltpu.VMEM((BLOCKS, tokens, wide_z), f32),
            pltpu.VMEM((BLOCKS, tokens, wide_y), f32),
            pltpu.VMEM((LAYERS, tokens, ff // 2), bf16),
            pltpu.VMEM((LAYERS, tokens, ff // 2), bf16),
            pltpu.VMEM(acts.shape, bf16),
            pltpu.VMEM(counts.shape, counts.dtype),
            pltpu.VMEM(weights.shape, f32),
            pltpu.VMEM(shadow.shape, f32),
            pltpu.VMEM((LAYERS, tokens, rows), f32),
            pltpu.VMEM((LAYERS, tokens, rows), f32),
            pltpu.VMEM((rows, 2 * tokens), f32),
            pltpu.VMEM((LAYERS, rows, 2 * tokens), bf16),
            pltpu.VMEM((LAYERS, unit // 2, ff), f32),
            pltpu.VMEM((4, LAYERS, 128), f32),
            pltpu.VMEM((3, LAYERS, 128), f32),
            pltpu.VMEM((2 * LAYERS, 128), f32),
            pltpu.VMEM((31, 2 * LAYERS, 128), f32),
            pltpu.VMEM((LAYERS, unit // 2, 128), f32),
            dma((LAYERS, 2, 3)),
            dma((4,)),
            dma((2,)),
            dma((10,)),
            dma((2,)),
            dma((2, LAYERS)),
            dma((2,)),
            dma((16, 2)),
            dma((2,)),
            dma((LAYERS, 2)),
            dma((LAYERS, 2)),
            dma((2,)),
            dma((5,)),
            dma((2,)),
            dma((LAYERS,)),
            dma((LAYERS,)),
            dma((2,)),
            dma((2, 3)),
            dma((2,)),
        ],
        compiler_params=pltpu.CompilerParams(
            collective_id=0, has_side_effects=True, vmem_limit_bytes=58 * 1024 * 1024
        ),
    )(acts, og, counts, weights, shadow)
    return pl.pallas_call(
        writer,
        out_shape=(jax.ShapeDtypeStruct(weights.shape, f32), jax.ShapeDtypeStruct(shadow.shape, f32)),
        in_specs=[vmem, vmem],
        out_specs=(hbm, hbm),
        scratch_shapes=[dma((2, LAYERS))],
    )(*(pltpu.with_memory_space_constraint(a, pltpu.VMEM) for a in (updated, smoothed)))


def solution(mesh):
    split = Mesh(
        mesh.devices.reshape(mesh.shape["dp"], 4, 2, 2, 2),
        ("dp", "expert_0", "expert_1", "shard_0", "shard_1"),
    )
    return jax.shard_map(
        on_device,
        mesh=split,
        in_specs=(
            P(None, EXPERT, DP_SHARD, None),
            P(None, EXPERT, DP_SHARD, None),
            P(None, EXPERT, DP_SHARD, None),
            P(None, EXPERT, DP_SHARD, None),
            P(None, DP_EXPERT_SHARD, None),
        ),
        out_specs=(P(None, EXPERT, DP_SHARD, None), P(None, EXPERT, DP_SHARD, None)),
        check_vma=False,
    )
```

```python
import jax
import jax.numpy as jnp
from jax import lax
from jax.experimental import pallas as pl
from jax.experimental.pallas import tpu as pltpu
from jax.sharding import Mesh
from jax.sharding import PartitionSpec as P

MESH = pl.DeviceIdType.MESH
LAYERS = 2
EXPERT = ("expert_0", "expert_1")
DP_EXPERT_SHARD = ("dp", "expert_0", "expert_1", "shard_0", "shard_1")
DP_SHARD = ("dp", "shard_0", "shard_1")

step_size = 0.5
clip_level = 1.0

NZ = 8
BLOCKS = 4
Z, Y, YH = 0, 1, 2


def kernel(
    acts_in, og, counts_in, weights, shadow, gbuf, w_in, s_in, scalars,
    part_z, part_y, ring_z, ring_y, y_got, y_relay, z_got, z_relay, x_got_z, x_got_y, x_out_z, x_out_y,
    own_half, other_half, acts, counts, a_out, a_got, a_rows, a_t, c_own, c_got, q_own, q_got, q_acc,
    og_sem, in_sem, x_send, x_recv, x_recv_late, a_sem, ring_send, ring_recv,
    y_send, y_mid, y_end, y_parts, y_unit, z_send, z_mid, z_end_sem, g_sem, c_sem, q_sem,
):
    z = lax.axis_index("dp")
    x = lax.axis_index("expert_0")
    y_lo = lax.axis_index("expert_1")
    y_hi = lax.axis_index("shard_0")
    core = lax.axis_index("shard_1")
    y = y_hi * 2 + y_lo
    tokens = acts.shape[1]
    rows = acts.shape[2]
    half_rows = rows // 2
    unit = half_rows // NZ
    own_rows = unit // 2
    part = (part_z, part_y, part_y)
    ring = (ring_z, ring_y, ring_y)
    x_got = (x_got_z, x_got_y)
    x_out = (x_out_z, x_out_y)
    width = (part_z.shape[-1], part_y.shape[-1], part_y.shape[-1] // 2)
    first_col = (0, BLOCKS * width[Z])
    half_cols = BLOCKS * (width[Z] + width[Y])

    def at(z=z, x=x, y_lo=y_lo, y_hi=y_hi, core=core):
        return (z, x, y_lo, y_hi, core)

    def z_next(sign):
        return at(z=lax.rem(z + sign + NZ, NZ))

    def y_next(sign):
        to = lax.rem(y + sign + 4, 4)
        return at(y_lo=lax.rem(to, 2), y_hi=to // 2)

    mate = at(core=1 - core)
    me_group = z * 4 + y_hi * 2 + core
    me_expert = x * 2 + y_lo

    def group_device(offset):
        to = lax.rem(me_group + offset, 32)
        return at(z=to // 4, y_hi=lax.rem(to // 2, 2), core=lax.rem(to, 2))

    def remote(src, dst, send, recv, device):
        return pltpu.make_async_remote_copy(
            src_ref=src, dst_ref=dst, send_sem=send, recv_sem=recv, device_id=device, device_id_type=MESH
        )

    def loop(low, high, act):
        def body(i, _):
            act(i)
            return 0
        lax.fori_loop(low, high, body, 0)

    pieces = ((0, 4 * width[Z]), (first_col[Y], 2 * width[Y]), (first_col[Y] + 2 * width[Y], 2 * width[Y]))

    def og_copy(layer, which, piece):
        first = core if which == 0 else 1 - core
        to = own_half if which == 0 else other_half
        begin, size = pieces[piece]
        cols = pl.ds(pl.multiple_of(first * half_cols + begin, 128), size)
        return pltpu.make_async_copy(
            og.at[layer, :, cols], to.at[layer, :, begin : begin + size], og_sem.at[layer, which, piece]
        )

    in_copies = [
        pltpu.make_async_copy(src, dst, in_sem.at[i])
        for i, (src, dst) in enumerate(((acts_in, acts), (counts_in, counts), (weights, w_in), (shadow, s_in)))
    ]

    barrier = pltpu.get_barrier_semaphore()
    near = (
        mate, z_next(1), z_next(-1), y_next(1), y_next(-1), at(x=x + 1 - 2 * lax.rem(x, 2)), at(x=3 - x)
    )
    for device in near:
        pl.semaphore_signal(barrier, inc=1, device_id=device, device_id_type=MESH)

    og_copy(0, 1, 1).start()
    in_copies[0].start()
    for which, piece in ((0, 1), (1, 0), (0, 0), (1, 2), (0, 2)):
        og_copy(0, which, piece).start()
    in_copies[1].start()

    def cols_of(kind, j):
        return pl.ds(pl.multiple_of(first_col[kind] + j * width[kind], 128), width[kind])

    def convert(layer, kind, j):
        x_out[kind][j] = other_half[layer, :, cols_of(kind, j)].astype(jnp.float32)

    def x_copy(layer, kind, j):
        sem = x_recv.at[4 * kind + j] if layer == 0 else x_recv_late.at[kind]
        return remote(x_out[kind].at[j], x_got[kind].at[layer, j], x_send.at[kind], sem, mate)

    quarter = width[YH] // 2

    def half_cols_of(h):
        return pl.ds(h * quarter, quarter if h == 0 else width[Y] - quarter)

    def x_half(j, h):
        cols = half_cols_of(h)
        return remote(x_out_y.at[j, :, cols], x_got_y.at[0, j, :, cols], x_send.at[Y], x_recv.at[4 + j + 4 * h], mate)

    def x_all(layer, kind):
        return remote(x_out[kind], x_got[kind].at[layer], x_send.at[kind], x_recv_late.at[kind], mate)

    def a_copy(layer):
        return remote(a_out.at[layer], a_got.at[layer], a_sem.at[0, layer], a_sem.at[1, layer], mate)

    def a_join(layer):
        a_rows[:, 0:tokens] = a_out[layer].T
        a_copy(layer).wait_recv()
        a_rows[:, tokens : 2 * tokens] = a_got[layer].T
        for half in range(2):
            side = y_hi if half == 0 else 1 - y_hi
            for zz in range(NZ):
                piece = a_rows[pl.ds(pl.multiple_of(zz * 2 * unit + side * unit, unit), unit), :]
                a_t[layer, half * half_rows + zz * unit : half * half_rows + (zz + 1) * unit, :] = piece.astype(jnp.bfloat16)

    def swap(layer, kind, low, high):
        def act(j):
            convert(layer, kind, j)
            x_copy(layer, kind, j).start()
        loop(low, high, act)

    c_copies = [
        remote(c_own.at[i], c_got.at[i], c_sem.at[0, i], c_sem.at[1, i], device)
        for i, device in enumerate((near[5], near[6], at(y_lo=1 - y_lo)))
    ]

    def c_next(i):
        c_copies[i].wait_recv()
        c_own[i + 1] = c_own[i] + c_got[i]
        if i < 2:
            c_copies[i + 1].start()

    og_copy(0, 1, 1).wait()
    loop(0, 2, lambda j: convert(0, Y, j))
    in_copies[0].wait()
    a_out[...] = acts[...].astype(jnp.float32)
    pl.semaphore_wait(barrier, len(near))

    a_copy(0).start()
    loop(0, 2, lambda j: x_half(j, 0).start())
    og_copy(0, 1, 0).wait()
    swap(0, Z, 0, 2)
    loop(0, 2, lambda j: x_half(j, 1).start())
    swap(0, Z, 2, 4)
    og_copy(0, 1, 2).wait()
    swap(0, Y, 2, 4)
    a_copy(1).start()
    a_join(0)

    def multiply(layer, kind, j):
        if layer == 0:
            x_copy(layer, kind, j).wait_recv()
        theirs = x_got[kind][layer, j].astype(jnp.bfloat16)
        both = jnp.concatenate([own_half[layer, :, cols_of(kind, j)], theirs], axis=0)
        part[kind][layer, j] = jnp.dot(a_t[layer], both, preferred_element_type=jnp.float32)

    def stream(kind, layer, slot):
        full = pl.ds(0, width[kind])
        if kind == Z:
            return slot // 2, lax.rem(slot, 2), layer * 8 + slot, layer * 8 + slot, full
        if kind == Y:
            return slot, 0, layer * 4 + slot, layer * 4 + slot, full
        j = 2 + lax.rem(slot, 2)
        cols = pl.ds(pl.multiple_of(slot // 2 * width[YH], 128), width[YH])
        return j, 0, layer * 4 + j, layer * 4 + 2 + slot, cols

    def sign_of(slot):
        return 1 - 2 * lax.rem(slot, 2)

    def chunk(kind, layer, slot, away):
        j, half, _, _, cols = stream(kind, layer, slot)
        index = lax.rem(z + away + NZ, NZ)
        return part[kind].at[layer, j, pl.ds(pl.multiple_of(half * half_rows + index * unit, unit), unit), cols]

    def long_copy(kind, layer, slot, step):
        _, _, k, sem, cols = stream(kind, layer, slot)
        sign = sign_of(slot)
        src = chunk(kind, layer, slot, sign * 4) if step == 0 else ring[kind].at[k, step - 1, :, cols]
        dst = ring[kind].at[k, step, :, cols]
        return remote(src, dst, ring_send.at[min(kind, Y)], ring_recv.at[sem, step % 2], z_next(sign))

    def short_copy(kind, layer, slot, step):
        _, _, k, sem, cols = stream(kind, layer, slot)
        sign = sign_of(slot)
        src = chunk(kind, layer, slot, sign * -3) if step == 0 else ring[kind].at[k, 3 + step, :, cols]
        dst = ring[kind].at[k, 4 + step, :, cols]
        return remote(src, dst, ring_send.at[min(kind, Y)], ring_recv.at[sem, step % 2], z_next(-sign))

    def both_of(kind, layer, slot, step):
        _, _, k, sem, cols = stream(kind, layer, slot)
        two = ring[kind].at[k, 0:2, :, cols]
        return remote(two, two, ring_send.at[min(kind, Y)], ring_recv.at[sem, step % 2], z_next(1))

    def chain_start(kind, layer, slot):
        long_copy(kind, layer, slot, 0).start()
        short_copy(kind, layer, slot, 0).start()

    def chain_step(kind, layer, slot, step):
        _, _, k, _, cols = stream(kind, layer, slot)
        held = ring[kind]
        sign = sign_of(slot)
        both_of(kind, layer, slot, step - 1).wait_recv()
        held[k, step - 1, :, cols] = held[k, step - 1, :, cols] + chunk(kind, layer, slot, sign * (4 - step))[...]
        if step < 3:
            held[k, 3 + step, :, cols] = held[k, 3 + step, :, cols] + chunk(kind, layer, slot, sign * (step - 3))[...]
        long_copy(kind, layer, slot, step).start()
        if step < 3:
            short_copy(kind, layer, slot, step).start()

    def chain_last(kind, layer, slot):
        _, _, k, _, cols = stream(kind, layer, slot)
        long_copy(kind, layer, slot, 3).wait_recv()
        return ring[kind][k, 3, :, cols] + chunk(kind, layer, slot, 0)[...] + ring[kind][k, 6, :, cols]

    def steps(kind, layer, low, high, step):
        loop(low, high, lambda slot: chain_step(kind, layer, slot, step))

    def starts(kind, layer, low, high):
        loop(low, high, lambda slot: chain_start(kind, layer, slot))

    def z_last(layer):
        def act(slot):
            ring_z[layer * 8 + slot, 3] = chain_last(Z, layer, slot)
        loop(0, 8, act)

    def y_copy(layer, j):
        return remote(
            part_y.at[layer, j, pl.ds(half_rows, half_rows), :], y_relay.at[layer, j],
            y_send.at[0], y_mid.at[layer, j // 2], y_next(sign_of(j)),
        )

    def y_pass(layer, j):
        return remote(y_relay.at[layer, j], y_got.at[layer, j], y_send.at[1], y_end.at[layer, j // 2], y_next(sign_of(j)))

    def pair(layer, p, sems):
        two = y_relay.at[layer, 2 * p : 2 * p + 2]
        return remote(two, two, y_send.at[1], sems.at[layer, p], mate)

    def y_forward(layer, p):
        pair(layer, p, y_mid).wait_recv()
        loop(2 * p, 2 * p + 2, lambda j: y_pass(layer, j).start())

    groups = ((4, -3), (3, -2), (2, -1), (1,), (0,))

    def unit_rows(away):
        return pl.ds(pl.multiple_of(lax.rem(z + away + NZ, NZ) * unit, unit), unit)

    def y_first(layer, j, at_rows, sign, part_of, g):
        others = pl.ds(pl.multiple_of(half_rows + at_rows.start, unit), unit)
        return remote(
            part_y.at[layer, j, others, :], y_relay.at[layer, j, at_rows, :], y_send.at[0], y_parts.at[part_of], y_next(sign)
        )

    def y_second(layer, j, at_rows, sign, part_of, g):
        return remote(
            y_relay.at[layer, j, at_rows, :], y_got.at[layer, j, at_rows, :], y_send.at[1], y_unit.at[g], y_next(sign)
        )

    def y_units(layer, p, hop, part_of, which):
        for g in which:
            for away in groups[g]:
                def act(j):
                    sign = sign_of(j)
                    hop(layer, j, unit_rows(sign * away), sign, part_of, g).start()
                loop(2 * p, 2 * p + 2, act)

    def y_units_wait(layer, p, part_of, units):
        these = y_relay.at[layer, 2 * p : 2 * p + 2, 0 : unit * units, :]
        remote(these, these, y_send.at[0], y_parts.at[part_of], mate).wait_recv()

    def y_units_add(layer, p, g):
        four = y_got.at[layer, 2 * p : 2 * p + 2, 0 : unit * len(groups[g]), :]
        remote(four, four, y_send.at[1], y_unit.at[g], mate).wait_recv()
        for away in groups[g]:
            def act(j):
                at_rows = unit_rows(sign_of(j) * away)
                part_y[layer, j, at_rows, :] = part_y[layer, j, at_rows, :] + y_got[layer, j, at_rows, :]
            loop(2 * p, 2 * p + 2, act)

    def y_begin(layer, p):
        pair(layer, p, y_end).wait_recv()

        def act(j):
            part_y[layer, j, 0:half_rows, :] = part_y[layer, j, 0:half_rows, :] + y_got[layer, j]
            chain_start(Y, layer, j)
        loop(2 * p, 2 * p + 2, act)

    def z_copy(layer, j):
        return remote(
            ring_z.at[layer * 8 + j * 2 + 1, 3], z_relay.at[layer, j], z_send.at[0], z_mid.at[layer], y_next(sign_of(j))
        )

    def z_pass(layer, j):
        return remote(z_relay.at[layer, j], z_got.at[layer, j], z_send.at[1], z_end_sem.at[layer], y_next(sign_of(j)))

    def z_all(layer, sems):
        return remote(z_relay.at[layer], z_got.at[layer], z_send.at[1], sems.at[layer], mate)

    def z_forward(layer):
        z_all(layer, z_mid).wait_recv()
        loop(0, BLOCKS, lambda j: z_pass(layer, j).start())

    def finish(kind, layer, slot, value):
        j, _, k, _, cols = stream(kind, layer, slot)
        held = ring[kind]
        held[k, 3, :, cols] = value
        col = core * half_cols + first_col[min(kind, Y)] + j * width[min(kind, Y)] + cols.start
        where = pl.ds(pl.multiple_of(col, 128), width[kind])

        def of(c):
            return pl.ds(pl.multiple_of(c * own_rows, own_rows), own_rows)

        remote(
            held.at[k, 3, of(1 - core), cols], gbuf.at[layer, :, where], g_sem.at[0], g_sem.at[1], mate
        ).start()
        gbuf[layer, :, where] = held[k, 3, of(core), cols]
        squares = value * value
        folded = squares[0:own_rows] + squares[own_rows : 2 * own_rows]
        total = folded[:, 0:128]
        for i in range(1, width[kind] // 128):
            total = total + folded[:, i * 128 : (i + 1) * 128]
        q_acc[layer] = q_acc[layer] + total

    def z_finish(layer):
        z_all(layer, z_end_sem).wait_recv()
        loop(0, BLOCKS, lambda j: finish(Z, layer, 2 * j, ring_z[layer * 8 + 2 * j, 3] + z_got[layer, j]))

    def y_finish(layer, low, high, kind=Y):
        loop(low, high, lambda slot: finish(kind, layer, slot, chain_last(kind, layer, slot)))

    def q_copy(offset):
        return remote(q_own, q_got.at[offset - 1], q_sem.at[0], q_sem.at[1], group_device(offset))

    def all_of(got, sems):
        return remote(got, got, sems.at[0], sems.at[1], mate)

    def to_y(layer, j):
        multiply(layer, Y, j)
        y_copy(layer, j).start()

    def to_z(j):
        multiply(0, Z, j)
        chain_start(Z, 0, 2 * j)
        chain_start(Z, 0, 2 * j + 1)

    def to_y_half(j, h):
        cols = half_cols_of(h)
        x_half(j, h).wait_recv()
        mine = own_half[0, :, pl.ds(pl.multiple_of(first_col[Y] + j * width[Y] + cols.start, 128), cols.size)]
        both = jnp.concatenate([mine, x_got_y[0, j, :, cols].astype(jnp.bfloat16)], axis=0)
        part_y[0, j, :, cols] = jnp.dot(a_t[0], both, preferred_element_type=jnp.float32)
        remote(
            part_y.at[0, j, pl.ds(half_rows, half_rows), cols], y_relay.at[0, j, :, cols],
            y_send.at[0], y_mid.at[0, 0], y_next(sign_of(j)),
        ).start()

    og_copy(0, 0, 1).wait()
    loop(0, 2, lambda j: to_y_half(j, 0))
    og_copy(0, 0, 0).wait()
    loop(0, 2, to_z)
    loop(0, 2, lambda j: to_y_half(j, 1))
    loop(2, 4, to_z)
    og_copy(0, 0, 2).wait()
    loop(2, 4, lambda j: to_y(0, j))

    for which in (1, 0):
        for piece in (1, 2, 0):
            og_copy(1, which, piece).start()
    in_copies[1].wait()
    c_own[0] = jnp.zeros_like(c_own[0])
    c_own[0, :, 0:8] = counts[:, 0, :].astype(jnp.float32)
    c_copies[0].start()
    q_acc[...] = jnp.zeros_like(q_acc)
    for kind in (Y, Z):
        x_all(0, kind).wait_send()
        for piece in ((0,), (1, 2))[kind]:
            og_copy(1, 1, piece).wait()
        swap(1, kind, 0, 4)
    in_copies[2].start()
    in_copies[3].start()
    for piece in range(3):
        og_copy(1, 0, piece).wait()

    steps(Z, 0, 0, 8, 1)
    a_join(1)
    x_all(1, Y).wait_recv()
    loop(0, 2, lambda j: to_y(1, j))
    x_all(1, Z).wait_recv()
    loop(0, 4, lambda j: multiply(1, Z, j))
    steps(Z, 0, 0, 8, 2)
    y_forward(0, 0)
    loop(2, 4, lambda j: multiply(1, Y, j))
    steps(Z, 0, 0, 8, 3)
    starts(Z, 1, 0, 8)
    y_forward(0, 1)
    z_last(0)
    c_next(0)
    steps(Z, 1, 0, 8, 1)
    y_units(1, 1, y_first, 0, (0, 1, 2))
    y_forward(1, 0)
    steps(Z, 1, 0, 8, 2)
    c_next(1)
    steps(Z, 1, 0, 8, 3)

    y_begin(0, 0)
    y_begin(0, 1)
    z_last(1)
    steps(Y, 0, 0, 4, 1)
    y_units_wait(1, 1, 0, 6)
    y_units(1, 1, y_second, 0, (0, 1, 2))
    y_units(1, 1, y_first, 1, (3, 4))
    for layer in range(LAYERS):
        loop(0, BLOCKS, lambda j: z_copy(layer, j).start())
    steps(Y, 0, 0, 4, 2)
    steps(Y, 0, 0, 2, 3)
    y_begin(1, 0)
    y_units_add(1, 1, 0)
    starts(YH, 1, 0, 4)
    steps(Y, 1, 0, 2, 1)
    y_units_add(1, 1, 1)
    steps(YH, 1, 0, 4, 1)
    y_units_wait(1, 1, 1, 2)
    y_units(1, 1, y_second, 0, (3, 4))
    steps(Y, 1, 0, 2, 2)
    y_units_add(1, 1, 2)
    steps(YH, 1, 0, 4, 2)
    z_forward(0)
    steps(Y, 1, 0, 2, 3)
    z_forward(1)
    c_next(2)
    y_units_add(1, 1, 3)
    steps(YH, 1, 0, 2, 3)
    steps(Y, 0, 2, 4, 3)
    steps(YH, 1, 2, 4, 3)
    y_finish(0, 0, 2)
    y_finish(1, 0, 2)
    z_finish(0)
    y_units_add(1, 1, 4)
    y_finish(1, 0, 2, YH)
    y_finish(0, 2, 4)
    z_finish(1)
    y_finish(1, 2, 4, YH)

    q_own[0:2] = jnp.sum(q_acc[...], axis=1)
    q_own[2:4] = c_own[3]
    for away in (4, 3, 5, 2, 6, 1, 7):
        loop(away * 4, away * 4 + 4, lambda offset: q_copy(offset).start())
    loop(1, 4, lambda offset: q_copy(offset).start())

    landed = gbuf.at[:, :, 0:half_cols]
    all_g = remote(landed, landed, g_sem.at[0], g_sem.at[1], mate)
    all_g.wait_recv()
    in_copies[2].wait()
    in_copies[3].wait()

    all_g.wait_send()
    for i in range(2):
        remote(y_relay, y_got, y_send.at[i], y_unit.at[0], mate).wait_send()
        remote(z_relay, z_got, z_send.at[i], z_mid.at[0], mate).wait_send()
    for kind in (Z, Y):
        x_all(1, kind).wait_send()
        remote(ring[kind], ring[kind], ring_send.at[kind], ring_recv.at[0, 0], mate).wait_send()
    for layer in range(LAYERS):
        a_copy(layer).wait_send()
    for copy in c_copies:
        copy.wait_send()
    all_of(q_got, q_sem).wait_send()

    all_of(q_got, q_sem).wait_recv()
    sums = q_own[...] + jnp.sum(q_got[...], axis=0)
    root_mean = jnp.sqrt(jnp.sum(sums[0:2], axis=1, keepdims=True) / float(rows * 2 * half_cols))
    totals = sums[2:4]
    lanes = lax.broadcasted_iota(jnp.int32, totals.shape, 1)
    mean_load = jnp.sum(totals, axis=1, keepdims=True) / 8.0
    own_load = jnp.sum(jnp.where(lanes == me_expert, totals, 0.0), axis=1, keepdims=True)
    factor = step_size * (own_load / mean_load) * clip_level / jnp.maximum(root_mean, clip_level)
    beta = own_load / (own_load + mean_load)
    scalars[0:2] = jnp.broadcast_to(factor, (LAYERS, 128))
    scalars[2:4] = jnp.broadcast_to(beta, (LAYERS, 128))


def update(summed, weights, shadow, scalars, new_weights, new_shadow, w_out, s_out, sems):
    rows, ff = summed.shape[1:]
    pieces = 2
    copies = []
    for layer in range(LAYERS):
        factor = jnp.broadcast_to(scalars[layer : layer + 1, :], (rows, 128))
        beta = jnp.broadcast_to(scalars[LAYERS + layer : LAYERS + layer + 1, :], (rows, 128))
        for piece in range(pieces):

            def some(i, _):
                for n in range(8):
                    cols = pl.ds(pl.multiple_of(piece * (ff // pieces) + i * 1024 + n * 128, 128), 128)
                    updated = weights[layer, 0, :, cols] - factor * summed[layer, :, cols]
                    w_out[layer, 0, :, cols] = updated
                    previous = shadow[layer, 0, :, cols]
                    s_out[layer, 0, :, cols] = previous + beta * (updated - previous)
                return 0

            lax.fori_loop(0, ff // pieces // 1024, some, 0)
            cols = pl.ds(piece * (ff // pieces), ff // pieces)
            for i, (src, dst) in enumerate(((w_out, new_weights), (s_out, new_shadow))):
                copy = pltpu.make_async_copy(
                    src.at[layer, 0, :, cols], dst.at[layer, 0, :, cols], sems.at[i, layer, piece]
                )
                copy.start()
                copies.append(copy)
    for copy in copies:
        copy.wait()


def on_device(activations, out_grads, weights, shadow, counts):
    acts, og = activations[:, 0], out_grads[:, 0]
    tokens, rows = acts.shape[1:]
    ff = og.shape[2]
    unit = rows // 2 // NZ
    half = rows // 2
    tiles = ff // 2 // 128 // BLOCKS
    wide_z, wide_y = (tiles * 3 // 7) * 128, (tiles - tiles * 3 // 7) * 128
    f32, bf16 = jnp.float32, jnp.bfloat16
    dma = pltpu.SemaphoreType.DMA
    vmem = pl.BlockSpec(memory_space=pltpu.VMEM)
    hbm = pl.BlockSpec(memory_space=pl.ANY)
    held = pl.pallas_call(
        kernel,
        out_shape=(
            pltpu.VMEM((LAYERS, unit // 2, ff), f32),
            pltpu.VMEM(weights.shape, f32),
            pltpu.VMEM(shadow.shape, f32),
            pltpu.VMEM((2 * LAYERS, 128), f32),
        ),
        in_specs=[hbm] * 5,
        out_specs=(vmem,) * 4,
        scratch_shapes=[
            pltpu.VMEM((LAYERS, BLOCKS, rows, wide_z), f32),
            pltpu.VMEM((LAYERS, BLOCKS, rows, wide_y), f32),
            pltpu.VMEM((LAYERS * 8, NZ - 1, unit, wide_z), f32),
            pltpu.VMEM((LAYERS * 4, NZ - 1, unit, wide_y), f32),
            pltpu.VMEM((LAYERS, BLOCKS, half, wide_y), f32),
            pltpu.VMEM((LAYERS, BLOCKS, half, wide_y), f32),
            pltpu.VMEM((LAYERS, BLOCKS, unit, wide_z), f32),
            pltpu.VMEM((LAYERS, BLOCKS, unit, wide_z), f32),
            pltpu.VMEM((LAYERS, BLOCKS, tokens, wide_z), f32),
            pltpu.VMEM((LAYERS, BLOCKS, tokens, wide_y), f32),
            pltpu.VMEM((BLOCKS, tokens, wide_z), f32),
            pltpu.VMEM((BLOCKS, tokens, wide_y), f32),
            pltpu.VMEM((LAYERS, tokens, ff // 2), bf16),
            pltpu.VMEM((LAYERS, tokens, ff // 2), bf16),
            pltpu.VMEM(acts.shape, bf16),
            pltpu.VMEM(counts.shape, counts.dtype),
            pltpu.VMEM((LAYERS, tokens, rows), f32),
            pltpu.VMEM((LAYERS, tokens, rows), f32),
            pltpu.VMEM((rows, 2 * tokens), f32),
            pltpu.VMEM((LAYERS, rows, 2 * tokens), bf16),
            pltpu.VMEM((4, LAYERS, 128), f32),
            pltpu.VMEM((3, LAYERS, 128), f32),
            pltpu.VMEM((2 * LAYERS, 128), f32),
            pltpu.VMEM((31, 2 * LAYERS, 128), f32),
            pltpu.VMEM((LAYERS, unit // 2, 128), f32),
            dma((LAYERS, 2, 3)),
            dma((4,)),
            dma((2,)),
            dma((10,)),
            dma((2,)),
            dma((2, LAYERS)),
            dma((2,)),
            dma((16, 2)),
            dma((2,)),
            dma((LAYERS, 2)),
            dma((LAYERS, 2)),
            dma((2,)),
            dma((5,)),
            dma((2,)),
            dma((LAYERS,)),
            dma((LAYERS,)),
            dma((2,)),
            dma((2, 3)),
            dma((2,)),
        ],
        compiler_params=pltpu.CompilerParams(
            collective_id=0, has_side_effects=True, vmem_limit_bytes=56 * 1024 * 1024
        ),
    )(acts, og, counts, weights, shadow)
    return pl.pallas_call(
        update,
        out_shape=(jax.ShapeDtypeStruct(weights.shape, f32), jax.ShapeDtypeStruct(shadow.shape, f32)),
        in_specs=[vmem] * 4,
        out_specs=(hbm, hbm),
        scratch_shapes=[pltpu.VMEM(weights.shape, f32), pltpu.VMEM(shadow.shape, f32), dma((2, LAYERS, 2))],
        compiler_params=pltpu.CompilerParams(vmem_limit_bytes=4 * 1024 * 1024),
    )(*(pltpu.with_memory_space_constraint(a, pltpu.VMEM) for a in held))


def solution(mesh):
    split = Mesh(
        mesh.devices.reshape(mesh.shape["dp"], 4, 2, 2, 2),
        ("dp", "expert_0", "expert_1", "shard_0", "shard_1"),
    )
    return jax.shard_map(
        on_device,
        mesh=split,
        in_specs=(
            P(None, EXPERT, DP_SHARD, None),
            P(None, EXPERT, DP_SHARD, None),
            P(None, EXPERT, DP_SHARD, None),
            P(None, EXPERT, DP_SHARD, None),
            P(None, DP_EXPERT_SHARD, None),
        ),
        out_specs=(P(None, EXPERT, DP_SHARD, None), P(None, EXPERT, DP_SHARD, None)),
        check_vma=False,
    )
```

```python
import jax
import jax.numpy as jnp
from jax import lax
from jax.experimental import pallas as pl
from jax.experimental.pallas import tpu as pltpu
from jax.sharding import Mesh
from jax.sharding import PartitionSpec as P

MESH = pl.DeviceIdType.MESH
LAYERS = 2
EXPERT = ("expert_0", "expert_1")
DP_EXPERT_SHARD = ("dp", "expert_0", "expert_1", "shard_0", "shard_1")
DP_SHARD = ("dp", "shard_0", "shard_1")

step_size = 0.5
clip_level = 1.0

NZ = 8
BLOCKS = 4
Z, Y, YH = 0, 1, 2


def kernel(
    acts_in, og, counts_in, weights, shadow, gbuf, w_in, s_in, scalars,
    part_z, part_y, ring_z, ring_y, y_got, y_relay, z_got, z_relay, x_got_z, x_got_y, x_out_z, x_out_y,
    own_half, other_half, acts, counts, a_out, a_got, a_rows, a_t, c_own, c_got, q_own, q_got, q_acc,
    og_sem, in_sem, x_send, x_recv, x_recv_late, a_sem, ring_send, ring_recv,
    y_send, y_mid, y_end, y_parts, y_unit, z_send, z_mid, z_end_sem, g_sem, c_sem, q_sem,
):
    z = lax.axis_index("dp")
    x = lax.axis_index("expert_0")
    y_lo = lax.axis_index("expert_1")
    y_hi = lax.axis_index("shard_0")
    core = lax.axis_index("shard_1")
    y = y_hi * 2 + y_lo
    tokens = acts.shape[1]
    rows = acts.shape[2]
    half_rows = rows // 2
    unit = half_rows // NZ
    own_rows = unit // 2
    part = (part_z, part_y, part_y)
    ring = (ring_z, ring_y, ring_y)
    x_got = (x_got_z, x_got_y)
    x_out = (x_out_z, x_out_y)
    width = (part_z.shape[-1], part_y.shape[-1], part_y.shape[-1] // 2)
    first_col = (0, BLOCKS * width[Z])
    half_cols = BLOCKS * (width[Z] + width[Y])

    def at(z=z, x=x, y_lo=y_lo, y_hi=y_hi, core=core):
        return (z, x, y_lo, y_hi, core)

    def z_next(sign):
        return at(z=lax.rem(z + sign + NZ, NZ))

    def y_next(sign):
        to = lax.rem(y + sign + 4, 4)
        return at(y_lo=lax.rem(to, 2), y_hi=to // 2)

    mate = at(core=1 - core)
    me_group = z * 4 + y_hi * 2 + core
    me_expert = x * 2 + y_lo

    def group_device(offset):
        to = lax.rem(me_group + offset, 32)
        return at(z=to // 4, y_hi=lax.rem(to // 2, 2), core=lax.rem(to, 2))

    def remote(src, dst, send, recv, device):
        return pltpu.make_async_remote_copy(
            src_ref=src, dst_ref=dst, send_sem=send, recv_sem=recv, device_id=device, device_id_type=MESH
        )

    def loop(low, high, act):
        def body(i, _):
            act(i)
            return 0
        lax.fori_loop(low, high, body, 0)

    pieces = ((0, 4 * width[Z]), (first_col[Y], 2 * width[Y]), (first_col[Y] + 2 * width[Y], 2 * width[Y]))

    def og_copy(layer, which, piece):
        first = core if which == 0 else 1 - core
        to = own_half if which == 0 else other_half
        begin, size = pieces[piece]
        cols = pl.ds(pl.multiple_of(first * half_cols + begin, 128), size)
        return pltpu.make_async_copy(
            og.at[layer, :, cols], to.at[layer, :, begin : begin + size], og_sem.at[layer, which, piece]
        )

    in_copies = [
        pltpu.make_async_copy(src, dst, in_sem.at[i])
        for i, (src, dst) in enumerate(((acts_in, acts), (counts_in, counts), (weights, w_in), (shadow, s_in)))
    ]

    barrier = pltpu.get_barrier_semaphore()
    near = (
        mate, z_next(1), z_next(-1), y_next(1), y_next(-1), at(x=x + 1 - 2 * lax.rem(x, 2)), at(x=3 - x)
    )
    for device in near:
        pl.semaphore_signal(barrier, inc=1, device_id=device, device_id_type=MESH)

    og_copy(0, 1, 1).start()
    in_copies[0].start()
    for which, piece in ((0, 1), (1, 0), (0, 0), (1, 2), (0, 2)):
        og_copy(0, which, piece).start()
    in_copies[1].start()

    def cols_of(kind, j):
        return pl.ds(pl.multiple_of(first_col[kind] + j * width[kind], 128), width[kind])

    def convert(layer, kind, j):
        x_out[kind][j] = other_half[layer, :, cols_of(kind, j)].astype(jnp.float32)

    def x_copy(layer, kind, j):
        sem = x_recv.at[4 * kind + j] if layer == 0 else x_recv_late.at[kind]
        return remote(x_out[kind].at[j], x_got[kind].at[layer, j], x_send.at[kind], sem, mate)

    quarter = width[YH] // 2

    def half_cols_of(h):
        return pl.ds(h * quarter, quarter if h == 0 else width[Y] - quarter)

    def x_half(j, h):
        cols = half_cols_of(h)
        return remote(x_out_y.at[j, :, cols], x_got_y.at[0, j, :, cols], x_send.at[Y], x_recv.at[4 + j + 4 * h], mate)

    def x_all(layer, kind):
        return remote(x_out[kind], x_got[kind].at[layer], x_send.at[kind], x_recv_late.at[kind], mate)

    def a_copy(layer):
        return remote(a_out.at[layer], a_got.at[layer], a_sem.at[0, layer], a_sem.at[1, layer], mate)

    def a_join(layer):
        a_rows[:, 0:tokens] = a_out[layer].T
        a_copy(layer).wait_recv()
        a_rows[:, tokens : 2 * tokens] = a_got[layer].T
        for half in range(2):
            side = y_hi if half == 0 else 1 - y_hi
            for zz in range(NZ):
                piece = a_rows[pl.ds(pl.multiple_of(zz * 2 * unit + side * unit, unit), unit), :]
                a_t[layer, half * half_rows + zz * unit : half * half_rows + (zz + 1) * unit, :] = piece.astype(jnp.bfloat16)

    def swap(layer, kind, low, high):
        def act(j):
            convert(layer, kind, j)
            x_copy(layer, kind, j).start()
        loop(low, high, act)

    c_copies = [
        remote(c_own.at[i], c_got.at[i], c_sem.at[0, i], c_sem.at[1, i], device)
        for i, device in enumerate((near[5], near[6], at(y_lo=1 - y_lo)))
    ]

    def c_next(i):
        c_copies[i].wait_recv()
        c_own[i + 1] = c_own[i] + c_got[i]
        if i < 2:
            c_copies[i + 1].start()

    og_copy(0, 1, 1).wait()
    loop(0, 2, lambda j: convert(0, Y, j))
    in_copies[0].wait()
    a_out[...] = acts[...].astype(jnp.float32)
    pl.semaphore_wait(barrier, len(near))

    a_copy(0).start()
    loop(0, 2, lambda j: x_half(j, 0).start())
    og_copy(0, 1, 0).wait()
    swap(0, Z, 0, 2)
    loop(0, 2, lambda j: x_half(j, 1).start())
    swap(0, Z, 2, 4)
    og_copy(0, 1, 2).wait()
    swap(0, Y, 2, 4)
    a_copy(1).start()
    a_join(0)

    def multiply(layer, kind, j):
        if layer == 0:
            x_copy(layer, kind, j).wait_recv()
        theirs = x_got[kind][layer, j].astype(jnp.bfloat16)
        both = jnp.concatenate([own_half[layer, :, cols_of(kind, j)], theirs], axis=0)
        part[kind][layer, j] = jnp.dot(a_t[layer], both, preferred_element_type=jnp.float32)

    def stream(kind, layer, slot):
        full = pl.ds(0, width[kind])
        if kind == Z:
            return slot // 2, lax.rem(slot, 2), layer * 8 + slot, layer * 8 + slot, full
        if kind == Y:
            return slot, 0, layer * 4 + slot, layer * 4 + slot, full
        j = 2 + lax.rem(slot, 2)
        cols = pl.ds(pl.multiple_of(slot // 2 * width[YH], 128), width[YH])
        return j, 0, layer * 4 + j, layer * 4 + 2 + slot, cols

    def sign_of(slot):
        return 1 - 2 * lax.rem(slot, 2)

    def chunk(kind, layer, slot, away):
        j, half, _, _, cols = stream(kind, layer, slot)
        index = lax.rem(z + away + NZ, NZ)
        return part[kind].at[layer, j, pl.ds(pl.multiple_of(half * half_rows + index * unit, unit), unit), cols]

    def long_copy(kind, layer, slot, step):
        _, _, k, sem, cols = stream(kind, layer, slot)
        sign = sign_of(slot)
        src = chunk(kind, layer, slot, sign * 4) if step == 0 else ring[kind].at[k, step - 1, :, cols]
        dst = ring[kind].at[k, step, :, cols]
        return remote(src, dst, ring_send.at[min(kind, Y)], ring_recv.at[sem, step % 2], z_next(sign))

    def short_copy(kind, layer, slot, step):
        _, _, k, sem, cols = stream(kind, layer, slot)
        sign = sign_of(slot)
        src = chunk(kind, layer, slot, sign * -3) if step == 0 else ring[kind].at[k, 3 + step, :, cols]
        dst = ring[kind].at[k, 4 + step, :, cols]
        return remote(src, dst, ring_send.at[min(kind, Y)], ring_recv.at[sem, step % 2], z_next(-sign))

    def both_of(kind, layer, slot, step):
        _, _, k, sem, cols = stream(kind, layer, slot)
        two = ring[kind].at[k, 0:2, :, cols]
        return remote(two, two, ring_send.at[min(kind, Y)], ring_recv.at[sem, step % 2], z_next(1))

    def chain_start(kind, layer, slot):
        long_copy(kind, layer, slot, 0).start()
        short_copy(kind, layer, slot, 0).start()

    def chain_step(kind, layer, slot, step):
        _, _, k, _, cols = stream(kind, layer, slot)
        held = ring[kind]
        sign = sign_of(slot)
        both_of(kind, layer, slot, step - 1).wait_recv()
        held[k, step - 1, :, cols] = held[k, step - 1, :, cols] + chunk(kind, layer, slot, sign * (4 - step))[...]
        if step < 3:
            held[k, 3 + step, :, cols] = held[k, 3 + step, :, cols] + chunk(kind, layer, slot, sign * (step - 3))[...]
        long_copy(kind, layer, slot, step).start()
        if step < 3:
            short_copy(kind, layer, slot, step).start()

    def chain_last(kind, layer, slot):
        _, _, k, _, cols = stream(kind, layer, slot)
        long_copy(kind, layer, slot, 3).wait_recv()
        return ring[kind][k, 3, :, cols] + chunk(kind, layer, slot, 0)[...] + ring[kind][k, 6, :, cols]

    def steps(kind, layer, low, high, step):
        loop(low, high, lambda slot: chain_step(kind, layer, slot, step))

    def starts(kind, layer, low, high):
        loop(low, high, lambda slot: chain_start(kind, layer, slot))

    def z_last(layer):
        def act(slot):
            ring_z[layer * 8 + slot, 3] = chain_last(Z, layer, slot)
        loop(0, 8, act)

    def y_copy(layer, j):
        return remote(
            part_y.at[layer, j, pl.ds(half_rows, half_rows), :], y_relay.at[layer, j],
            y_send.at[0], y_mid.at[layer, j // 2], y_next(sign_of(j)),
        )

    def y_pass(layer, j):
        return remote(y_relay.at[layer, j], y_got.at[layer, j], y_send.at[1], y_end.at[layer, j // 2], y_next(sign_of(j)))

    def pair(layer, p, sems):
        two = y_relay.at[layer, 2 * p : 2 * p + 2]
        return remote(two, two, y_send.at[1], sems.at[layer, p], mate)

    def y_forward(layer, p):
        pair(layer, p, y_mid).wait_recv()
        loop(2 * p, 2 * p + 2, lambda j: y_pass(layer, j).start())

    groups = ((4, -3), (3, -2), (2, -1), (1,), (0,))

    def unit_rows(away):
        return pl.ds(pl.multiple_of(lax.rem(z + away + NZ, NZ) * unit, unit), unit)

    def y_first(layer, j, at_rows, sign, part_of, g):
        others = pl.ds(pl.multiple_of(half_rows + at_rows.start, unit), unit)
        return remote(
            part_y.at[layer, j, others, :], y_relay.at[layer, j, at_rows, :], y_send.at[0], y_parts.at[part_of], y_next(sign)
        )

    def y_second(layer, j, at_rows, sign, part_of, g):
        return remote(
            y_relay.at[layer, j, at_rows, :], y_got.at[layer, j, at_rows, :], y_send.at[1], y_unit.at[g], y_next(sign)
        )

    def y_units(layer, p, hop, part_of, which):
        for g in which:
            for away in groups[g]:
                def act(j):
                    sign = sign_of(j)
                    hop(layer, j, unit_rows(sign * away), sign, part_of, g).start()
                loop(2 * p, 2 * p + 2, act)

    def y_units_wait(layer, p, part_of, units):
        these = y_relay.at[layer, 2 * p : 2 * p + 2, 0 : unit * units, :]
        remote(these, these, y_send.at[0], y_parts.at[part_of], mate).wait_recv()

    def y_units_add(layer, p, g):
        four = y_got.at[layer, 2 * p : 2 * p + 2, 0 : unit * len(groups[g]), :]
        remote(four, four, y_send.at[1], y_unit.at[g], mate).wait_recv()
        for away in groups[g]:
            def act(j):
                at_rows = unit_rows(sign_of(j) * away)
                part_y[layer, j, at_rows, :] = part_y[layer, j, at_rows, :] + y_got[layer, j, at_rows, :]
            loop(2 * p, 2 * p + 2, act)

    def y_begin(layer, p):
        pair(layer, p, y_end).wait_recv()

        def act(j):
            part_y[layer, j, 0:half_rows, :] = part_y[layer, j, 0:half_rows, :] + y_got[layer, j]
            chain_start(Y, layer, j)
        loop(2 * p, 2 * p + 2, act)

    def z_copy(layer, j):
        return remote(
            ring_z.at[layer * 8 + j * 2 + 1, 3], z_relay.at[layer, j], z_send.at[0], z_mid.at[layer], y_next(sign_of(j))
        )

    def z_pass(layer, j):
        return remote(z_relay.at[layer, j], z_got.at[layer, j], z_send.at[1], z_end_sem.at[layer], y_next(sign_of(j)))

    def z_all(layer, sems):
        return remote(z_relay.at[layer], z_got.at[layer], z_send.at[1], sems.at[layer], mate)

    def z_forward(layer):
        z_all(layer, z_mid).wait_recv()
        loop(0, BLOCKS, lambda j: z_pass(layer, j).start())

    def finish(kind, layer, slot, value):
        j, _, k, _, cols = stream(kind, layer, slot)
        held = ring[kind]
        held[k, 3, :, cols] = value
        col = core * half_cols + first_col[min(kind, Y)] + j * width[min(kind, Y)] + cols.start
        where = pl.ds(pl.multiple_of(col, 128), width[kind])

        def of(c):
            return pl.ds(pl.multiple_of(c * own_rows, own_rows), own_rows)

        remote(
            held.at[k, 3, of(1 - core), cols], gbuf.at[layer, :, where], g_sem.at[0], g_sem.at[1], mate
        ).start()
        gbuf[layer, :, where] = held[k, 3, of(core), cols]
        squares = value * value
        folded = squares[0:own_rows] + squares[own_rows : 2 * own_rows]
        total = folded[:, 0:128]
        for i in range(1, width[kind] // 128):
            total = total + folded[:, i * 128 : (i + 1) * 128]
        q_acc[layer] = q_acc[layer] + total

    def z_finish(layer):
        z_all(layer, z_end_sem).wait_recv()
        loop(0, BLOCKS, lambda j: finish(Z, layer, 2 * j, ring_z[layer * 8 + 2 * j, 3] + z_got[layer, j]))

    def y_finish(layer, low, high, kind=Y):
        loop(low, high, lambda slot: finish(kind, layer, slot, chain_last(kind, layer, slot)))

    def q_copy(offset):
        return remote(q_own, q_got.at[offset - 1], q_sem.at[0], q_sem.at[1], group_device(offset))

    def all_of(got, sems):
        return remote(got, got, sems.at[0], sems.at[1], mate)

    def to_y(layer, j):
        multiply(layer, Y, j)
        y_copy(layer, j).start()

    def to_z(j):
        multiply(0, Z, j)
        chain_start(Z, 0, 2 * j)
        chain_start(Z, 0, 2 * j + 1)

    def to_y_half(j, h):
        cols = half_cols_of(h)
        x_half(j, h).wait_recv()
        mine = own_half[0, :, pl.ds(pl.multiple_of(first_col[Y] + j * width[Y] + cols.start, 128), cols.size)]
        both = jnp.concatenate([mine, x_got_y[0, j, :, cols].astype(jnp.bfloat16)], axis=0)
        part_y[0, j, :, cols] = jnp.dot(a_t[0], both, preferred_element_type=jnp.float32)
        remote(
            part_y.at[0, j, pl.ds(half_rows, half_rows), cols], y_relay.at[0, j, :, cols],
            y_send.at[0], y_mid.at[0, 0], y_next(sign_of(j)),
        ).start()

    og_copy(0, 0, 1).wait()
    loop(0, 2, lambda j: to_y_half(j, 0))
    og_copy(0, 0, 0).wait()
    loop(0, 2, to_z)
    loop(0, 2, lambda j: to_y_half(j, 1))
    loop(2, 4, to_z)
    og_copy(0, 0, 2).wait()
    loop(2, 4, lambda j: to_y(0, j))

    for which in (1, 0):
        for piece in (1, 2, 0):
            og_copy(1, which, piece).start()
    in_copies[1].wait()
    c_own[0] = jnp.zeros_like(c_own[0])
    c_own[0, :, 0:8] = counts[:, 0, :].astype(jnp.float32)
    c_copies[0].start()
    q_acc[...] = jnp.zeros_like(q_acc)
    for kind in (Y, Z):
        x_all(0, kind).wait_send()
        for piece in ((0,), (1, 2))[kind]:
            og_copy(1, 1, piece).wait()
        swap(1, kind, 0, 4)
    in_copies[2].start()
    in_copies[3].start()
    for piece in range(3):
        og_copy(1, 0, piece).wait()

    steps(Z, 0, 0, 8, 1)
    a_join(1)
    x_all(1, Y).wait_recv()
    loop(0, 2, lambda j: to_y(1, j))
    x_all(1, Z).wait_recv()
    loop(0, 4, lambda j: multiply(1, Z, j))
    steps(Z, 0, 0, 8, 2)
    y_forward(0, 0)
    loop(2, 4, lambda j: multiply(1, Y, j))
    steps(Z, 0, 0, 8, 3)
    starts(Z, 1, 0, 8)
    y_forward(0, 1)
    z_last(0)
    c_next(0)
    steps(Z, 1, 0, 8, 1)
    y_units(1, 1, y_first, 0, (0, 1))
    y_forward(1, 0)
    steps(Z, 1, 0, 8, 2)
    c_next(1)
    steps(Z, 1, 0, 8, 3)

    y_begin(0, 0)
    y_begin(0, 1)
    z_last(1)
    steps(Y, 0, 0, 4, 1)
    y_units_wait(1, 1, 0, 4)
    y_units(1, 1, y_second, 0, (0, 1))
    y_units(1, 1, y_first, 1, (2,))
    y_units(1, 1, y_first, 2, (3, 4))
    steps(Y, 0, 0, 4, 2)
    steps(Y, 0, 0, 2, 3)
    y_begin(1, 0)
    y_units_add(1, 1, 0)
    starts(YH, 1, 0, 4)
    steps(Y, 1, 0, 2, 1)
    y_units_wait(1, 1, 1, 2)
    y_units(1, 1, y_second, 0, (2,))
    for layer in range(LAYERS):
        loop(0, BLOCKS, lambda j: z_copy(layer, j).start())
    y_units_add(1, 1, 1)
    steps(YH, 1, 0, 4, 1)
    y_units_wait(1, 1, 2, 2)
    y_units(1, 1, y_second, 0, (3, 4))
    steps(Y, 1, 0, 2, 2)
    y_units_add(1, 1, 2)
    steps(YH, 1, 0, 4, 2)
    z_forward(0)
    steps(Y, 1, 0, 2, 3)
    z_forward(1)
    c_next(2)
    y_units_add(1, 1, 3)
    steps(YH, 1, 0, 2, 3)
    steps(Y, 0, 2, 4, 3)
    steps(YH, 1, 2, 4, 3)
    y_finish(0, 0, 2)
    y_finish(1, 0, 2)
    z_finish(0)
    y_units_add(1, 1, 4)
    y_finish(1, 0, 2, YH)
    y_finish(0, 2, 4)
    z_finish(1)
    y_finish(1, 2, 4, YH)

    q_own[0:2] = jnp.sum(q_acc[...], axis=1)
    q_own[2:4] = c_own[3]
    for away in (4, 3, 5, 2, 6, 1, 7):
        loop(away * 4, away * 4 + 4, lambda offset: q_copy(offset).start())
    loop(1, 4, lambda offset: q_copy(offset).start())

    landed = gbuf.at[:, :, 0:half_cols]
    all_g = remote(landed, landed, g_sem.at[0], g_sem.at[1], mate)
    all_g.wait_recv()
    in_copies[2].wait()
    in_copies[3].wait()

    all_g.wait_send()
    for i in range(2):
        remote(y_relay, y_got, y_send.at[i], y_unit.at[0], mate).wait_send()
        remote(z_relay, z_got, z_send.at[i], z_mid.at[0], mate).wait_send()
    for kind in (Z, Y):
        x_all(1, kind).wait_send()
        remote(ring[kind], ring[kind], ring_send.at[kind], ring_recv.at[0, 0], mate).wait_send()
    for layer in range(LAYERS):
        a_copy(layer).wait_send()
    for copy in c_copies:
        copy.wait_send()
    all_of(q_got, q_sem).wait_send()

    all_of(q_got, q_sem).wait_recv()
    sums = q_own[...] + jnp.sum(q_got[...], axis=0)
    root_mean = jnp.sqrt(jnp.sum(sums[0:2], axis=1, keepdims=True) / float(rows * 2 * half_cols))
    totals = sums[2:4]
    lanes = lax.broadcasted_iota(jnp.int32, totals.shape, 1)
    mean_load = jnp.sum(totals, axis=1, keepdims=True) / 8.0
    own_load = jnp.sum(jnp.where(lanes == me_expert, totals, 0.0), axis=1, keepdims=True)
    factor = step_size * (own_load / mean_load) * clip_level / jnp.maximum(root_mean, clip_level)
    beta = own_load / (own_load + mean_load)
    scalars[0:2] = jnp.broadcast_to(factor, (LAYERS, 128))
    scalars[2:4] = jnp.broadcast_to(beta, (LAYERS, 128))


def update(summed, weights, shadow, scalars, new_weights, new_shadow, w_out, s_out, sems):
    rows, ff = summed.shape[1:]
    pieces = 2
    copies = []
    for layer in range(LAYERS):
        factor = jnp.broadcast_to(scalars[layer : layer + 1, :], (rows, 128))
        beta = jnp.broadcast_to(scalars[LAYERS + layer : LAYERS + layer + 1, :], (rows, 128))
        for piece in range(pieces):

            def some(i, _):
                for n in range(8):
                    cols = pl.ds(pl.multiple_of(piece * (ff // pieces) + i * 1024 + n * 128, 128), 128)
                    updated = weights[layer, 0, :, cols] - factor * summed[layer, :, cols]
                    w_out[layer, 0, :, cols] = updated
                    previous = shadow[layer, 0, :, cols]
                    s_out[layer, 0, :, cols] = previous + beta * (updated - previous)
                return 0

            lax.fori_loop(0, ff // pieces // 1024, some, 0)
            cols = pl.ds(piece * (ff // pieces), ff // pieces)
            for i, (src, dst) in enumerate(((w_out, new_weights), (s_out, new_shadow))):
                copy = pltpu.make_async_copy(
                    src.at[layer, 0, :, cols], dst.at[layer, 0, :, cols], sems.at[i, layer, piece]
                )
                copy.start()
                copies.append(copy)
    for copy in copies:
        copy.wait()


def on_device(activations, out_grads, weights, shadow, counts):
    acts, og = activations[:, 0], out_grads[:, 0]
    tokens, rows = acts.shape[1:]
    ff = og.shape[2]
    unit = rows // 2 // NZ
    half = rows // 2
    tiles = ff // 2 // 128 // BLOCKS
    wide_z, wide_y = (tiles * 3 // 7) * 128, (tiles - tiles * 3 // 7) * 128
    f32, bf16 = jnp.float32, jnp.bfloat16
    dma = pltpu.SemaphoreType.DMA
    vmem = pl.BlockSpec(memory_space=pltpu.VMEM)
    hbm = pl.BlockSpec(memory_space=pl.ANY)
    held = pl.pallas_call(
        kernel,
        out_shape=(
            pltpu.VMEM((LAYERS, unit // 2, ff), f32),
            pltpu.VMEM(weights.shape, f32),
            pltpu.VMEM(shadow.shape, f32),
            pltpu.VMEM((2 * LAYERS, 128), f32),
        ),
        in_specs=[hbm] * 5,
        out_specs=(vmem,) * 4,
        scratch_shapes=[
            pltpu.VMEM((LAYERS, BLOCKS, rows, wide_z), f32),
            pltpu.VMEM((LAYERS, BLOCKS, rows, wide_y), f32),
            pltpu.VMEM((LAYERS * 8, NZ - 1, unit, wide_z), f32),
            pltpu.VMEM((LAYERS * 4, NZ - 1, unit, wide_y), f32),
            pltpu.VMEM((LAYERS, BLOCKS, half, wide_y), f32),
            pltpu.VMEM((LAYERS, BLOCKS, half, wide_y), f32),
            pltpu.VMEM((LAYERS, BLOCKS, unit, wide_z), f32),
            pltpu.VMEM((LAYERS, BLOCKS, unit, wide_z), f32),
            pltpu.VMEM((LAYERS, BLOCKS, tokens, wide_z), f32),
            pltpu.VMEM((LAYERS, BLOCKS, tokens, wide_y), f32),
            pltpu.VMEM((BLOCKS, tokens, wide_z), f32),
            pltpu.VMEM((BLOCKS, tokens, wide_y), f32),
            pltpu.VMEM((LAYERS, tokens, ff // 2), bf16),
            pltpu.VMEM((LAYERS, tokens, ff // 2), bf16),
            pltpu.VMEM(acts.shape, bf16),
            pltpu.VMEM(counts.shape, counts.dtype),
            pltpu.VMEM((LAYERS, tokens, rows), f32),
            pltpu.VMEM((LAYERS, tokens, rows), f32),
            pltpu.VMEM((rows, 2 * tokens), f32),
            pltpu.VMEM((LAYERS, rows, 2 * tokens), bf16),
            pltpu.VMEM((4, LAYERS, 128), f32),
            pltpu.VMEM((3, LAYERS, 128), f32),
            pltpu.VMEM((2 * LAYERS, 128), f32),
            pltpu.VMEM((31, 2 * LAYERS, 128), f32),
            pltpu.VMEM((LAYERS, unit // 2, 128), f32),
            dma((LAYERS, 2, 3)),
            dma((4,)),
            dma((2,)),
            dma((10,)),
            dma((2,)),
            dma((2, LAYERS)),
            dma((2,)),
            dma((16, 2)),
            dma((2,)),
            dma((LAYERS, 2)),
            dma((LAYERS, 2)),
            dma((3,)),
            dma((5,)),
            dma((2,)),
            dma((LAYERS,)),
            dma((LAYERS,)),
            dma((2,)),
            dma((2, 3)),
            dma((2,)),
        ],
        compiler_params=pltpu.CompilerParams(
            collective_id=0, has_side_effects=True, vmem_limit_bytes=56 * 1024 * 1024
        ),
    )(acts, og, counts, weights, shadow)
    return pl.pallas_call(
        update,
        out_shape=(jax.ShapeDtypeStruct(weights.shape, f32), jax.ShapeDtypeStruct(shadow.shape, f32)),
        in_specs=[vmem] * 4,
        out_specs=(hbm, hbm),
        scratch_shapes=[pltpu.VMEM(weights.shape, f32), pltpu.VMEM(shadow.shape, f32), dma((2, LAYERS, 2))],
        compiler_params=pltpu.CompilerParams(vmem_limit_bytes=4 * 1024 * 1024),
    )(*(pltpu.with_memory_space_constraint(a, pltpu.VMEM) for a in held))


def solution(mesh):
    split = Mesh(
        mesh.devices.reshape(mesh.shape["dp"], 4, 2, 2, 2),
        ("dp", "expert_0", "expert_1", "shard_0", "shard_1"),
    )
    return jax.shard_map(
        on_device,
        mesh=split,
        in_specs=(
            P(None, EXPERT, DP_SHARD, None),
            P(None, EXPERT, DP_SHARD, None),
            P(None, EXPERT, DP_SHARD, None),
            P(None, EXPERT, DP_SHARD, None),
            P(None, DP_EXPERT_SHARD, None),
        ),
        out_specs=(P(None, EXPERT, DP_SHARD, None), P(None, EXPERT, DP_SHARD, None)),
        check_vma=False,
    )
```

```python
import jax
import jax.numpy as jnp
from jax import lax
from jax.experimental import pallas as pl
from jax.experimental.pallas import tpu as pltpu
from jax.sharding import Mesh
from jax.sharding import PartitionSpec as P

MESH = pl.DeviceIdType.MESH
LAYERS = 2
EXPERT = ("expert_0", "expert_1")
DP_EXPERT_SHARD = ("dp", "expert_0", "expert_1", "shard_0", "shard_1")
DP_SHARD = ("dp", "shard_0", "shard_1")

step_size = 0.5
clip_level = 1.0

NZ = 8
BLOCKS = 4
Z, Y, YH = 0, 1, 2


def kernel(
    acts_in, og, counts_in, weights, shadow, gbuf, w_in, s_in, scalars,
    part_z, part_y, ring_z, ring_y, y_got, y_relay, z_got, z_relay, x_got_z, x_got_y, x_out_z, x_out_y,
    own_half, other_half, acts, counts, a_out, a_got, a_rows, a_t, c_own, c_got, q_own, q_got, q_acc,
    og_sem, in_sem, x_send, x_recv, x_recv_late, a_sem, ring_send, ring_recv,
    y_send, y_mid, y_end, y_parts, y_unit, z_send, z_mid, z_end_sem, g_sem, c_sem, q_sem,
):
    z = lax.axis_index("dp")
    x = lax.axis_index("expert_0")
    y_lo = lax.axis_index("expert_1")
    y_hi = lax.axis_index("shard_0")
    core = lax.axis_index("shard_1")
    y = y_hi * 2 + y_lo
    tokens = acts.shape[1]
    rows = acts.shape[2]
    half_rows = rows // 2
    unit = half_rows // NZ
    own_rows = unit // 2
    part = (part_z, part_y, part_y)
    ring = (ring_z, ring_y, ring_y)
    x_got = (x_got_z, x_got_y)
    x_out = (x_out_z, x_out_y)
    width = (part_z.shape[-1], part_y.shape[-1], part_y.shape[-1] // 2)
    first_col = (0, BLOCKS * width[Z])
    half_cols = BLOCKS * (width[Z] + width[Y])

    def at(z=z, x=x, y_lo=y_lo, y_hi=y_hi, core=core):
        return (z, x, y_lo, y_hi, core)

    def z_next(sign):
        return at(z=lax.rem(z + sign + NZ, NZ))

    def y_next(sign):
        to = lax.rem(y + sign + 4, 4)
        return at(y_lo=lax.rem(to, 2), y_hi=to // 2)

    mate = at(core=1 - core)
    me_group = z * 4 + y_hi * 2 + core
    me_expert = x * 2 + y_lo

    def group_device(offset):
        to = lax.rem(me_group + offset, 32)
        return at(z=to // 4, y_hi=lax.rem(to // 2, 2), core=lax.rem(to, 2))

    def remote(src, dst, send, recv, device):
        return pltpu.make_async_remote_copy(
            src_ref=src, dst_ref=dst, send_sem=send, recv_sem=recv, device_id=device, device_id_type=MESH
        )

    def loop(low, high, act):
        def body(i, _):
            act(i)
            return 0
        lax.fori_loop(low, high, body, 0)

    pieces = ((0, 4 * width[Z]), (first_col[Y], 2 * width[Y]), (first_col[Y] + 2 * width[Y], 2 * width[Y]))

    def og_copy(layer, which, piece):
        first = core if which == 0 else 1 - core
        to = own_half if which == 0 else other_half
        begin, size = pieces[piece]
        cols = pl.ds(pl.multiple_of(first * half_cols + begin, 128), size)
        return pltpu.make_async_copy(
            og.at[layer, :, cols], to.at[layer, :, begin : begin + size], og_sem.at[layer, which, piece]
        )

    in_copies = [
        pltpu.make_async_copy(src, dst, in_sem.at[i])
        for i, (src, dst) in enumerate(((acts_in, acts), (counts_in, counts), (weights, w_in), (shadow, s_in)))
    ]

    barrier = pltpu.get_barrier_semaphore()
    near = (
        mate, z_next(1), z_next(-1), y_next(1), y_next(-1), at(x=x + 1 - 2 * lax.rem(x, 2)), at(x=3 - x)
    )
    for device in near:
        pl.semaphore_signal(barrier, inc=1, device_id=device, device_id_type=MESH)

    og_copy(0, 1, 1).start()
    in_copies[0].start()
    for which, piece in ((0, 1), (1, 0), (0, 0), (1, 2), (0, 2)):
        og_copy(0, which, piece).start()
    in_copies[1].start()

    def cols_of(kind, j):
        return pl.ds(pl.multiple_of(first_col[kind] + j * width[kind], 128), width[kind])

    def convert(layer, kind, j):
        x_out[kind][j] = other_half[layer, :, cols_of(kind, j)].astype(jnp.float32)

    def x_copy(layer, kind, j):
        sem = x_recv.at[4 * kind + j] if layer == 0 else x_recv_late.at[kind]
        return remote(x_out[kind].at[j], x_got[kind].at[layer, j], x_send.at[kind], sem, mate)

    quarter = width[YH] // 2

    def half_cols_of(h):
        return pl.ds(h * quarter, quarter if h == 0 else width[Y] - quarter)

    def x_half(j, h):
        cols = half_cols_of(h)
        return remote(x_out_y.at[j, :, cols], x_got_y.at[0, j, :, cols], x_send.at[Y], x_recv.at[4 + j + 4 * h], mate)

    def x_all(layer, kind):
        return remote(x_out[kind], x_got[kind].at[layer], x_send.at[kind], x_recv_late.at[kind], mate)

    def a_copy(layer):
        return remote(a_out.at[layer], a_got.at[layer], a_sem.at[0, layer], a_sem.at[1, layer], mate)

    def a_join(layer):
        a_rows[:, 0:tokens] = a_out[layer].T
        a_copy(layer).wait_recv()
        a_rows[:, tokens : 2 * tokens] = a_got[layer].T
        for half in range(2):
            side = y_hi if half == 0 else 1 - y_hi
            for zz in range(NZ):
                piece = a_rows[pl.ds(pl.multiple_of(zz * 2 * unit + side * unit, unit), unit), :]
                a_t[layer, half * half_rows + zz * unit : half * half_rows + (zz + 1) * unit, :] = piece.astype(jnp.bfloat16)

    def swap(layer, kind, low, high):
        def act(j):
            convert(layer, kind, j)
            x_copy(layer, kind, j).start()
        loop(low, high, act)

    c_copies = [
        remote(c_own.at[i], c_got.at[i], c_sem.at[0, i], c_sem.at[1, i], device)
        for i, device in enumerate((near[5], near[6], at(y_lo=1 - y_lo)))
    ]

    def c_next(i):
        c_copies[i].wait_recv()
        c_own[i + 1] = c_own[i] + c_got[i]
        if i < 2:
            c_copies[i + 1].start()

    og_copy(0, 1, 1).wait()
    loop(0, 2, lambda j: convert(0, Y, j))
    in_copies[0].wait()
    a_out[...] = acts[...].astype(jnp.float32)
    pl.semaphore_wait(barrier, len(near))

    a_copy(0).start()
    loop(0, 2, lambda j: x_half(j, 0).start())
    og_copy(0, 1, 0).wait()
    swap(0, Z, 0, 2)
    loop(0, 2, lambda j: x_half(j, 1).start())
    swap(0, Z, 2, 4)
    og_copy(0, 1, 2).wait()
    swap(0, Y, 2, 4)
    a_copy(1).start()
    a_join(0)

    def multiply(layer, kind, j):
        if layer == 0:
            x_copy(layer, kind, j).wait_recv()
        theirs = x_got[kind][layer, j].astype(jnp.bfloat16)
        both = jnp.concatenate([own_half[layer, :, cols_of(kind, j)], theirs], axis=0)
        part[kind][layer, j] = jnp.dot(a_t[layer], both, preferred_element_type=jnp.float32)

    def stream(kind, layer, slot):
        full = pl.ds(0, width[kind])
        if kind == Z:
            return slot // 2, lax.rem(slot, 2), layer * 8 + slot, layer * 8 + slot, full
        if kind == Y:
            return slot, 0, layer * 4 + slot, layer * 4 + slot, full
        j = 2 + lax.rem(slot, 2)
        cols = pl.ds(pl.multiple_of(slot // 2 * width[YH], 128), width[YH])
        return j, 0, layer * 4 + j, layer * 4 + 2 + slot, cols

    def sign_of(slot):
        return 1 - 2 * lax.rem(slot, 2)

    def chunk(kind, layer, slot, away):
        j, half, _, _, cols = stream(kind, layer, slot)
        index = lax.rem(z + away + NZ, NZ)
        return part[kind].at[layer, j, pl.ds(pl.multiple_of(half * half_rows + index * unit, unit), unit), cols]

    def long_copy(kind, layer, slot, step):
        _, _, k, sem, cols = stream(kind, layer, slot)
        sign = sign_of(slot)
        src = chunk(kind, layer, slot, sign * 4) if step == 0 else ring[kind].at[k, step - 1, :, cols]
        dst = ring[kind].at[k, step, :, cols]
        return remote(src, dst, ring_send.at[min(kind, Y)], ring_recv.at[sem, step % 2], z_next(sign))

    def short_copy(kind, layer, slot, step):
        _, _, k, sem, cols = stream(kind, layer, slot)
        sign = sign_of(slot)
        src = chunk(kind, layer, slot, sign * -3) if step == 0 else ring[kind].at[k, 3 + step, :, cols]
        dst = ring[kind].at[k, 4 + step, :, cols]
        return remote(src, dst, ring_send.at[min(kind, Y)], ring_recv.at[sem, step % 2], z_next(-sign))

    def both_of(kind, layer, slot, step):
        _, _, k, sem, cols = stream(kind, layer, slot)
        two = ring[kind].at[k, 0:2, :, cols]
        return remote(two, two, ring_send.at[min(kind, Y)], ring_recv.at[sem, step % 2], z_next(1))

    def chain_start(kind, layer, slot):
        long_copy(kind, layer, slot, 0).start()
        short_copy(kind, layer, slot, 0).start()

    def chain_step(kind, layer, slot, step):
        _, _, k, _, cols = stream(kind, layer, slot)
        held = ring[kind]
        sign = sign_of(slot)
        both_of(kind, layer, slot, step - 1).wait_recv()
        held[k, step - 1, :, cols] = held[k, step - 1, :, cols] + chunk(kind, layer, slot, sign * (4 - step))[...]
        if step < 3:
            held[k, 3 + step, :, cols] = held[k, 3 + step, :, cols] + chunk(kind, layer, slot, sign * (step - 3))[...]
        long_copy(kind, layer, slot, step).start()
        if step < 3:
            short_copy(kind, layer, slot, step).start()

    def chain_last(kind, layer, slot):
        _, _, k, _, cols = stream(kind, layer, slot)
        long_copy(kind, layer, slot, 3).wait_recv()
        return ring[kind][k, 3, :, cols] + chunk(kind, layer, slot, 0)[...] + ring[kind][k, 6, :, cols]

    def steps(kind, layer, low, high, step):
        loop(low, high, lambda slot: chain_step(kind, layer, slot, step))

    def starts(kind, layer, low, high):
        loop(low, high, lambda slot: chain_start(kind, layer, slot))

    def z_last(layer):
        def act(slot):
            ring_z[layer * 8 + slot, 3] = chain_last(Z, layer, slot)
        loop(0, 8, act)

    def y_copy(layer, j):
        return remote(
            part_y.at[layer, j, pl.ds(half_rows, half_rows), :], y_relay.at[layer, j],
            y_send.at[0], y_mid.at[layer, j // 2], y_next(sign_of(j)),
        )

    def y_pass(layer, j):
        return remote(y_relay.at[layer, j], y_got.at[layer, j], y_send.at[1], y_end.at[layer, j // 2], y_next(sign_of(j)))

    def pair(layer, p, sems):
        two = y_relay.at[layer, 2 * p : 2 * p + 2]
        return remote(two, two, y_send.at[1], sems.at[layer, p], mate)

    def y_forward(layer, p):
        pair(layer, p, y_mid).wait_recv()
        loop(2 * p, 2 * p + 2, lambda j: y_pass(layer, j).start())

    groups = ((4, -3), (3, -2), (2, -1), (1,), (0,))

    def unit_rows(away):
        return pl.ds(pl.multiple_of(lax.rem(z + away + NZ, NZ) * unit, unit), unit)

    def y_first(layer, j, at_rows, sign, part_of, g):
        others = pl.ds(pl.multiple_of(half_rows + at_rows.start, unit), unit)
        return remote(
            part_y.at[layer, j, others, :], y_relay.at[layer, j, at_rows, :], y_send.at[0], y_parts.at[part_of], y_next(sign)
        )

    def y_second(layer, j, at_rows, sign, part_of, g):
        return remote(
            y_relay.at[layer, j, at_rows, :], y_got.at[layer, j, at_rows, :], y_send.at[1], y_unit.at[g], y_next(sign)
        )

    def y_units(layer, p, hop, part_of, which):
        for g in which:
            for away in groups[g]:
                def act(j):
                    sign = sign_of(j)
                    hop(layer, j, unit_rows(sign * away), sign, part_of, g).start()
                loop(2 * p, 2 * p + 2, act)

    def y_units_wait(layer, p, part_of, units):
        these = y_relay.at[layer, 2 * p : 2 * p + 2, 0 : unit * units, :]
        remote(these, these, y_send.at[0], y_parts.at[part_of], mate).wait_recv()

    def y_units_add(layer, p, g):
        four = y_got.at[layer, 2 * p : 2 * p + 2, 0 : unit * len(groups[g]), :]
        remote(four, four, y_send.at[1], y_unit.at[g], mate).wait_recv()
        for away in groups[g]:
            def act(j):
                at_rows = unit_rows(sign_of(j) * away)
                part_y[layer, j, at_rows, :] = part_y[layer, j, at_rows, :] + y_got[layer, j, at_rows, :]
            loop(2 * p, 2 * p + 2, act)

    def y_begin(layer, p):
        pair(layer, p, y_end).wait_recv()

        def act(j):
            part_y[layer, j, 0:half_rows, :] = part_y[layer, j, 0:half_rows, :] + y_got[layer, j]
            chain_start(Y, layer, j)
        loop(2 * p, 2 * p + 2, act)

    def z_copy(layer, j):
        return remote(
            ring_z.at[layer * 8 + j * 2 + 1, 3], z_relay.at[layer, j], z_send.at[0], z_mid.at[layer], y_next(sign_of(j))
        )

    def z_pass(layer, j):
        return remote(z_relay.at[layer, j], z_got.at[layer, j], z_send.at[1], z_end_sem.at[layer], y_next(sign_of(j)))

    def z_all(layer, sems):
        return remote(z_relay.at[layer], z_got.at[layer], z_send.at[1], sems.at[layer], mate)

    def z_forward(layer):
        z_all(layer, z_mid).wait_recv()
        loop(0, BLOCKS, lambda j: z_pass(layer, j).start())

    def finish(kind, layer, slot, value):
        j, _, k, _, cols = stream(kind, layer, slot)
        held = ring[kind]
        held[k, 3, :, cols] = value
        col = core * half_cols + first_col[min(kind, Y)] + j * width[min(kind, Y)] + cols.start
        where = pl.ds(pl.multiple_of(col, 128), width[kind])

        def of(c):
            return pl.ds(pl.multiple_of(c * own_rows, own_rows), own_rows)

        remote(
            held.at[k, 3, of(1 - core), cols], gbuf.at[layer, :, where], g_sem.at[0], g_sem.at[1], mate
        ).start()
        gbuf[layer, :, where] = held[k, 3, of(core), cols]
        squares = value * value
        folded = squares[0:own_rows] + squares[own_rows : 2 * own_rows]
        total = folded[:, 0:128]
        for i in range(1, width[kind] // 128):
            total = total + folded[:, i * 128 : (i + 1) * 128]
        q_acc[layer] = q_acc[layer] + total

    def z_finish(layer):
        z_all(layer, z_end_sem).wait_recv()
        loop(0, BLOCKS, lambda j: finish(Z, layer, 2 * j, ring_z[layer * 8 + 2 * j, 3] + z_got[layer, j]))

    def y_finish(layer, low, high, kind=Y):
        loop(low, high, lambda slot: finish(kind, layer, slot, chain_last(kind, layer, slot)))

    def q_copy(offset):
        return remote(q_own, q_got.at[offset - 1], q_sem.at[0], q_sem.at[1], group_device(offset))

    def all_of(got, sems):
        return remote(got, got, sems.at[0], sems.at[1], mate)

    def to_y(layer, j):
        multiply(layer, Y, j)
        y_copy(layer, j).start()

    def to_z(j):
        multiply(0, Z, j)
        chain_start(Z, 0, 2 * j)
        chain_start(Z, 0, 2 * j + 1)

    def to_y_half(j, h):
        cols = half_cols_of(h)
        x_half(j, h).wait_recv()
        mine = own_half[0, :, pl.ds(pl.multiple_of(first_col[Y] + j * width[Y] + cols.start, 128), cols.size)]
        both = jnp.concatenate([mine, x_got_y[0, j, :, cols].astype(jnp.bfloat16)], axis=0)
        part_y[0, j, :, cols] = jnp.dot(a_t[0], both, preferred_element_type=jnp.float32)
        remote(
            part_y.at[0, j, pl.ds(half_rows, half_rows), cols], y_relay.at[0, j, :, cols],
            y_send.at[0], y_mid.at[0, 0], y_next(sign_of(j)),
        ).start()

    og_copy(0, 0, 1).wait()
    loop(0, 2, lambda j: to_y_half(j, 0))
    og_copy(0, 0, 0).wait()
    loop(0, 2, to_z)
    loop(0, 2, lambda j: to_y_half(j, 1))
    loop(2, 4, to_z)
    og_copy(0, 0, 2).wait()
    loop(2, 4, lambda j: to_y(0, j))

    for which in (1, 0):
        for piece in (1, 2, 0):
            og_copy(1, which, piece).start()
    in_copies[1].wait()
    c_own[0] = jnp.zeros_like(c_own[0])
    c_own[0, :, 0:8] = counts[:, 0, :].astype(jnp.float32)
    c_copies[0].start()
    q_acc[...] = jnp.zeros_like(q_acc)
    for kind in (Y, Z):
        x_all(0, kind).wait_send()
        for piece in ((0,), (1, 2))[kind]:
            og_copy(1, 1, piece).wait()
        swap(1, kind, 0, 4)
    in_copies[2].start()
    in_copies[3].start()
    for piece in range(3):
        og_copy(1, 0, piece).wait()

    steps(Z, 0, 0, 8, 1)
    a_join(1)
    x_all(1, Y).wait_recv()
    loop(0, 2, lambda j: to_y(1, j))
    x_all(1, Z).wait_recv()
    loop(0, 4, lambda j: multiply(1, Z, j))
    steps(Z, 0, 0, 8, 2)
    y_forward(0, 0)
    loop(2, 4, lambda j: multiply(1, Y, j))
    steps(Z, 0, 0, 8, 3)
    starts(Z, 1, 0, 8)
    y_forward(0, 1)
    z_last(0)
    c_next(0)
    steps(Z, 1, 0, 8, 1)
    y_units(1, 1, y_first, 0, (0, 1))
    y_forward(1, 0)
    steps(Z, 1, 0, 8, 2)
    c_next(1)
    steps(Z, 1, 0, 8, 3)

    y_begin(0, 0)
    y_begin(0, 1)
    z_last(1)
    steps(Y, 0, 0, 4, 1)
    y_units_wait(1, 1, 0, 4)
    y_units(1, 1, y_second, 0, (0, 1))
    y_units(1, 1, y_first, 1, (2,))
    y_units(1, 1, y_first, 2, (3, 4))
    steps(Y, 0, 0, 4, 2)
    y_begin(1, 0)
    steps(Y, 0, 0, 2, 3)
    y_units_add(1, 1, 0)
    starts(YH, 1, 0, 4)
    steps(Y, 1, 0, 2, 1)
    y_units_wait(1, 1, 1, 2)
    y_units(1, 1, y_second, 0, (2,))
    for layer in range(LAYERS):
        loop(0, BLOCKS, lambda j: z_copy(layer, j).start())
    y_units_add(1, 1, 1)
    steps(YH, 1, 0, 4, 1)
    y_units_wait(1, 1, 2, 2)
    y_units(1, 1, y_second, 0, (3, 4))
    steps(Y, 1, 0, 2, 2)
    y_units_add(1, 1, 2)
    steps(YH, 1, 0, 4, 2)
    z_forward(0)
    steps(Y, 1, 0, 2, 3)
    z_forward(1)
    c_next(2)
    y_units_add(1, 1, 3)
    steps(YH, 1, 0, 2, 3)
    steps(Y, 0, 2, 4, 3)
    steps(YH, 1, 2, 4, 3)
    y_finish(0, 0, 2)
    y_finish(1, 0, 2)
    z_finish(0)
    y_units_add(1, 1, 4)
    y_finish(1, 0, 2, YH)
    y_finish(0, 2, 4)
    z_finish(1)
    y_finish(1, 2, 4, YH)

    q_own[0:2] = jnp.sum(q_acc[...], axis=1)
    q_own[2:4] = c_own[3]
    for away in (4, 3, 5, 2, 6, 1, 7):
        loop(away * 4, away * 4 + 4, lambda offset: q_copy(offset).start())
    loop(1, 4, lambda offset: q_copy(offset).start())

    landed = gbuf.at[:, :, 0:half_cols]
    all_g = remote(landed, landed, g_sem.at[0], g_sem.at[1], mate)
    all_g.wait_recv()
    in_copies[2].wait()
    in_copies[3].wait()

    all_g.wait_send()
    for i in range(2):
        remote(y_relay, y_got, y_send.at[i], y_unit.at[0], mate).wait_send()
        remote(z_relay, z_got, z_send.at[i], z_mid.at[0], mate).wait_send()
    for kind in (Z, Y):
        x_all(1, kind).wait_send()
        remote(ring[kind], ring[kind], ring_send.at[kind], ring_recv.at[0, 0], mate).wait_send()
    for layer in range(LAYERS):
        a_copy(layer).wait_send()
    for copy in c_copies:
        copy.wait_send()
    all_of(q_got, q_sem).wait_send()

    all_of(q_got, q_sem).wait_recv()
    sums = q_own[...] + jnp.sum(q_got[...], axis=0)
    root_mean = jnp.sqrt(jnp.sum(sums[0:2], axis=1, keepdims=True) / float(rows * 2 * half_cols))
    totals = sums[2:4]
    lanes = lax.broadcasted_iota(jnp.int32, totals.shape, 1)
    mean_load = jnp.sum(totals, axis=1, keepdims=True) / 8.0
    own_load = jnp.sum(jnp.where(lanes == me_expert, totals, 0.0), axis=1, keepdims=True)
    factor = step_size * (own_load / mean_load) * clip_level / jnp.maximum(root_mean, clip_level)
    beta = own_load / (own_load + mean_load)
    scalars[0:2] = jnp.broadcast_to(factor, (LAYERS, 128))
    scalars[2:4] = jnp.broadcast_to(beta, (LAYERS, 128))


def update(summed, weights, shadow, scalars, new_weights, new_shadow, w_out, s_out, sems):
    rows, ff = summed.shape[1:]
    pieces = 2
    copies = []
    for layer in range(LAYERS):
        factor = jnp.broadcast_to(scalars[layer : layer + 1, :], (rows, 128))
        beta = jnp.broadcast_to(scalars[LAYERS + layer : LAYERS + layer + 1, :], (rows, 128))
        for piece in range(pieces):

            def some(i, _):
                for n in range(8):
                    cols = pl.ds(pl.multiple_of(piece * (ff // pieces) + i * 1024 + n * 128, 128), 128)
                    updated = weights[layer, 0, :, cols] - factor * summed[layer, :, cols]
                    w_out[layer, 0, :, cols] = updated
                    previous = shadow[layer, 0, :, cols]
                    s_out[layer, 0, :, cols] = previous + beta * (updated - previous)
                return 0

            lax.fori_loop(0, ff // pieces // 1024, some, 0)
            cols = pl.ds(piece * (ff // pieces), ff // pieces)
            for i, (src, dst) in enumerate(((w_out, new_weights), (s_out, new_shadow))):
                copy = pltpu.make_async_copy(
                    src.at[layer, 0, :, cols], dst.at[layer, 0, :, cols], sems.at[i, layer, piece]
                )
                copy.start()
                copies.append(copy)
    for copy in copies:
        copy.wait()


def on_device(activations, out_grads, weights, shadow, counts):
    acts, og = activations[:, 0], out_grads[:, 0]
    tokens, rows = acts.shape[1:]
    ff = og.shape[2]
    unit = rows // 2 // NZ
    half = rows // 2
    tiles = ff // 2 // 128 // BLOCKS
    wide_z, wide_y = (tiles * 3 // 7) * 128, (tiles - tiles * 3 // 7) * 128
    f32, bf16 = jnp.float32, jnp.bfloat16
    dma = pltpu.SemaphoreType.DMA
    vmem = pl.BlockSpec(memory_space=pltpu.VMEM)
    hbm = pl.BlockSpec(memory_space=pl.ANY)
    held = pl.pallas_call(
        kernel,
        out_shape=(
            pltpu.VMEM((LAYERS, unit // 2, ff), f32),
            pltpu.VMEM(weights.shape, f32),
            pltpu.VMEM(shadow.shape, f32),
            pltpu.VMEM((2 * LAYERS, 128), f32),
        ),
        in_specs=[hbm] * 5,
        out_specs=(vmem,) * 4,
        scratch_shapes=[
            pltpu.VMEM((LAYERS, BLOCKS, rows, wide_z), f32),
            pltpu.VMEM((LAYERS, BLOCKS, rows, wide_y), f32),
            pltpu.VMEM((LAYERS * 8, NZ - 1, unit, wide_z), f32),
            pltpu.VMEM((LAYERS * 4, NZ - 1, unit, wide_y), f32),
            pltpu.VMEM((LAYERS, BLOCKS, half, wide_y), f32),
            pltpu.VMEM((LAYERS, BLOCKS, half, wide_y), f32),
            pltpu.VMEM((LAYERS, BLOCKS, unit, wide_z), f32),
            pltpu.VMEM((LAYERS, BLOCKS, unit, wide_z), f32),
            pltpu.VMEM((LAYERS, BLOCKS, tokens, wide_z), f32),
            pltpu.VMEM((LAYERS, BLOCKS, tokens, wide_y), f32),
            pltpu.VMEM((BLOCKS, tokens, wide_z), f32),
            pltpu.VMEM((BLOCKS, tokens, wide_y), f32),
            pltpu.VMEM((LAYERS, tokens, ff // 2), bf16),
            pltpu.VMEM((LAYERS, tokens, ff // 2), bf16),
            pltpu.VMEM(acts.shape, bf16),
            pltpu.VMEM(counts.shape, counts.dtype),
            pltpu.VMEM((LAYERS, tokens, rows), f32),
            pltpu.VMEM((LAYERS, tokens, rows), f32),
            pltpu.VMEM((rows, 2 * tokens), f32),
            pltpu.VMEM((LAYERS, rows, 2 * tokens), bf16),
            pltpu.VMEM((4, LAYERS, 128), f32),
            pltpu.VMEM((3, LAYERS, 128), f32),
            pltpu.VMEM((2 * LAYERS, 128), f32),
            pltpu.VMEM((31, 2 * LAYERS, 128), f32),
            pltpu.VMEM((LAYERS, unit // 2, 128), f32),
            dma((LAYERS, 2, 3)),
            dma((4,)),
            dma((2,)),
            dma((10,)),
            dma((2,)),
            dma((2, LAYERS)),
            dma((2,)),
            dma((16, 2)),
            dma((2,)),
            dma((LAYERS, 2)),
            dma((LAYERS, 2)),
            dma((3,)),
            dma((5,)),
            dma((2,)),
            dma((LAYERS,)),
            dma((LAYERS,)),
            dma((2,)),
            dma((2, 3)),
            dma((2,)),
        ],
        compiler_params=pltpu.CompilerParams(
            collective_id=0, has_side_effects=True, vmem_limit_bytes=56 * 1024 * 1024
        ),
    )(acts, og, counts, weights, shadow)
    return pl.pallas_call(
        update,
        out_shape=(jax.ShapeDtypeStruct(weights.shape, f32), jax.ShapeDtypeStruct(shadow.shape, f32)),
        in_specs=[vmem] * 4,
        out_specs=(hbm, hbm),
        scratch_shapes=[pltpu.VMEM(weights.shape, f32), pltpu.VMEM(shadow.shape, f32), dma((2, LAYERS, 2))],
        compiler_params=pltpu.CompilerParams(vmem_limit_bytes=4 * 1024 * 1024),
    )(*(pltpu.with_memory_space_constraint(a, pltpu.VMEM) for a in held))


def solution(mesh):
    split = Mesh(
        mesh.devices.reshape(mesh.shape["dp"], 4, 2, 2, 2),
        ("dp", "expert_0", "expert_1", "shard_0", "shard_1"),
    )
    return jax.shard_map(
        on_device,
        mesh=split,
        in_specs=(
            P(None, EXPERT, DP_SHARD, None),
            P(None, EXPERT, DP_SHARD, None),
            P(None, EXPERT, DP_SHARD, None),
            P(None, EXPERT, DP_SHARD, None),
            P(None, DP_EXPERT_SHARD, None),
        ),
        out_specs=(P(None, EXPERT, DP_SHARD, None), P(None, EXPERT, DP_SHARD, None)),
        check_vma=False,
    )
```

```python
import jax
import jax.numpy as jnp
from jax import lax
from jax.experimental import pallas as pl
from jax.experimental.pallas import tpu as pltpu
from jax.sharding import Mesh
from jax.sharding import PartitionSpec as P

MESH = pl.DeviceIdType.MESH
LAYERS = 2
EXPERT = ("expert_0", "expert_1")
DP_EXPERT_SHARD = ("dp", "expert_0", "expert_1", "shard_0", "shard_1")
DP_SHARD = ("dp", "shard_0", "shard_1")

step_size = 0.5
clip_level = 1.0

NZ = 8
BLOCKS = 4
Z, Y, YH = 0, 1, 2


def kernel(
    acts_in, og, counts_in, weights, shadow, gbuf, w_in, s_in, scalars,
    part_z, part_y, ring_z, ring_y, y_got, y_relay, z_got, z_relay, x_got_z, x_got_y, x_out_z, x_out_y,
    own_half, other_half, acts, counts, a_out, a_got, a_rows, a_t, c_own, c_got, q_own, q_got, q_acc,
    og_sem, in_sem, x_send, x_recv, x_recv_late, a_sem, ring_send, ring_recv,
    y_send, y_mid, y_end, y_parts, y_unit, z_send, z_mid, z_end_sem, g_sem, c_sem, q_sem,
):
    z = lax.axis_index("dp")
    x = lax.axis_index("expert_0")
    y_lo = lax.axis_index("expert_1")
    y_hi = lax.axis_index("shard_0")
    core = lax.axis_index("shard_1")
    y = y_hi * 2 + y_lo
    tokens = acts.shape[1]
    rows = acts.shape[2]
    half_rows = rows // 2
    unit = half_rows // NZ
    own_rows = unit // 2
    part = (part_z, part_y, part_y)
    ring = (ring_z, ring_y, ring_y)
    x_got = (x_got_z, x_got_y)
    x_out = (x_out_z, x_out_y)
    width = (part_z.shape[-1], part_y.shape[-1], part_y.shape[-1] // 2)
    first_col = (0, BLOCKS * width[Z])
    half_cols = BLOCKS * (width[Z] + width[Y])

    def at(z=z, x=x, y_lo=y_lo, y_hi=y_hi, core=core):
        return (z, x, y_lo, y_hi, core)

    def z_next(sign):
        return at(z=lax.rem(z + sign + NZ, NZ))

    def y_next(sign):
        to = lax.rem(y + sign + 4, 4)
        return at(y_lo=lax.rem(to, 2), y_hi=to // 2)

    mate = at(core=1 - core)
    me_group = z * 4 + y_hi * 2 + core
    me_expert = x * 2 + y_lo

    def group_device(offset):
        to = lax.rem(me_group + offset, 32)
        return at(z=to // 4, y_hi=lax.rem(to // 2, 2), core=lax.rem(to, 2))

    def remote(src, dst, send, recv, device):
        return pltpu.make_async_remote_copy(
            src_ref=src, dst_ref=dst, send_sem=send, recv_sem=recv, device_id=device, device_id_type=MESH
        )

    def loop(low, high, act):
        def body(i, _):
            act(i)
            return 0
        lax.fori_loop(low, high, body, 0)

    pieces = ((0, 4 * width[Z]), (first_col[Y], 2 * width[Y]), (first_col[Y] + 2 * width[Y], 2 * width[Y]))

    def og_copy(layer, which, piece):
        first = core if which == 0 else 1 - core
        to = own_half if which == 0 else other_half
        begin, size = pieces[piece]
        cols = pl.ds(pl.multiple_of(first * half_cols + begin, 128), size)
        return pltpu.make_async_copy(
            og.at[layer, :, cols], to.at[layer, :, begin : begin + size], og_sem.at[layer, which, piece]
        )

    in_copies = [
        pltpu.make_async_copy(src, dst, in_sem.at[i])
        for i, (src, dst) in enumerate(((acts_in, acts), (counts_in, counts), (weights, w_in), (shadow, s_in)))
    ]

    barrier = pltpu.get_barrier_semaphore()
    near = (
        mate, z_next(1), z_next(-1), y_next(1), y_next(-1), at(x=x + 1 - 2 * lax.rem(x, 2)), at(x=3 - x)
    )
    for device in near:
        pl.semaphore_signal(barrier, inc=1, device_id=device, device_id_type=MESH)

    og_copy(0, 1, 1).start()
    in_copies[0].start()
    for which, piece in ((0, 1), (1, 0), (0, 0), (1, 2), (0, 2)):
        og_copy(0, which, piece).start()
    in_copies[1].start()

    def cols_of(kind, j):
        return pl.ds(pl.multiple_of(first_col[kind] + j * width[kind], 128), width[kind])

    def convert(layer, kind, j):
        x_out[kind][j] = other_half[layer, :, cols_of(kind, j)].astype(jnp.float32)

    def x_copy(layer, kind, j):
        sem = x_recv.at[4 * kind + j] if layer == 0 else x_recv_late.at[kind]
        return remote(x_out[kind].at[j], x_got[kind].at[layer, j], x_send.at[kind], sem, mate)

    quarter = width[YH] // 2

    def half_cols_of(h):
        return pl.ds(h * quarter, quarter if h == 0 else width[Y] - quarter)

    def x_half(j, h):
        cols = half_cols_of(h)
        return remote(x_out_y.at[j, :, cols], x_got_y.at[0, j, :, cols], x_send.at[Y], x_recv.at[4 + j + 4 * h], mate)

    def x_all(layer, kind):
        return remote(x_out[kind], x_got[kind].at[layer], x_send.at[kind], x_recv_late.at[kind], mate)

    def a_copy(layer):
        return remote(a_out.at[layer], a_got.at[layer], a_sem.at[0, layer], a_sem.at[1, layer], mate)

    def a_join(layer):
        a_rows[:, 0:tokens] = a_out[layer].T
        a_copy(layer).wait_recv()
        a_rows[:, tokens : 2 * tokens] = a_got[layer].T
        for half in range(2):
            side = y_hi if half == 0 else 1 - y_hi
            for zz in range(NZ):
                piece = a_rows[pl.ds(pl.multiple_of(zz * 2 * unit + side * unit, unit), unit), :]
                a_t[layer, half * half_rows + zz * unit : half * half_rows + (zz + 1) * unit, :] = piece.astype(jnp.bfloat16)

    def swap(layer, kind, low, high):
        def act(j):
            convert(layer, kind, j)
            x_copy(layer, kind, j).start()
        loop(low, high, act)

    c_copies = [
        remote(c_own.at[i], c_got.at[i], c_sem.at[0, i], c_sem.at[1, i], device)
        for i, device in enumerate((near[5], near[6], at(y_lo=1 - y_lo)))
    ]

    def c_next(i):
        c_copies[i].wait_recv()
        c_own[i + 1] = c_own[i] + c_got[i]
        if i < 2:
            c_copies[i + 1].start()

    og_copy(0, 1, 1).wait()
    loop(0, 2, lambda j: convert(0, Y, j))
    in_copies[0].wait()
    a_out[...] = acts[...].astype(jnp.float32)
    pl.semaphore_wait(barrier, len(near))

    a_copy(0).start()
    loop(0, 2, lambda j: x_half(j, 0).start())
    og_copy(0, 1, 0).wait()
    swap(0, Z, 0, 2)
    loop(0, 2, lambda j: x_half(j, 1).start())
    swap(0, Z, 2, 4)
    og_copy(0, 1, 2).wait()
    swap(0, Y, 2, 4)
    a_copy(1).start()
    a_join(0)

    def multiply(layer, kind, j):
        if layer == 0:
            x_copy(layer, kind, j).wait_recv()
        theirs = x_got[kind][layer, j].astype(jnp.bfloat16)
        both = jnp.concatenate([own_half[layer, :, cols_of(kind, j)], theirs], axis=0)
        part[kind][layer, j] = jnp.dot(a_t[layer], both, preferred_element_type=jnp.float32)

    def stream(kind, layer, slot):
        full = pl.ds(0, width[kind])
        if kind == Z:
            return slot // 2, lax.rem(slot, 2), layer * 8 + slot, layer * 8 + slot, full
        if kind == Y:
            return slot, 0, layer * 4 + slot, layer * 4 + slot, full
        j = 2 + lax.rem(slot, 2)
        cols = pl.ds(pl.multiple_of(slot // 2 * width[YH], 128), width[YH])
        return j, 0, layer * 4 + j, layer * 4 + 2 + slot, cols

    def sign_of(slot):
        return 1 - 2 * lax.rem(slot, 2)

    def chunk(kind, layer, slot, away):
        j, half, _, _, cols = stream(kind, layer, slot)
        index = lax.rem(z + away + NZ, NZ)
        return part[kind].at[layer, j, pl.ds(pl.multiple_of(half * half_rows + index * unit, unit), unit), cols]

    def long_copy(kind, layer, slot, step):
        _, _, k, sem, cols = stream(kind, layer, slot)
        sign = sign_of(slot)
        src = chunk(kind, layer, slot, sign * 4) if step == 0 else ring[kind].at[k, step - 1, :, cols]
        dst = ring[kind].at[k, step, :, cols]
        return remote(src, dst, ring_send.at[min(kind, Y)], ring_recv.at[sem, step % 2], z_next(sign))

    def short_copy(kind, layer, slot, step):
        _, _, k, sem, cols = stream(kind, layer, slot)
        sign = sign_of(slot)
        src = chunk(kind, layer, slot, sign * -3) if step == 0 else ring[kind].at[k, 3 + step, :, cols]
        dst = ring[kind].at[k, 4 + step, :, cols]
        return remote(src, dst, ring_send.at[min(kind, Y)], ring_recv.at[sem, step % 2], z_next(-sign))

    def both_of(kind, layer, slot, step):
        _, _, k, sem, cols = stream(kind, layer, slot)
        two = ring[kind].at[k, 0:2, :, cols]
        return remote(two, two, ring_send.at[min(kind, Y)], ring_recv.at[sem, step % 2], z_next(1))

    def chain_start(kind, layer, slot):
        long_copy(kind, layer, slot, 0).start()
        short_copy(kind, layer, slot, 0).start()

    def chain_step(kind, layer, slot, step):
        _, _, k, _, cols = stream(kind, layer, slot)
        held = ring[kind]
        sign = sign_of(slot)
        both_of(kind, layer, slot, step - 1).wait_recv()
        held[k, step - 1, :, cols] = held[k, step - 1, :, cols] + chunk(kind, layer, slot, sign * (4 - step))[...]
        if step < 3:
            held[k, 3 + step, :, cols] = held[k, 3 + step, :, cols] + chunk(kind, layer, slot, sign * (step - 3))[...]
        long_copy(kind, layer, slot, step).start()
        if step < 3:
            short_copy(kind, layer, slot, step).start()

    def chain_last(kind, layer, slot):
        _, _, k, _, cols = stream(kind, layer, slot)
        long_copy(kind, layer, slot, 3).wait_recv()
        return ring[kind][k, 3, :, cols] + chunk(kind, layer, slot, 0)[...] + ring[kind][k, 6, :, cols]

    def steps(kind, layer, low, high, step):
        loop(low, high, lambda slot: chain_step(kind, layer, slot, step))

    def starts(kind, layer, low, high):
        loop(low, high, lambda slot: chain_start(kind, layer, slot))

    def z_last(layer):
        def act(slot):
            ring_z[layer * 8 + slot, 3] = chain_last(Z, layer, slot)
        loop(0, 8, act)

    def y_copy(layer, j):
        return remote(
            part_y.at[layer, j, pl.ds(half_rows, half_rows), :], y_relay.at[layer, j],
            y_send.at[0], y_mid.at[layer, j // 2], y_next(sign_of(j)),
        )

    def y_pass(layer, j):
        return remote(y_relay.at[layer, j], y_got.at[layer, j], y_send.at[1], y_end.at[layer, j // 2], y_next(sign_of(j)))

    def pair(layer, p, sems):
        two = y_relay.at[layer, 2 * p : 2 * p + 2]
        return remote(two, two, y_send.at[1], sems.at[layer, p], mate)

    def y_forward(layer, p):
        pair(layer, p, y_mid).wait_recv()
        loop(2 * p, 2 * p + 2, lambda j: y_pass(layer, j).start())

    groups = ((4, -3), (3, -2), (2, -1), (1,), (0,))

    def unit_rows(away):
        return pl.ds(pl.multiple_of(lax.rem(z + away + NZ, NZ) * unit, unit), unit)

    def y_first(layer, j, at_rows, sign, part_of, g):
        others = pl.ds(pl.multiple_of(half_rows + at_rows.start, unit), unit)
        return remote(
            part_y.at[layer, j, others, :], y_relay.at[layer, j, at_rows, :], y_send.at[0], y_parts.at[part_of], y_next(sign)
        )

    def y_second(layer, j, at_rows, sign, part_of, g):
        return remote(
            y_relay.at[layer, j, at_rows, :], y_got.at[layer, j, at_rows, :], y_send.at[1], y_unit.at[g], y_next(sign)
        )

    def y_units(layer, p, hop, part_of, which):
        for g in which:
            for away in groups[g]:
                def act(j):
                    sign = sign_of(j)
                    hop(layer, j, unit_rows(sign * away), sign, part_of, g).start()
                loop(2 * p, 2 * p + 2, act)

    def y_units_wait(layer, p, part_of, units):
        these = y_relay.at[layer, 2 * p : 2 * p + 2, 0 : unit * units, :]
        remote(these, these, y_send.at[0], y_parts.at[part_of], mate).wait_recv()

    def y_units_add(layer, p, g):
        four = y_got.at[layer, 2 * p : 2 * p + 2, 0 : unit * len(groups[g]), :]
        remote(four, four, y_send.at[1], y_unit.at[g], mate).wait_recv()
        for away in groups[g]:
            def act(j):
                at_rows = unit_rows(sign_of(j) * away)
                part_y[layer, j, at_rows, :] = part_y[layer, j, at_rows, :] + y_got[layer, j, at_rows, :]
            loop(2 * p, 2 * p + 2, act)

    def y_begin(layer, p):
        pair(layer, p, y_end).wait_recv()

        def act(j):
            part_y[layer, j, 0:half_rows, :] = part_y[layer, j, 0:half_rows, :] + y_got[layer, j]
            chain_start(Y, layer, j)
        loop(2 * p, 2 * p + 2, act)

    def z_copy(layer, j):
        return remote(
            ring_z.at[layer * 8 + j * 2 + 1, 3], z_relay.at[layer, j], z_send.at[0], z_mid.at[layer], y_next(sign_of(j))
        )

    def z_pass(layer, j):
        return remote(z_relay.at[layer, j], z_got.at[layer, j], z_send.at[1], z_end_sem.at[layer], y_next(sign_of(j)))

    def z_all(layer, sems):
        return remote(z_relay.at[layer], z_got.at[layer], z_send.at[1], sems.at[layer], mate)

    def z_forward(layer):
        z_all(layer, z_mid).wait_recv()
        loop(0, BLOCKS, lambda j: z_pass(layer, j).start())

    def finish(kind, layer, slot, value):
        j, _, k, _, cols = stream(kind, layer, slot)
        held = ring[kind]
        held[k, 3, :, cols] = value
        col = core * half_cols + first_col[min(kind, Y)] + j * width[min(kind, Y)] + cols.start
        where = pl.ds(pl.multiple_of(col, 128), width[kind])

        def of(c):
            return pl.ds(pl.multiple_of(c * own_rows, own_rows), own_rows)

        remote(
            held.at[k, 3, of(1 - core), cols], gbuf.at[layer, :, where], g_sem.at[0], g_sem.at[1], mate
        ).start()
        gbuf[layer, :, where] = held[k, 3, of(core), cols]
        squares = value * value
        folded = squares[0:own_rows] + squares[own_rows : 2 * own_rows]
        total = folded[:, 0:128]
        for i in range(1, width[kind] // 128):
            total = total + folded[:, i * 128 : (i + 1) * 128]
        q_acc[layer] = q_acc[layer] + total

    def z_finish(layer):
        z_all(layer, z_end_sem).wait_recv()
        loop(0, BLOCKS, lambda j: finish(Z, layer, 2 * j, ring_z[layer * 8 + 2 * j, 3] + z_got[layer, j]))

    def y_finish(layer, low, high, kind=Y):
        loop(low, high, lambda slot: finish(kind, layer, slot, chain_last(kind, layer, slot)))

    def q_copy(offset):
        return remote(q_own, q_got.at[offset - 1], q_sem.at[0], q_sem.at[1], group_device(offset))

    def all_of(got, sems):
        return remote(got, got, sems.at[0], sems.at[1], mate)

    def to_y(layer, j):
        multiply(layer, Y, j)
        y_copy(layer, j).start()

    def to_z(j):
        multiply(0, Z, j)
        chain_start(Z, 0, 2 * j)
        chain_start(Z, 0, 2 * j + 1)

    def to_y_half(j, h):
        cols = half_cols_of(h)
        x_half(j, h).wait_recv()
        mine = own_half[0, :, pl.ds(pl.multiple_of(first_col[Y] + j * width[Y] + cols.start, 128), cols.size)]
        both = jnp.concatenate([mine, x_got_y[0, j, :, cols].astype(jnp.bfloat16)], axis=0)
        part_y[0, j, :, cols] = jnp.dot(a_t[0], both, preferred_element_type=jnp.float32)
        remote(
            part_y.at[0, j, pl.ds(half_rows, half_rows), cols], y_relay.at[0, j, :, cols],
            y_send.at[0], y_mid.at[0, 0], y_next(sign_of(j)),
        ).start()

    og_copy(0, 0, 1).wait()
    loop(0, 2, lambda j: to_y_half(j, 0))
    og_copy(0, 0, 0).wait()
    loop(0, 2, to_z)
    loop(0, 2, lambda j: to_y_half(j, 1))
    loop(2, 4, to_z)
    og_copy(0, 0, 2).wait()
    loop(2, 4, lambda j: to_y(0, j))

    for which in (1, 0):
        for piece in (1, 2, 0):
            og_copy(1, which, piece).start()
    in_copies[1].wait()
    c_own[0] = jnp.zeros_like(c_own[0])
    c_own[0, :, 0:8] = counts[:, 0, :].astype(jnp.float32)
    c_copies[0].start()
    q_acc[...] = jnp.zeros_like(q_acc)
    for kind in (Y, Z):
        x_all(0, kind).wait_send()
        for piece in ((0,), (1, 2))[kind]:
            og_copy(1, 1, piece).wait()
        swap(1, kind, 0, 4)
    in_copies[2].start()
    in_copies[3].start()
    for piece in range(3):
        og_copy(1, 0, piece).wait()

    steps(Z, 0, 0, 8, 1)
    a_join(1)
    x_all(1, Y).wait_recv()
    loop(0, 2, lambda j: to_y(1, j))
    x_all(1, Z).wait_recv()
    loop(0, 4, lambda j: multiply(1, Z, j))
    steps(Z, 0, 0, 8, 2)
    y_forward(0, 0)
    loop(2, 4, lambda j: multiply(1, Y, j))
    steps(Z, 0, 0, 8, 3)
    starts(Z, 1, 0, 8)
    y_forward(0, 1)
    z_last(0)
    c_next(0)
    steps(Z, 1, 0, 8, 1)
    y_units(1, 1, y_first, 0, (0, 1))
    y_forward(1, 0)
    steps(Z, 1, 0, 8, 2)
    c_next(1)
    steps(Z, 1, 0, 8, 3)

    y_begin(0, 0)
    y_begin(0, 1)
    z_last(1)
    steps(Y, 0, 0, 4, 1)
    y_units_wait(1, 1, 0, 4)
    y_units(1, 1, y_second, 0, (0, 1))
    y_units(1, 1, y_first, 1, (2,))
    y_units(1, 1, y_first, 2, (3, 4))
    steps(Y, 0, 0, 4, 2)
    y_begin(1, 0)
    steps(Y, 0, 0, 2, 3)
    y_units_add(1, 1, 0)
    starts(YH, 1, 0, 4)
    steps(Y, 1, 0, 2, 1)
    y_units_wait(1, 1, 1, 2)
    y_units(1, 1, y_second, 0, (2,))
    loop(0, BLOCKS, lambda j: z_copy(0, j).start())
    y_units_add(1, 1, 1)
    steps(YH, 1, 0, 4, 1)
    y_units_wait(1, 1, 2, 2)
    y_units(1, 1, y_second, 0, (3,))
    loop(0, BLOCKS, lambda j: z_copy(1, j).start())
    y_units(1, 1, y_second, 0, (4,))
    steps(Y, 1, 0, 2, 2)
    y_units_add(1, 1, 2)
    steps(YH, 1, 0, 4, 2)
    z_forward(0)
    steps(Y, 1, 0, 2, 3)
    z_forward(1)
    c_next(2)
    y_units_add(1, 1, 3)
    steps(YH, 1, 0, 2, 3)
    steps(Y, 0, 2, 4, 3)
    steps(YH, 1, 2, 4, 3)
    y_finish(0, 0, 2)
    y_finish(1, 0, 2)
    z_finish(0)
    y_units_add(1, 1, 4)
    y_finish(1, 0, 2, YH)
    y_finish(0, 2, 4)
    z_finish(1)
    y_finish(1, 2, 4, YH)

    q_own[0:2] = jnp.sum(q_acc[...], axis=1)
    q_own[2:4] = c_own[3]
    for away in (4, 3, 5, 2, 6, 1, 7):
        loop(away * 4, away * 4 + 4, lambda offset: q_copy(offset).start())
    loop(1, 4, lambda offset: q_copy(offset).start())

    landed = gbuf.at[:, :, 0:half_cols]
    all_g = remote(landed, landed, g_sem.at[0], g_sem.at[1], mate)
    all_g.wait_recv()
    in_copies[2].wait()
    in_copies[3].wait()

    all_g.wait_send()
    for i in range(2):
        remote(y_relay, y_got, y_send.at[i], y_unit.at[0], mate).wait_send()
        remote(z_relay, z_got, z_send.at[i], z_mid.at[0], mate).wait_send()
    for kind in (Z, Y):
        x_all(1, kind).wait_send()
        remote(ring[kind], ring[kind], ring_send.at[kind], ring_recv.at[0, 0], mate).wait_send()
    for layer in range(LAYERS):
        a_copy(layer).wait_send()
    for copy in c_copies:
        copy.wait_send()
    all_of(q_got, q_sem).wait_send()

    all_of(q_got, q_sem).wait_recv()
    sums = q_own[...] + jnp.sum(q_got[...], axis=0)
    root_mean = jnp.sqrt(jnp.sum(sums[0:2], axis=1, keepdims=True) / float(rows * 2 * half_cols))
    totals = sums[2:4]
    lanes = lax.broadcasted_iota(jnp.int32, totals.shape, 1)
    mean_load = jnp.sum(totals, axis=1, keepdims=True) / 8.0
    own_load = jnp.sum(jnp.where(lanes == me_expert, totals, 0.0), axis=1, keepdims=True)
    factor = step_size * (own_load / mean_load) * clip_level / jnp.maximum(root_mean, clip_level)
    beta = own_load / (own_load + mean_load)
    scalars[0:2] = jnp.broadcast_to(factor, (LAYERS, 128))
    scalars[2:4] = jnp.broadcast_to(beta, (LAYERS, 128))


def update(summed, weights, shadow, scalars, new_weights, new_shadow, w_out, s_out, sems):
    rows, ff = summed.shape[1:]
    pieces = 2
    copies = []
    for layer in range(LAYERS):
        factor = jnp.broadcast_to(scalars[layer : layer + 1, :], (rows, 128))
        beta = jnp.broadcast_to(scalars[LAYERS + layer : LAYERS + layer + 1, :], (rows, 128))
        for piece in range(pieces):

            def some(i, _):
                for n in range(8):
                    cols = pl.ds(pl.multiple_of(piece * (ff // pieces) + i * 1024 + n * 128, 128), 128)
                    updated = weights[layer, 0, :, cols] - factor * summed[layer, :, cols]
                    w_out[layer, 0, :, cols] = updated
                    previous = shadow[layer, 0, :, cols]
                    s_out[layer, 0, :, cols] = previous + beta * (updated - previous)
                return 0

            lax.fori_loop(0, ff // pieces // 1024, some, 0)
            cols = pl.ds(piece * (ff // pieces), ff // pieces)
            for i, (src, dst) in enumerate(((w_out, new_weights), (s_out, new_shadow))):
                copy = pltpu.make_async_copy(
                    src.at[layer, 0, :, cols], dst.at[layer, 0, :, cols], sems.at[i, layer, piece]
                )
                copy.start()
                copies.append(copy)
    for copy in copies:
        copy.wait()


def on_device(activations, out_grads, weights, shadow, counts):
    acts, og = activations[:, 0], out_grads[:, 0]
    tokens, rows = acts.shape[1:]
    ff = og.shape[2]
    unit = rows // 2 // NZ
    half = rows // 2
    tiles = ff // 2 // 128 // BLOCKS
    wide_z, wide_y = (tiles * 3 // 7) * 128, (tiles - tiles * 3 // 7) * 128
    f32, bf16 = jnp.float32, jnp.bfloat16
    dma = pltpu.SemaphoreType.DMA
    vmem = pl.BlockSpec(memory_space=pltpu.VMEM)
    hbm = pl.BlockSpec(memory_space=pl.ANY)
    held = pl.pallas_call(
        kernel,
        out_shape=(
            pltpu.VMEM((LAYERS, unit // 2, ff), f32),
            pltpu.VMEM(weights.shape, f32),
            pltpu.VMEM(shadow.shape, f32),
            pltpu.VMEM((2 * LAYERS, 128), f32),
        ),
        in_specs=[hbm] * 5,
        out_specs=(vmem,) * 4,
        scratch_shapes=[
            pltpu.VMEM((LAYERS, BLOCKS, rows, wide_z), f32),
            pltpu.VMEM((LAYERS, BLOCKS, rows, wide_y), f32),
            pltpu.VMEM((LAYERS * 8, NZ - 1, unit, wide_z), f32),
            pltpu.VMEM((LAYERS * 4, NZ - 1, unit, wide_y), f32),
            pltpu.VMEM((LAYERS, BLOCKS, half, wide_y), f32),
            pltpu.VMEM((LAYERS, BLOCKS, half, wide_y), f32),
            pltpu.VMEM((LAYERS, BLOCKS, unit, wide_z), f32),
            pltpu.VMEM((LAYERS, BLOCKS, unit, wide_z), f32),
            pltpu.VMEM((LAYERS, BLOCKS, tokens, wide_z), f32),
            pltpu.VMEM((LAYERS, BLOCKS, tokens, wide_y), f32),
            pltpu.VMEM((BLOCKS, tokens, wide_z), f32),
            pltpu.VMEM((BLOCKS, tokens, wide_y), f32),
            pltpu.VMEM((LAYERS, tokens, ff // 2), bf16),
            pltpu.VMEM((LAYERS, tokens, ff // 2), bf16),
            pltpu.VMEM(acts.shape, bf16),
            pltpu.VMEM(counts.shape, counts.dtype),
            pltpu.VMEM((LAYERS, tokens, rows), f32),
            pltpu.VMEM((LAYERS, tokens, rows), f32),
            pltpu.VMEM((rows, 2 * tokens), f32),
            pltpu.VMEM((LAYERS, rows, 2 * tokens), bf16),
            pltpu.VMEM((4, LAYERS, 128), f32),
            pltpu.VMEM((3, LAYERS, 128), f32),
            pltpu.VMEM((2 * LAYERS, 128), f32),
            pltpu.VMEM((31, 2 * LAYERS, 128), f32),
            pltpu.VMEM((LAYERS, unit // 2, 128), f32),
            dma((LAYERS, 2, 3)),
            dma((4,)),
            dma((2,)),
            dma((10,)),
            dma((2,)),
            dma((2, LAYERS)),
            dma((2,)),
            dma((16, 2)),
            dma((2,)),
            dma((LAYERS, 2)),
            dma((LAYERS, 2)),
            dma((3,)),
            dma((5,)),
            dma((2,)),
            dma((LAYERS,)),
            dma((LAYERS,)),
            dma((2,)),
            dma((2, 3)),
            dma((2,)),
        ],
        compiler_params=pltpu.CompilerParams(
            collective_id=0, has_side_effects=True, vmem_limit_bytes=56 * 1024 * 1024
        ),
    )(acts, og, counts, weights, shadow)
    return pl.pallas_call(
        update,
        out_shape=(jax.ShapeDtypeStruct(weights.shape, f32), jax.ShapeDtypeStruct(shadow.shape, f32)),
        in_specs=[vmem] * 4,
        out_specs=(hbm, hbm),
        scratch_shapes=[pltpu.VMEM(weights.shape, f32), pltpu.VMEM(shadow.shape, f32), dma((2, LAYERS, 2))],
        compiler_params=pltpu.CompilerParams(vmem_limit_bytes=4 * 1024 * 1024),
    )(*(pltpu.with_memory_space_constraint(a, pltpu.VMEM) for a in held))


def solution(mesh):
    split = Mesh(
        mesh.devices.reshape(mesh.shape["dp"], 4, 2, 2, 2),
        ("dp", "expert_0", "expert_1", "shard_0", "shard_1"),
    )
    return jax.shard_map(
        on_device,
        mesh=split,
        in_specs=(
            P(None, EXPERT, DP_SHARD, None),
            P(None, EXPERT, DP_SHARD, None),
            P(None, EXPERT, DP_SHARD, None),
            P(None, EXPERT, DP_SHARD, None),
            P(None, DP_EXPERT_SHARD, None),
        ),
        out_specs=(P(None, EXPERT, DP_SHARD, None), P(None, EXPERT, DP_SHARD, None)),
        check_vma=False,
    )
```
